8 devices in a mesh: data: 1 (over z), heads: 2 (over y), seq: 4 (over x, core).
Axes of the slice: x: 2, y: 2, z: 1, core: 2. Of those that a mesh axis runs over, the one named last changes fastest.
Arguments:
- tokens: bfloat16 [16, 768, 1024], P('data', 'seq')
- theta_q: bfloat16 [1024, 1024], P(None, 'heads')
- theta_k: bfloat16 [1024, 1024], P(None, 'heads')
- theta_v: bfloat16 [1024, 1024], P(None, 'heads')
- w_out: bfloat16 [1024, 1024], P('heads')
- w_one: float32 [16, 64, 256], P('heads')
- b_one: float32 [16, 256], P('heads')
- w_two: float32 [16, 256, 64], P('heads')
- b_two: float32 [16, 64], P('heads')
- ln_gain: float32 [16, 64], P('heads')
- ln_bias: float32 [16, 64], P('heads')
- inner_lr: float32 [16], P('heads')
Outputs:
- output: bfloat16 [16, 768, 1024], P('data', 'seq')
All inputs are finite; a program needn't handle non-finite values.
Results may differ from the reference program's by a relative error of at most 0.001.
Values are sent between devices in bfloat16 or wider.
A program may use at most 1 GiB of HBM per device.

```python
import jax
import jax.numpy as jnp
from jax import lax

NUM_SEQS = 16
SEQ_LEN = 768
MODEL_DIM = 1024
NUM_HEADS = 16
HEAD_DIM = 64
MINI_BATCH = 16
LN_EPS = 1e-6


def setup_inputs(seed: int = 0, part: int = 0) -> dict:
    base_key = jax.random.key(seed)
    tok_key = jax.random.fold_in(base_key, part)
    sub_keys = jax.random.split(base_key, 11)
    inner_dim = 4 * HEAD_DIM
    proj_width = NUM_HEADS * HEAD_DIM
    tokens = jax.random.normal(tok_key, (NUM_SEQS, SEQ_LEN, MODEL_DIM), jnp.float32)
    theta_q = jax.random.normal(sub_keys[0], (MODEL_DIM, proj_width), jnp.float32) * MODEL_DIM ** -0.5
    theta_k = jax.random.normal(sub_keys[1], (MODEL_DIM, proj_width), jnp.float32) * MODEL_DIM ** -0.5
    theta_v = jax.random.normal(sub_keys[2], (MODEL_DIM, proj_width), jnp.float32) * MODEL_DIM ** -0.5
    w_out = jax.random.normal(sub_keys[3], (proj_width, MODEL_DIM), jnp.float32) * proj_width ** -0.5
    w_one = jax.random.normal(sub_keys[4], (NUM_HEADS, HEAD_DIM, inner_dim), jnp.float32) * HEAD_DIM ** -0.5
    b_one = 0.5 * jax.random.normal(sub_keys[5], (NUM_HEADS, inner_dim), jnp.float32)
    w_two = jax.random.normal(sub_keys[6], (NUM_HEADS, inner_dim, HEAD_DIM), jnp.float32) * inner_dim ** -0.5
    b_two = 0.3 * jax.random.normal(sub_keys[7], (NUM_HEADS, HEAD_DIM), jnp.float32)
    ln_gain = 1.0 + 0.2 * jax.random.normal(sub_keys[8], (NUM_HEADS, HEAD_DIM), jnp.float32)
    ln_bias = 0.2 * jax.random.normal(sub_keys[9], (NUM_HEADS, HEAD_DIM), jnp.float32)
    inner_lr = jax.random.uniform(sub_keys[10], (NUM_HEADS,), jnp.float32, 0.5, 1.5) / inner_dim
    return dict(tokens=tokens.astype(jnp.bfloat16), theta_q=theta_q.astype(jnp.bfloat16), theta_k=theta_k.astype(jnp.bfloat16), theta_v=theta_v.astype(jnp.bfloat16), w_out=w_out.astype(jnp.bfloat16), w_one=w_one, b_one=b_one, w_two=w_two, b_two=b_two, ln_gain=ln_gain, ln_bias=ln_bias, inner_lr=inner_lr)


def layer_norm(z_out, ln_gain, ln_bias):
    row_mean = jnp.mean(z_out, axis=-1, keepdims=True)
    centered = z_out - row_mean
    row_var = jnp.mean(centered * centered, axis=-1, keepdims=True)
    return centered * lax.rsqrt(row_var + LN_EPS) * ln_gain + ln_bias


def inner_model(params, z_in, ln_gain, ln_bias):
    w_one, b_one, w_two, b_two = params
    hidden = jax.nn.gelu(z_in @ w_one + b_one, approximate=True)
    return z_in + layer_norm(hidden @ w_two + b_two, ln_gain, ln_bias)


def head_step(params, key_blk, query_blk, value_blk, ln_gain, ln_bias, inner_lr):
    def inner_loss(cur_params):
        recon_err = inner_model(cur_params, key_blk, ln_gain, ln_bias) - value_blk
        return jnp.sum(recon_err * recon_err)
    inner_grads = jax.grad(inner_loss)(params)
    new_params = tuple(weight_arr - (inner_lr / MINI_BATCH) * grad_val for weight_arr, grad_val in zip(params, inner_grads))
    return new_params, inner_model(new_params, query_blk, ln_gain, ln_bias)


def reference(tokens, theta_q, theta_k, theta_v, w_out, w_one, b_one, w_two, b_two, ln_gain, ln_bias, inner_lr):
    num_steps = SEQ_LEN // MINI_BATCH
    flat_tok = tokens.reshape(NUM_SEQS * SEQ_LEN, MODEL_DIM)

    def project(weight_mat):
        projected = jnp.dot(flat_tok, weight_mat, preferred_element_type=jnp.float32)
        projected = projected.reshape(NUM_SEQS, num_steps, MINI_BATCH, NUM_HEADS, HEAD_DIM)
        return jnp.transpose(projected, (1, 0, 3, 2, 4))

    per_head = jax.vmap(head_step, in_axes=(0, 0, 0, 0, 0, 0, 0))
    per_seq = jax.vmap(per_head, in_axes=(0, 0, 0, 0, None, None, None))

    def scan_step(inner_state, block_set):
        key_blk, query_blk, value_blk = block_set
        return per_seq(inner_state, key_blk, query_blk, value_blk, ln_gain, ln_bias, inner_lr)

    init_state = tuple(jnp.broadcast_to(weight_arr, (NUM_SEQS,) + weight_arr.shape) for weight_arr in (w_one, b_one, w_two, b_two))
    final_state, head_outs = lax.scan(scan_step, init_state, (project(theta_k), project(theta_q), project(theta_v)))
    head_outs = jnp.transpose(head_outs, (1, 0, 3, 2, 4)).reshape(NUM_SEQS * SEQ_LEN, NUM_HEADS * HEAD_DIM)
    result = jnp.dot(head_outs.astype(jnp.bfloat16), w_out, preferred_element_type=jnp.float32)
    return result.astype(jnp.bfloat16).reshape(NUM_SEQS, SEQ_LEN, MODEL_DIM)
```

```python
import functools

import jax
import jax.numpy as jnp
from jax import lax
from jax.experimental import pallas as pl
from jax.experimental.pallas import tpu as pltpu
from jax.sharding import PartitionSpec as P

MINI_BATCH = 16
LN_EPS = 1e-6
GELU_C0 = 0.7978845608028654
GELU_C1 = 0.044715
f32 = jnp.float32
bf16 = jnp.bfloat16


def split3(val):
    high = val.astype(bf16)
    rest = val - high.astype(f32)
    mid = rest.astype(bf16)
    return high, mid, (rest - mid.astype(f32)).astype(bf16)


def dot_nn(lhs, rhs):
    return lax.dot_general(lhs, rhs, (((1,), (0,)), ((), ())), preferred_element_type=f32)


def dot_nt(lhs, rhs):
    return lax.dot_general(lhs, rhs, (((1,), (1,)), ((), ())), preferred_element_type=f32)


def dot_tn(lhs, rhs):
    return lax.dot_general(lhs, rhs, (((0,), (0,)), ((), ())), preferred_element_type=f32)


def rows(*parts):
    return jnp.concatenate(parts, 0)


def lanes(*parts):
    return jnp.concatenate(parts, 1)


def rep8(val, count):
    return rows(*([val] * (count // 8)))


def sum3(val, count):
    return val[0:count] + val[count:2 * count] + val[2 * count:3 * count]


def gelu_and_slope(z_val, key_rows):
    square = z_val * z_val
    tanh_val = jnp.tanh(z_val * (GELU_C0 + (GELU_C0 * GELU_C1) * square))
    half = 0.5 * z_val
    act = half + half * tanh_val
    tanh_key = tanh_val[:key_rows]
    slope = (0.5 + 0.5 * tanh_key) + half[:key_rows] * (1.0 - tanh_key * tanh_key) * (GELU_C0 + (3 * GELU_C0 * GELU_C1) * square[:key_rows])
    return act, slope


def inner_kernel(steps, groups, heads, k_ref, q_ref, v_ref, w1_in, w2_in, b1_in, b2_in, gain, bias, rate, o_ref,
                 w1, w2, w1_parts, w2_parts, b1, b2, act, slope, d_two, d_one, key_t, key_dup, query_dup, value_dup):
    low = lax.broadcasted_iota(jnp.int32, (16, 128), 1) < 64
    pad64 = jnp.zeros((64, 256), bf16)
    one = jnp.ones((16, 128), bf16)
    zero = jnp.zeros((16, 128), bf16)

    @pl.loop(0, groups)
    def _(g):
        for h in range(heads):
            first, second = w1_in[h], w2_in[h]
            w1[g, h] = first
            w2[g, h] = second
            w1_parts[g, h] = rows(*split3(first))
            w2_parts[g, h] = rows(*split3(second))
            b1[g, h] = b1_in[h]
            b2[g, h] = b2_in[h]

    def both_halves(tile):
        turned = pltpu.roll(tile, 64, 1)
        return jnp.where(low, tile, turned), jnp.where(low, turned, tile)

    def stage_hidden(g, k_step, q_step):
        for pair in range(heads // 2):
            cols = slice(128 * pair, 128 * pair + 128)
            keys = both_halves(k_ref[g, k_step, :, cols])
            queries = both_halves(q_ref[g, q_step, :, cols])
            values = both_halves(v_ref[g, k_step, :, cols])
            for side in range(2):
                h = 2 * pair + side
                key_dup[g, h] = keys[side]
                query_dup[g, h] = queries[side]
                value_dup[g, h] = values[side]
                kp = split3(keys[side])
                qp = split3(queries[side])
                key_t[g, h] = rows(jnp.where(low, kp[0], one), jnp.where(low, kp[1], zero), jnp.where(low, kp[2], zero))
                lhs = rows(kp[0], qp[0], kp[1], qp[1], kp[2], qp[2])
                z_one = sum3(dot_nn(lanes(lhs, lhs), rows(w1_parts[g, h], pad64)), 32) + rep8(b1[g, h], 32)
                hidden, slope_val = gelu_and_slope(z_one, 16)
                slope[g, h] = slope_val
                act[g, h] = rows(*split3(hidden))

    def stage_norm(g, q_step):
        outs = []
        for h in range(heads):
            raw = sum3(dot_nt(act[g, h], rows(w2_parts[g, h], pad64)), 32)
            folded = raw[:, :128] + raw[:, 128:]
            z_two = folded + pltpu.roll(folded, 64, 1) + rep8(b2[g, h], 32)
            centered = z_two - jnp.sum(z_two, 1, keepdims=True) * (1 / 128)
            inv_std = lax.rsqrt(jnp.sum(centered * centered, 1, keepdims=True) * (1 / 128) + LN_EPS)
            normed = centered * inv_std
            gain_h = gain[h]
            out = rows(key_dup[g, h], query_dup[g, h]) + (normed * rep8(gain_h, 32) + rep8(bias[h], 32))
            outs.append(out[16:])
            d_norm = (2.0 * (out[:16] - value_dup[g, h])) * rep8(gain_h, 16)
            normed_k = normed[:16]
            mean_d = jnp.sum(d_norm, 1, keepdims=True) * (1 / 128)
            mean_dn = jnp.sum(d_norm * normed_k, 1, keepdims=True) * (1 / 128)
            d_val = inv_std[:16] * (d_norm - mean_d - normed_k * mean_dn)
            d_two[g, h] = rows(*split3(d_val))
            total = d_val[:8] + d_val[8:]
            for shift in (4, 2, 1):
                total = total + pltpu.roll(total, shift, 0)
            b2[g, h] = b2[g, h] - rate[h] * total
        for pair in range(heads // 2):
            o_ref[g, q_step, :, 128 * pair:128 * pair + 128] = jnp.where(low, outs[2 * pair], outs[2 * pair + 1]).astype(bf16)

    def stage_second(g):
        for h in range(heads):
            dp = d_two[g, h]
            d_hidden = sum3(dot_nn(lanes(dp, dp), rows(w2_parts[g, h], pad64)), 16)
            d_one[g, h] = rows(*split3(d_hidden * slope[g, h]))
            lhs = rows(dp[:16], dp[:16], dp[:16], dp[16:32], dp[16:32], dp[32:])[:, :64]
            acts = act[g, h]
            high, mid, low_part = acts[0:16], acts[32:48], acts[64:80]
            grad = dot_tn(lhs, rows(high, mid, low_part, high, mid, high))
            new = w2[g, h] - rate[h] * grad
            w2[g, h] = new
            w2_parts[g, h] = rows(*split3(new))

    def stage_first(g):
        for h in range(heads):
            kt = key_t[g, h]
            dp = d_one[g, h]
            lhs = rows(kt[:16], kt[:16], kt[:16], kt[16:32], kt[16:32], kt[32:])[:, :80]
            grad = dot_tn(lhs, rows(dp, dp[0:32], dp[0:16]))
            new = w1[g, h] - rate[h] * grad[:64]
            w1[g, h] = new
            w1_parts[g, h] = rows(*split3(new))
            b1[g, h] = b1[g, h] - rate[h] * grad[64:72]

    def body(step, first=False, last=False):
        for turn in range(groups):
            for stage in range(4):
                before = turn < stage
                g = (turn - stage) % groups
                if (first and before) or (last and not before and stage >= 2):
                    continue
                at = step - 1 if before else step
                q_step = jnp.maximum(at - 1, 0)
                if stage == 0:
                    stage_hidden(g, jnp.minimum(at, steps - 1), q_step)
                elif stage == 1:
                    stage_norm(g, q_step)
                elif stage == 2:
                    stage_second(g)
                else:
                    stage_first(g)

    body(jnp.int32(0), first=True)

    def loop_body(step, carry):
        body(step)
        return carry

    lax.fori_loop(1, steps, loop_body, 0)
    body(jnp.int32(steps), last=True)
    stage_norm(groups - 1, steps - 1)


def run_inner(keys, queries, values, w1, w2t, b1, b2, gain, bias, rate):
    groups, steps = keys.shape[:2]
    heads = w1.shape[0]
    vmem = pl.BlockSpec(memory_space=pltpu.VMEM)
    smem = pl.BlockSpec(memory_space=pltpu.SMEM)
    per_pair = (groups, heads)
    scratch = [((64, 256), f32), ((64, 256), f32), ((192, 256), bf16), ((192, 256), bf16), ((8, 256), f32), ((8, 128), f32),
               ((96, 256), bf16), ((16, 256), f32), ((48, 128), bf16), ((48, 256), bf16), ((48, 128), bf16),
               ((16, 128), f32), ((16, 128), f32), ((16, 128), f32)]
    return pl.pallas_call(
        functools.partial(inner_kernel, steps, groups, heads),
        out_shape=jax.ShapeDtypeStruct(keys.shape, bf16),
        in_specs=[vmem] * 9 + [smem],
        out_specs=vmem,
        scratch_shapes=[pltpu.VMEM(per_pair + shape, dtype) for shape, dtype in scratch],
        compiler_params=pltpu.CompilerParams(vmem_limit_bytes=60 * 2 ** 20),
    )(keys, queries, values, w1, w2t, b1, b2, gain, bias, rate)


def solution(mesh):
    def local_fn(tokens, theta_q, theta_k, theta_v, w_out, w_one, b_one, w_two, b_two, ln_gain, ln_bias, inner_lr):
        tok_local, model_dim = tokens.shape[1:]
        heads = w_one.shape[0]
        seqs = lax.all_to_all(tokens, 'seq', 0, 1, tiled=True)
        num_seqs, seq_len = seqs.shape[:2]
        steps = seq_len // MINI_BATCH

        def project(weight):
            out = jnp.dot(seqs.reshape(num_seqs * seq_len, model_dim), weight, preferred_element_type=f32)
            return out.reshape(num_seqs, steps, MINI_BATCH, weight.shape[1])

        def eight(vec, twice):
            vec = jnp.concatenate([vec, vec], -1) if twice else vec
            return jnp.broadcast_to(vec[:, None, :], (heads, 8, vec.shape[-1]))

        outs = run_inner(project(theta_k), project(theta_q), project(theta_v), w_one, jnp.swapaxes(w_two, 1, 2), eight(b_one, False),
                         eight(b_two, True), eight(ln_gain, True), eight(ln_bias, True), inner_lr / MINI_BATCH)
        outs = outs.reshape(num_seqs, seq_len, outs.shape[-1])
        outs = lax.all_to_all(outs, 'seq', 1, 0, tiled=True)
        outs = lax.all_gather(outs, 'heads', axis=2, tiled=True)
        w_full = lax.all_gather(w_out, 'heads', axis=0, tiled=True)
        return jnp.einsum('bte,ed->btd', outs, w_full, preferred_element_type=f32).astype(bf16)

    arg_specs = (P('data', 'seq', None), P(None, 'heads'), P(None, 'heads'), P(None, 'heads'), P('heads', None), P('heads', None, None), P('heads', None), P('heads', None, None), P('heads', None), P('heads', None), P('heads', None), P('heads'))
    return jax.shard_map(local_fn, mesh=mesh, in_specs=arg_specs, out_specs=P('data', 'seq', None), check_vma=False)
```

```python
import functools

import jax
import jax.numpy as jnp
from jax import lax
from jax.experimental import pallas as pl
from jax.experimental.pallas import tpu as pltpu
from jax.sharding import PartitionSpec as P

MINI_BATCH = 16
LN_EPS = 1e-6
GELU_C0 = 0.7978845608028654
GELU_C1 = 0.044715
f32 = jnp.float32
bf16 = jnp.bfloat16


def split3(val):
    high = val.astype(bf16)
    rest = val - high.astype(f32)
    mid = rest.astype(bf16)
    return high, mid, (rest - mid.astype(f32)).astype(bf16)


def dot_nn(lhs, rhs):
    return lax.dot_general(lhs, rhs, (((1,), (0,)), ((), ())), preferred_element_type=f32)


def dot_nt(lhs, rhs):
    return lax.dot_general(lhs, rhs, (((1,), (1,)), ((), ())), preferred_element_type=f32)


def dot_tn(lhs, rhs):
    return lax.dot_general(lhs, rhs, (((0,), (0,)), ((), ())), preferred_element_type=f32)


def rows(*parts):
    return jnp.concatenate(parts, 0)


def lanes(*parts):
    return jnp.concatenate(parts, 1)


def rep8(val, count):
    return rows(*([val] * (count // 8)))


def sum3(val, count):
    return val[0:count] + val[count:2 * count] + val[2 * count:3 * count]


def gelu_and_slope(z_val, key_rows):
    square = z_val * z_val
    tanh_val = jnp.tanh(z_val * (GELU_C0 + (GELU_C0 * GELU_C1) * square))
    half = 0.5 * z_val
    act = half + half * tanh_val
    tanh_key = tanh_val[:key_rows]
    slope = (0.5 + 0.5 * tanh_key) + half[:key_rows] * (1.0 - tanh_key * tanh_key) * (GELU_C0 + (3 * GELU_C0 * GELU_C1) * square[:key_rows])
    return act, slope


def inner_kernel(steps, groups, heads, k_ref, q_ref, v_ref, w1_in, w2_in, b1_in, b2_in, gain, bias, rate, w_mine, o_ref, w_other,
                 w1, w2, w1_parts, w2_parts, b1, b2, act, slope, d_two, d_one, key_t, key_dup, query_dup, value_dup, send_sem, recv_sem):
    peer = {'heads': 1 - lax.axis_index('heads')}
    barrier = pltpu.get_barrier_semaphore()
    pl.semaphore_signal(barrier, inc=1, device_id=peer, device_id_type=pl.DeviceIdType.MESH)
    pl.semaphore_wait(barrier, 1)
    swap = pltpu.make_async_remote_copy(w_mine, w_other, send_sem, recv_sem, device_id=peer, device_id_type=pl.DeviceIdType.MESH)
    swap.start()
    low = lax.broadcasted_iota(jnp.int32, (16, 128), 1) < 64
    pad64 = jnp.zeros((64, 256), bf16)
    one = jnp.ones((16, 128), bf16)
    zero = jnp.zeros((16, 128), bf16)

    @pl.loop(0, groups)
    def _(g):
        for h in range(heads):
            first, second = w1_in[h], w2_in[h]
            w1[g, h] = first
            w2[g, h] = second
            w1_parts[g, h] = rows(*split3(first))
            w2_parts[g, h] = rows(*split3(second))
            b1[g, h] = b1_in[h]
            b2[g, h] = b2_in[h]

    def both_halves(tile):
        turned = pltpu.roll(tile, 64, 1)
        return jnp.where(low, tile, turned), jnp.where(low, turned, tile)

    def stage_hidden(g, k_step, q_step):
        for pair in range(heads // 2):
            cols = slice(128 * pair, 128 * pair + 128)
            keys = both_halves(k_ref[g, k_step, :, cols])
            queries = both_halves(q_ref[g, q_step, :, cols])
            values = both_halves(v_ref[g, k_step, :, cols])
            for side in range(2):
                h = 2 * pair + side
                key_dup[g, h] = keys[side]
                query_dup[g, h] = queries[side]
                value_dup[g, h] = values[side]
                kp = split3(keys[side])
                qp = split3(queries[side])
                key_t[g, h] = rows(jnp.where(low, kp[0], one), jnp.where(low, kp[1], zero), jnp.where(low, kp[2], zero))
                lhs = rows(kp[0], qp[0], kp[1], qp[1], kp[2], qp[2])
                z_one = sum3(dot_nn(lanes(lhs, lhs), rows(w1_parts[g, h], pad64)), 32) + rep8(b1[g, h], 32)
                hidden, slope_val = gelu_and_slope(z_one, 16)
                slope[g, h] = slope_val
                act[g, h] = rows(*split3(hidden))

    def stage_norm(g, q_step):
        outs = []
        for h in range(heads):
            raw = sum3(dot_nt(act[g, h], rows(w2_parts[g, h], pad64)), 32)
            folded = raw[:, :128] + raw[:, 128:]
            z_two = folded + pltpu.roll(folded, 64, 1) + rep8(b2[g, h], 32)
            centered = z_two - jnp.sum(z_two, 1, keepdims=True) * (1 / 128)
            inv_std = lax.rsqrt(jnp.sum(centered * centered, 1, keepdims=True) * (1 / 128) + LN_EPS)
            normed = centered * inv_std
            gain_h = gain[h]
            out = rows(key_dup[g, h], query_dup[g, h]) + (normed * rep8(gain_h, 32) + rep8(bias[h], 32))
            outs.append(out[16:])
            d_norm = (2.0 * (out[:16] - value_dup[g, h])) * rep8(gain_h, 16)
            normed_k = normed[:16]
            mean_d = jnp.sum(d_norm, 1, keepdims=True) * (1 / 128)
            mean_dn = jnp.sum(d_norm * normed_k, 1, keepdims=True) * (1 / 128)
            d_val = inv_std[:16] * (d_norm - mean_d - normed_k * mean_dn)
            d_two[g, h] = rows(*split3(d_val))
            total = d_val[:8] + d_val[8:]
            for shift in (4, 2, 1):
                total = total + pltpu.roll(total, shift, 0)
            b2[g, h] = b2[g, h] - rate[h] * total
        for pair in range(heads // 2):
            o_ref[g, q_step, :, 128 * pair:128 * pair + 128] = jnp.where(low, outs[2 * pair], outs[2 * pair + 1]).astype(bf16)

    def stage_second(g):
        for h in range(heads):
            dp = d_two[g, h]
            d_hidden = sum3(dot_nn(lanes(dp, dp), rows(w2_parts[g, h], pad64)), 16)
            d_one[g, h] = rows(*split3(d_hidden * slope[g, h]))
            lhs = rows(dp[:16], dp[:16], dp[:16], dp[16:32], dp[16:32], dp[32:])[:, :64]
            acts = act[g, h]
            high, mid, low_part = acts[0:16], acts[32:48], acts[64:80]
            grad = dot_tn(lhs, rows(high, mid, low_part, high, mid, high))
            new = w2[g, h] - rate[h] * grad
            w2[g, h] = new
            w2_parts[g, h] = rows(*split3(new))

    def stage_first(g):
        for h in range(heads):
            kt = key_t[g, h]
            dp = d_one[g, h]
            lhs = rows(kt[:16], kt[:16], kt[:16], kt[16:32], kt[16:32], kt[32:])[:, :80]
            grad = dot_tn(lhs, rows(dp, dp[0:32], dp[0:16]))
            new = w1[g, h] - rate[h] * grad[:64]
            w1[g, h] = new
            w1_parts[g, h] = rows(*split3(new))
            b1[g, h] = b1[g, h] - rate[h] * grad[64:72]

    def body(step, first=False, last=False):
        for turn in range(groups):
            for stage in range(4):
                before = turn < stage
                g = (turn - stage) % groups
                if (first and before) or (last and not before and stage >= 2):
                    continue
                at = step - 1 if before else step
                q_step = jnp.maximum(at - 1, 0)
                if stage == 0:
                    stage_hidden(g, jnp.minimum(at, steps - 1), q_step)
                elif stage == 1:
                    stage_norm(g, q_step)
                elif stage == 2:
                    stage_second(g)
                else:
                    stage_first(g)

    body(jnp.int32(0), first=True)

    def loop_body(step, carry):
        body(step)
        return carry

    lax.fori_loop(1, steps, loop_body, 0)
    body(jnp.int32(steps), last=True)
    stage_norm(groups - 1, steps - 1)
    swap.wait()


def run_inner(keys, queries, values, w1, w2t, b1, b2, gain, bias, rate, w_out):
    groups, steps = keys.shape[:2]
    heads = w1.shape[0]
    vmem = pl.BlockSpec(memory_space=pltpu.VMEM)
    hbm = pl.BlockSpec(memory_space=pl.ANY)
    smem = pl.BlockSpec(memory_space=pltpu.SMEM)
    per_pair = (groups, heads)
    scratch = [((64, 256), f32), ((64, 256), f32), ((192, 256), bf16), ((192, 256), bf16), ((8, 256), f32), ((8, 128), f32),
               ((96, 256), bf16), ((16, 256), f32), ((48, 128), bf16), ((48, 256), bf16), ((48, 128), bf16),
               ((16, 128), f32), ((16, 128), f32), ((16, 128), f32)]
    return pl.pallas_call(
        functools.partial(inner_kernel, steps, groups, heads),
        out_shape=(jax.ShapeDtypeStruct(keys.shape, bf16), jax.ShapeDtypeStruct(w_out.shape, bf16)),
        in_specs=[vmem] * 9 + [smem, hbm],
        out_specs=(vmem, hbm),
        scratch_shapes=[pltpu.VMEM(per_pair + shape, dtype) for shape, dtype in scratch] + [pltpu.SemaphoreType.DMA] * 2,
        compiler_params=pltpu.CompilerParams(vmem_limit_bytes=60 * 2 ** 20, collective_id=0, has_side_effects=True),
    )(keys, queries, values, w1, w2t, b1, b2, gain, bias, rate, w_out)


def solution(mesh):
    def local_fn(tokens, theta_q, theta_k, theta_v, w_out, w_one, b_one, w_two, b_two, ln_gain, ln_bias, inner_lr):
        tok_local, model_dim = tokens.shape[1:]
        heads = w_one.shape[0]
        seqs = lax.all_to_all(tokens, 'seq', 0, 1, tiled=True)
        num_seqs, seq_len = seqs.shape[:2]
        steps = seq_len // MINI_BATCH

        def project(weight):
            out = jnp.dot(seqs.reshape(num_seqs * seq_len, model_dim), weight, preferred_element_type=f32)
            return out.reshape(num_seqs, steps, MINI_BATCH, weight.shape[1])

        def eight(vec, twice):
            vec = jnp.concatenate([vec, vec], -1) if twice else vec
            return jnp.broadcast_to(vec[:, None, :], (heads, 8, vec.shape[-1]))

        outs, w_other = run_inner(project(theta_k), project(theta_q), project(theta_v), w_one, jnp.swapaxes(w_two, 1, 2), eight(b_one, False),
                         eight(b_two, True), eight(ln_gain, True), eight(ln_bias, True), inner_lr / MINI_BATCH, w_out)
        outs = outs.reshape(num_seqs, seq_len, outs.shape[-1])
        outs = lax.all_to_all(outs, 'seq', 1, 0, tiled=True)
        outs = lax.all_gather(outs, 'heads', axis=2, tiled=True)
        first = lax.axis_index('heads') == 0
        w_full = jnp.concatenate([jnp.where(first, w_out, w_other), jnp.where(first, w_other, w_out)], 0)
        return jnp.einsum('bte,ed->btd', outs, w_full, preferred_element_type=f32).astype(bf16)

    arg_specs = (P('data', 'seq', None), P(None, 'heads'), P(None, 'heads'), P(None, 'heads'), P('heads', None), P('heads', None, None), P('heads', None), P('heads', None, None), P('heads', None), P('heads', None), P('heads', None), P('heads'))
    return jax.shard_map(local_fn, mesh=mesh, in_specs=arg_specs, out_specs=P('data', 'seq', None), check_vma=False)
```

```python
import functools

import jax
import jax.numpy as jnp
from jax import lax
from jax.experimental import pallas as pl
from jax.experimental.pallas import tpu as pltpu
from jax.sharding import PartitionSpec as P

MINI_BATCH = 16
LN_EPS = 1e-6
GELU_C0 = 0.7978845608028654
GELU_C1 = 0.044715
f32 = jnp.float32
bf16 = jnp.bfloat16


def split3(val):
    high = val.astype(bf16)
    rest = val - high.astype(f32)
    mid = rest.astype(bf16)
    return high, mid, (rest - mid.astype(f32)).astype(bf16)


def dot_nn(lhs, rhs):
    return lax.dot_general(lhs, rhs, (((1,), (0,)), ((), ())), preferred_element_type=f32)


def dot_nt(lhs, rhs):
    return lax.dot_general(lhs, rhs, (((1,), (1,)), ((), ())), preferred_element_type=f32)


def dot_tn(lhs, rhs):
    return lax.dot_general(lhs, rhs, (((0,), (0,)), ((), ())), preferred_element_type=f32)


def rows(*parts):
    return jnp.concatenate(parts, 0)


def lanes(*parts):
    return jnp.concatenate(parts, 1)


def rep8(val, count):
    return rows(*([val] * (count // 8)))


def sum3(val, count):
    return val[0:count] + val[count:2 * count] + val[2 * count:3 * count]


def gelu_and_slope(z_val, key_rows):
    square = z_val * z_val
    tanh_val = jnp.tanh(z_val * (GELU_C0 + (GELU_C0 * GELU_C1) * square))
    half = 0.5 * z_val
    act = half + half * tanh_val
    tanh_key = tanh_val[:key_rows]
    slope = (0.5 + 0.5 * tanh_key) + half[:key_rows] * (1.0 - tanh_key * tanh_key) * (GELU_C0 + (3 * GELU_C0 * GELU_C1) * square[:key_rows])
    return act, slope


def eight_rows(row, twice):
    row = lanes(row, row) if twice else row
    return jnp.broadcast_to(row, (8, row.shape[1]))


def layer_kernel(steps, groups, heads, parts_of_seq, tokens, theta_k, theta_q, theta_v, w_out, w1_in, w2_in, b1_in, b2_in, gain_in, bias_in, rate_in,
                 o_full, w_full,
                 w1, w2, w1_parts, w2_parts, b1, b2, act, slope, d_two, d_one, key_t, key_dup, query_dup, value_dup, gain, bias,
                 tok, outs, k_now, v_now, q_now, q_next, k_new, v_new, q_new,
                 tok_send, tok_recv, out_send, out_recv, own_sem, w_send, w_recv, w_own):
    low = lax.broadcasted_iota(jnp.int32, (16, 128), 1) < 64
    pad64 = jnp.zeros((64, 256), bf16)
    one = jnp.ones((16, 128), bf16)
    zero = jnp.zeros((16, 128), bf16)
    width = 64 * heads
    own_steps = steps // parts_of_seq
    row_axis = lax.axis_index('heads')
    me = lax.axis_index('seq')
    other_row = 1 - row_axis
    my_cols = pl.ds(pl.multiple_of(row_axis * width, width), width)
    mesh_ids = pl.DeviceIdType.MESH

    def other_core(place):
        return place + 1 - 2 * lax.rem(place, 2)

    near = other_core(me)
    far_a = lax.rem(me + 2, 4)
    far_b = other_core(far_a)

    barrier = pltpu.get_barrier_semaphore()
    for shift_row in range(2):
        for shift in range(parts_of_seq):
            if shift_row or shift:
                pl.semaphore_signal(barrier, inc=1, device_id={'heads': lax.rem(row_axis + shift_row, 2), 'seq': lax.rem(me + shift, parts_of_seq)}, device_id_type=mesh_ids)
    pl.semaphore_wait(barrier, 2 * parts_of_seq - 1)

    def token_copy(slot, dest, chunk):
        at = me * own_steps + chunk
        return pltpu.make_async_remote_copy(tokens.at[pl.ds(groups * dest, groups), pl.ds(MINI_BATCH * chunk, MINI_BATCH)], tok.at[:, at],
                                            tok_send.at[slot, chunk], tok_recv.at[at], device_id={'seq': dest}, device_id_type=mesh_ids)

    def own_tokens(chunk):
        at = me * own_steps + chunk
        return pltpu.make_async_copy(tokens.at[pl.ds(groups * me, groups), pl.ds(MINI_BATCH * chunk, MINI_BATCH)], tok.at[:, at], tok_recv.at[at])

    def send_far():
        @pl.loop(0, own_steps)
        def _(chunk):
            token_copy(1, far_a, chunk).start()
            token_copy(2, far_b, chunk).start()

    @pl.when(lax.rem(me, 2) == 0)
    def _():
        send_far()

    @pl.loop(0, own_steps)
    def _(chunk):
        own_tokens(chunk).start()
        token_copy(0, near, chunk).start()

    def wait_tokens(step):
        pltpu.make_async_remote_copy(tokens.at[pl.ds(0, groups), pl.ds(0, MINI_BATCH)], tok.at[:, step], tok_send.at[0, 0], tok_recv.at[step],
                                     device_id={'seq': near}, device_id_type=mesh_ids).wait_recv()

    my_w_rows = w_full.at[pl.ds(pl.multiple_of(row_axis * width, width), width)]
    w_swap = pltpu.make_async_remote_copy(w_out, my_w_rows, w_send, w_recv, device_id={'heads': other_row}, device_id_type=mesh_ids)
    w_keep = pltpu.make_async_copy(w_out, my_w_rows, w_own)
    w_swap.start()
    w_keep.start()

    def out_target(step, place):
        return o_full.at[pl.ds(groups * place, groups), pl.ds(MINI_BATCH * lax.rem(step, own_steps), MINI_BATCH), my_cols]

    def send_out(step):
        owner = step // own_steps
        across = pltpu.make_async_remote_copy(outs.at[:, step], out_target(step, me), out_send.at[1], out_recv.at[row_axis, me],
                                              device_id={'heads': other_row, 'seq': owner}, device_id_type=mesh_ids)
        across.start()

        @pl.when(owner != me)
        def _():
            pltpu.make_async_remote_copy(outs.at[:, step], out_target(step, me), out_send.at[0], out_recv.at[row_axis, me],
                                         device_id={'seq': owner}, device_id_type=mesh_ids).start()

        @pl.when(owner == me)
        def _():
            pltpu.make_async_copy(outs.at[:, step], out_target(step, me), own_sem).start()

    for h in range(heads):
        b1[0, h] = eight_rows(b1_in[h:h + 1], False)
        b2[0, h] = eight_rows(b2_in[h:h + 1], True)
        gain[h] = eight_rows(gain_in[h:h + 1], True)
        bias[h] = eight_rows(bias_in[h:h + 1], True)
        first, second = rows(*split3(w1_in[h])), rows(*split3(w2_in[h]))
        for g in range(groups):
            w1[g, h] = w1_in[h]
            w2[g, h] = w2_in[h]
            w1_parts[g, h] = first
            w2_parts[g, h] = second
            if g:
                b1[g, h] = b1[0, h]
                b2[g, h] = b2[0, h]
    q_next[...] = jnp.zeros(q_next.shape, f32)
    rate = [rate_in[h] * (1 / MINI_BATCH) for h in range(heads)]

    def project(step):
        toks = tok[:, step].reshape(groups * MINI_BATCH, tok.shape[3])
        for theta, target in ((theta_k, k_new), (theta_q, q_new), (theta_v, v_new)):
            for col in range(0, width, 256):
                target[:, :, col:col + 256] = dot_nn(toks, theta[:, col:col + 256]).reshape(groups, MINI_BATCH, 256)

    def shift_in():
        q_now[...] = q_next[...]
        q_next[...] = q_new[...]
        k_now[...] = k_new[...]
        v_now[...] = v_new[...]

    def both_halves(tile):
        turned = pltpu.roll(tile, 64, 1)
        return jnp.where(low, tile, turned), jnp.where(low, turned, tile)

    def stage_hidden(g):
        for pair in range(heads // 2):
            cols = slice(128 * pair, 128 * pair + 128)
            keys = both_halves(k_now[g, :, cols])
            queries = both_halves(q_now[g, :, cols])
            values = both_halves(v_now[g, :, cols])
            for side in range(2):
                h = 2 * pair + side
                key_dup[g, h] = keys[side]
                query_dup[g, h] = queries[side]
                value_dup[g, h] = values[side]
                kp = split3(keys[side])
                qp = split3(queries[side])
                key_t[g, h] = rows(jnp.where(low, kp[0], one), jnp.where(low, kp[1], zero), jnp.where(low, kp[2], zero))
                lhs = rows(kp[0], qp[0], kp[1], qp[1], kp[2], qp[2])
                z_one = sum3(dot_nn(lanes(lhs, lhs), rows(w1_parts[g, h], pad64)), 32) + rep8(b1[g, h], 32)
                hidden, slope_val = gelu_and_slope(z_one, 16)
                slope[g, h] = slope_val
                act[g, h] = rows(*split3(hidden))

    def stage_norm(g, q_step):
        vals = []
        for h in range(heads):
            raw = sum3(dot_nt(act[g, h], rows(w2_parts[g, h], pad64)), 32)
            folded = raw[:, :128] + raw[:, 128:]
            z_two = folded + pltpu.roll(folded, 64, 1) + rep8(b2[g, h], 32)
            centered = z_two - jnp.sum(z_two, 1, keepdims=True) * (1 / 128)
            inv_std = lax.rsqrt(jnp.sum(centered * centered, 1, keepdims=True) * (1 / 128) + LN_EPS)
            normed = centered * inv_std
            gain_h = gain[h]
            out = rows(key_dup[g, h], query_dup[g, h]) + (normed * rep8(gain_h, 32) + rep8(bias[h], 32))
            vals.append(out[16:])
            d_norm = (2.0 * (out[:16] - value_dup[g, h])) * rep8(gain_h, 16)
            normed_k = normed[:16]
            mean_d = jnp.sum(d_norm, 1, keepdims=True) * (1 / 128)
            mean_dn = jnp.sum(d_norm * normed_k, 1, keepdims=True) * (1 / 128)
            d_val = inv_std[:16] * (d_norm - mean_d - normed_k * mean_dn)
            d_two[g, h] = rows(*split3(d_val))
            total = d_val[:8] + d_val[8:]
            for shift in (4, 2, 1):
                total = total + pltpu.roll(total, shift, 0)
            b2[g, h] = b2[g, h] - rate[h] * total
        for pair in range(heads // 2):
            outs[g, q_step, :, 128 * pair:128 * pair + 128] = jnp.where(low, vals[2 * pair], vals[2 * pair + 1]).astype(bf16)

    def stage_second(g):
        for h in range(heads):
            dp = d_two[g, h]
            d_hidden = sum3(dot_nn(lanes(dp, dp), rows(w2_parts[g, h], pad64)), 16)
            d_one[g, h] = rows(*split3(d_hidden * slope[g, h]))
            lhs = rows(dp[:16], dp[:16], dp[:16], dp[16:32], dp[16:32], dp[32:])[:, :64]
            acts = act[g, h]
            high, mid, low_part = acts[0:16], acts[32:48], acts[64:80]
            grad = dot_tn(lhs, rows(high, mid, low_part, high, mid, high))
            new = w2[g, h] - rate[h] * grad
            w2[g, h] = new
            w2_parts[g, h] = rows(*split3(new))

    def stage_first(g):
        for h in range(heads):
            kt = key_t[g, h]
            dp = d_one[g, h]
            lhs = rows(kt[:16], kt[:16], kt[:16], kt[16:32], kt[16:32], kt[32:])[:, :80]
            grad = dot_tn(lhs, rows(dp, dp[0:32], dp[0:16]))
            new = w1[g, h] - rate[h] * grad[:64]
            w1[g, h] = new
            w1_parts[g, h] = rows(*split3(new))
            b1[g, h] = b1[g, h] - rate[h] * grad[64:72]

    def body(step, first=False, last=False):
        shift_in()
        if not last:
            project(jnp.minimum(step + 1, steps - 1))
        for turn in range(groups):
            for stage in range(4):
                before = turn < stage
                g = (turn - stage) % groups
                if (first and before) or (last and not before and stage >= 2):
                    continue
                at = step - 1 if before else step
                if stage == 0:
                    stage_hidden(g)
                elif stage == 1:
                    stage_norm(g, jnp.maximum(at - 1, 0))
                elif stage == 2:
                    stage_second(g)
                else:
                    stage_first(g)

    wait_tokens(0)
    project(0)
    wait_tokens(1)
    body(jnp.int32(0), first=True)

    def loop_body(step, carry):
        @pl.when(step < steps - 1)
        def _():
            wait_tokens(step + 1)

        @pl.when((step == 7) & (lax.rem(me, 2) == 1))
        def _():
            send_far()

        @pl.when(step >= 3)
        def _():
            send_out(step - 3)

        body(step)
        return carry

    lax.fori_loop(1, steps, loop_body, 0)
    send_out(jnp.int32(steps - 3))
    body(jnp.int32(steps), last=True)
    send_out(jnp.int32(steps - 2))
    stage_norm(groups - 1, steps - 1)
    w_keep.wait()
    w_swap.wait()

    @pl.loop(0, own_steps)
    def _(chunk):
        token_copy(0, near, chunk).wait_send()
        token_copy(1, far_a, chunk).wait_send()
        token_copy(2, far_b, chunk).wait_send()

    send_out(jnp.int32(steps - 1))

    def out_wait(src, dst, send, recv):
        return pltpu.make_async_remote_copy(src, dst, send, recv, device_id={'heads': other_row}, device_id_type=mesh_ids)

    def landed(row_at, place):
        return o_full.at[pl.ds(groups * place, groups), :, pl.ds(width * row_at, width)]

    away = steps - own_steps
    whole = outs.at[:, pl.ds(0, away)]
    out_wait(whole, whole, out_send.at[0], out_recv.at[0, 0]).wait_send()
    out_wait(outs, outs, out_send.at[1], out_recv.at[0, 0]).wait_send()
    for row_at in range(2):
        for place in range(parts_of_seq):
            spot = landed(row_at, place)
            mine = (row_axis == row_at) & (me == place)

            @pl.when(mine)
            def _():
                pltpu.make_async_copy(spot, spot, own_sem).wait()

            @pl.when(jnp.logical_not(mine))
            def _():
                out_wait(spot, spot, out_send.at[0], out_recv.at[row_at, place]).wait_recv()


def run_layer(tokens, theta_k, theta_q, theta_v, w_out, w1, w2t, b1, b2, gain, bias, rate, parts_of_seq):
    num_seqs, own_len, model_dim = tokens.shape
    groups = num_seqs // parts_of_seq
    steps = own_len * parts_of_seq // MINI_BATCH
    heads = w1.shape[0]
    width = theta_k.shape[1]
    vmem = pl.BlockSpec(memory_space=pltpu.VMEM)
    smem = pl.BlockSpec(memory_space=pltpu.SMEM)
    hbm = pl.BlockSpec(memory_space=pl.ANY)
    per_pair = (groups, heads)
    scratch = [((64, 256), f32), ((64, 256), f32), ((192, 256), bf16), ((192, 256), bf16), ((8, 256), f32), ((8, 128), f32),
               ((96, 256), bf16), ((16, 256), f32), ((48, 128), bf16), ((48, 256), bf16), ((48, 128), bf16),
               ((16, 128), f32), ((16, 128), f32), ((16, 128), f32)]
    scratch = [pltpu.VMEM(per_pair + shape, dtype) for shape, dtype in scratch]
    scratch += [pltpu.VMEM((heads, 8, 128), f32)] * 2
    scratch += [pltpu.VMEM((groups, steps, MINI_BATCH, model_dim), bf16), pltpu.VMEM((groups, steps, MINI_BATCH, width), bf16)]
    scratch += [pltpu.VMEM((groups, MINI_BATCH, width), f32)] * 7
    own_steps = steps // parts_of_seq
    dma = pltpu.SemaphoreType.DMA
    scratch += [dma((3, own_steps)), dma((steps,)), dma((2,)), dma((2, parts_of_seq)), dma, dma, dma, dma]
    return pl.pallas_call(
        functools.partial(layer_kernel, steps, groups, heads, parts_of_seq),
        out_shape=(jax.ShapeDtypeStruct((num_seqs, own_len, 2 * width), bf16), jax.ShapeDtypeStruct((2 * width, model_dim), bf16)),
        in_specs=[hbm] + [vmem] * 3 + [hbm] + [vmem] * 6 + [smem],
        out_specs=(hbm, hbm),
        scratch_shapes=scratch,
        compiler_params=pltpu.CompilerParams(vmem_limit_bytes=60 * 2 ** 20, collective_id=0, has_side_effects=True),
    )(tokens, theta_k, theta_q, theta_v, w_out, w1, w2t, b1, b2, gain, bias, rate)


def solution(mesh):
    parts_of_seq = mesh.shape['seq']

    def local_fn(tokens, theta_q, theta_k, theta_v, w_out, w_one, b_one, w_two, b_two, ln_gain, ln_bias, inner_lr):
        outs, w_full = run_layer(tokens, theta_k, theta_q, theta_v, w_out, w_one, jnp.swapaxes(w_two, 1, 2), b_one, b_two, ln_gain, ln_bias, inner_lr, parts_of_seq)
        return jnp.einsum('bte,ed->btd', outs, w_full, preferred_element_type=f32).astype(bf16)

    arg_specs = (P('data', 'seq', None), P(None, 'heads'), P(None, 'heads'), P(None, 'heads'), P('heads', None), P('heads', None, None), P('heads', None), P('heads', None, None), P('heads', None), P('heads', None), P('heads', None), P('heads'))
    return jax.shard_map(local_fn, mesh=mesh, in_specs=arg_specs, out_specs=P('data', 'seq', None), check_vma=False)
```

```python
import functools

import jax
import jax.numpy as jnp
from jax import lax
from jax.experimental import pallas as pl
from jax.experimental.pallas import tpu as pltpu
from jax.sharding import PartitionSpec as P

MINI_BATCH = 16
AHEAD = 2
BATCH = 2
ORDER = 'CDGFAABEBAEABEGGGFFF'
PROJECT_EVERY = 2
PROJECT_FROM = 0
LN_EPS = 1e-6
GELU_C0 = 0.7978845608028654
GELU_C1 = 0.044715
f32 = jnp.float32
bf16 = jnp.bfloat16


def split3(val):
    high = val.astype(bf16)
    rest = val - high.astype(f32)
    mid = rest.astype(bf16)
    return high, mid, (rest - mid.astype(f32)).astype(bf16)


def dot_nn(lhs, rhs):
    return lax.dot_general(lhs, rhs, (((1,), (0,)), ((), ())), preferred_element_type=f32)


def dot_nt(lhs, rhs):
    return lax.dot_general(lhs, rhs, (((1,), (1,)), ((), ())), preferred_element_type=f32)


def dot_tn(lhs, rhs):
    return lax.dot_general(lhs, rhs, (((0,), (0,)), ((), ())), preferred_element_type=f32)


def rows(*parts):
    return jnp.concatenate(parts, 0)


def lanes(*parts):
    return jnp.concatenate(parts, 1)


def rep8(val, count):
    return rows(*([val] * (count // 8)))


def sum3(val, count):
    return val[0:count] + val[count:2 * count] + val[2 * count:3 * count]


def twice_gelu_and_slope(z_val):
    square = z_val * z_val
    tanh_val = jnp.tanh(z_val * (GELU_C0 + (GELU_C0 * GELU_C1) * square))
    plus = 1.0 + tanh_val
    slope = plus + (1.0 - tanh_val * tanh_val) * (z_val * (GELU_C0 + (3 * GELU_C0 * GELU_C1) * square))
    return z_val * plus, slope


def tile_parts(val, tile):
    return rows(*split3(val[:, 128 * tile:128 * tile + 128]))


def eight_rows(row, twice):
    row = lanes(row, row) if twice else row
    return jnp.broadcast_to(row, (8, row.shape[1]))


def layer_kernel(steps, seqs, heads, ahead, parts_of_seq, tokens, theta_k, theta_q, theta_v, w_out, w1_in, w2_in, b1_in, b2_in, gain_in, bias_in, rate_in,
                 o_full, w_full,
                 w1, w2, w1_parts, w2_parts, b1, act, slope, d_one, b2, key_parts, key_base, query_base, z_two, key_norm, key_inv, d_norm, d_two, gain_pair, bias_pair,
                 tok, outs, k_now, v_now, q_now, q_last, k_new, v_new, q_new,
                 tok_send, tok_recv, out_send, out_recv, own_sem, w_send, w_recv, w_own):
    low = lax.broadcasted_iota(jnp.int32, (16, 128), 1) < 64
    pad128 = jnp.zeros((128, 256), bf16)
    low_tall = lax.broadcasted_iota(jnp.int32, (32, 128), 1) < 64
    count_rows = jnp.where(lax.broadcasted_iota(jnp.int32, (16, 96), 1) < 48, 1.0, 0.0).astype(bf16)
    width = 64 * heads
    own_steps = steps // parts_of_seq
    row_axis = lax.axis_index('heads')
    me = lax.axis_index('seq')
    other_row = 1 - row_axis
    my_cols = pl.ds(pl.multiple_of(row_axis * width, width), width)
    mesh_ids = pl.DeviceIdType.MESH

    def other_core(place):
        return place + 1 - 2 * lax.rem(place, 2)

    near = other_core(me)
    far_a = lax.rem(me + 2, 4)
    far_b = other_core(far_a)

    barrier = pltpu.get_barrier_semaphore()
    for shift_row in range(2):
        for shift in range(parts_of_seq):
            if shift_row or shift:
                pl.semaphore_signal(barrier, inc=1, device_id={'heads': lax.rem(row_axis + shift_row, 2), 'seq': lax.rem(me + shift, parts_of_seq)}, device_id_type=mesh_ids)
    pl.semaphore_wait(barrier, 2 * parts_of_seq - 1)

    def token_copy(slot, dest, chunk):
        at = me * own_steps + chunk
        return pltpu.make_async_remote_copy(tokens.at[pl.ds(seqs * dest, seqs), pl.ds(MINI_BATCH * chunk, MINI_BATCH)], tok.at[:, at],
                                            tok_send.at[slot, chunk], tok_recv.at[at], device_id={'seq': dest}, device_id_type=mesh_ids)

    def own_tokens(chunk):
        at = me * own_steps + chunk
        return pltpu.make_async_copy(tokens.at[pl.ds(seqs * me, seqs), pl.ds(MINI_BATCH * chunk, MINI_BATCH)], tok.at[:, at], tok_recv.at[at])

    def send_far():
        @pl.loop(0, own_steps)
        def _(chunk):
            token_copy(1, far_a, chunk).start()
            token_copy(2, far_b, chunk).start()

    @pl.when(lax.rem(me, 2) == 0)
    def _():
        send_far()

    @pl.loop(0, own_steps)
    def _(chunk):
        own_tokens(chunk).start()
        token_copy(0, near, chunk).start()

    def wait_tokens(step):
        pltpu.make_async_remote_copy(tokens.at[pl.ds(0, seqs), pl.ds(0, MINI_BATCH)], tok.at[:, step], tok_send.at[0, 0], tok_recv.at[step],
                                     device_id={'seq': near}, device_id_type=mesh_ids).wait_recv()

    my_w_rows = w_full.at[pl.ds(pl.multiple_of(row_axis * width, width), width)]
    w_swap = pltpu.make_async_remote_copy(w_out, my_w_rows, w_send, w_recv, device_id={'heads': other_row}, device_id_type=mesh_ids)
    w_keep = pltpu.make_async_copy(w_out, my_w_rows, w_own)
    w_swap.start()
    w_keep.start()

    def out_target(step, place):
        return o_full.at[pl.ds(seqs * place, seqs), pl.ds(MINI_BATCH * lax.rem(step, own_steps), MINI_BATCH), my_cols]

    def send_out(step):
        owner = step // own_steps
        across = pltpu.make_async_remote_copy(outs.at[:, step], out_target(step, me), out_send.at[1], out_recv.at[row_axis, me],
                                              device_id={'heads': other_row, 'seq': owner}, device_id_type=mesh_ids)
        across.start()

        @pl.when(owner != me)
        def _():
            pltpu.make_async_remote_copy(outs.at[:, step], out_target(step, me), out_send.at[0], out_recv.at[row_axis, me],
                                         device_id={'seq': owner}, device_id_type=mesh_ids).start()

        @pl.when(owner == me)
        def _():
            pltpu.make_async_copy(outs.at[:, step], out_target(step, me), own_sem).start()

    for pair in range(heads // 2):
        even, odd = 2 * pair, 2 * pair + 1

        def pair_row(source, centered=False):
            sides = [source[even:even + 1], source[odd:odd + 1]]
            if centered:
                sides = [side - jnp.mean(side, 1, keepdims=True) for side in sides]
            return jnp.broadcast_to(lanes(*sides), (8, 128))

        gain_pair[pair] = pair_row(gain_in)
        bias_pair[pair] = pair_row(bias_in)
        offset = pair_row(b2_in, True)
        hidden_offset = rows(eight_rows(b1_in[even:even + 1], False), eight_rows(b1_in[odd:odd + 1], False))
        first = rows(w1_in[even], w1_in[odd])
        second = [0.5 * w2_in[even], 0.5 * w2_in[odd]]
        second = rows(*(side - jnp.mean(side, 0, keepdims=True) for side in second))
        for g in range(seqs):
            w1[g, pair] = first
            w2[g, pair] = second
            b1[g, pair] = hidden_offset
            b2[g, pair] = offset
        for tile in range(2):
            first_parts, second_parts = tile_parts(first, tile), tile_parts(second, tile)
            for g in range(seqs):
                w1_parts[g, pair, tile] = first_parts
                w2_parts[g, pair, tile] = second_parts
    q_last[...] = jnp.zeros(q_last.shape, f32)

    @pl.loop(0, seqs)
    def _(g):
        for ref in (act, slope, d_one, key_parts, key_base, query_base, z_two, key_norm, key_inv, d_norm, d_two):
            ref[g] = jnp.zeros(ref.shape[1:], ref.dtype)

    rate = [rate_in[h] * (1 / MINI_BATCH) for h in range(heads)]

    def both(unit):
        return [2 * pair + side for pair in unit for side in range(2)]

    def project(step):
        for theta, target in ((theta_k, k_new), (theta_q, q_new), (theta_v, v_new)):
            for col in range(0, width, 256):
                toks = tok[:, pl.ds(step, ahead)].reshape(seqs * ahead * MINI_BATCH, tok.shape[3])
                found = dot_nn(toks, theta[:, col:col + 256]).reshape(seqs, ahead, MINI_BATCH, 256)
                for j in range(ahead):
                    target[j, :, :, col:col + 256] = found[:, j]
                yield

    def shift_in():
        k_now[...] = k_new[...]
        v_now[...] = v_new[...]
        q_now[0] = q_last[...]
        for j in range(1, ahead):
            q_now[j] = q_new[j - 1]
        q_last[...] = q_new[ahead - 1]

    def states(ref, g, pair, first, last):
        return lanes(ref[g, pair, 0, first:last], ref[g, pair, 1, first:last])

    def by_side(val):
        keep = lax.broadcasted_iota(jnp.int32, val.shape, 1) < 64
        zero = jnp.zeros(val.shape, val.dtype)
        return [jnp.where(keep, val, zero), jnp.where(keep, zero, val)]

    def side_sums(val):
        keep = low if val.shape[0] == 16 else low_tall
        return jnp.where(keep, jnp.sum(jnp.where(keep, val, 0.0), 1, keepdims=True), jnp.sum(jnp.where(keep, 0.0, val), 1, keepdims=True))

    def stage_hidden(g, pair, j, q_step, live):
        cols = slice(128 * pair, 128 * pair + 128)
        key_tile = k_now[j, g, :, cols]
        query_tile = q_now[j, g, :, cols]
        bias_tile = rep8(bias_pair[pair], 16)
        query_base[g, pair] = query_tile + bias_tile
        key_base[g, pair] = (key_tile + bias_tile) - v_now[j, g, :, cols]
        kp = split3(key_tile)
        qp = split3(query_tile)
        key_parts[g, pair] = six_left(kp)
        lhs = rows(*by_side(rows(kp[0], qp[0])), *by_side(rows(kp[1], qp[1])), *by_side(rows(kp[2], qp[2])))
        yield
        top = dot_nn(lanes(lhs, lhs), states(w1_parts, g, pair, 0, 256))
        yield
        low_terms = dot_nn(lhs[:64], states(w1_parts, g, pair, 256, 384))
        yield
        offset = b1[g, pair]
        z_one = sum3(top, 64) + low_terms + rows(rep8(offset[:8], 32), rep8(offset[8:], 32))
        hidden, slope_val = twice_gelu_and_slope(z_one)
        slope[g, pair] = rows(slope_val[:16], slope_val[32:48])
        for tile in range(2):
            act[g, pair, tile] = tile_parts(hidden, tile)
        yield

    def stage_out(g, pair, j, q_step, live):
        acts = lanes(act[g, pair, 0], act[g, pair, 1])
        top = dot_nt(acts, states(w2_parts, g, pair, 0, 256))
        yield
        low_terms = dot_nt(acts[:64], rows(states(w2_parts, g, pair, 256, 384), pad128))
        yield
        total = sum3(top, 64) + low_terms
        total = total[:, :128] + total[:, 128:]
        z_two[g, pair] = jnp.where(low_tall, total[:32], total[32:]) + rep8(b2[g, pair], 32)
        yield

    def stage_norm(g, pair, j, q_step, live):
        z_val = z_two[g, pair]
        inv_std = lax.rsqrt(side_sums(z_val * z_val) * (1 / 64) + LN_EPS)
        normed = z_val * inv_std
        gain_tile = rep8(gain_pair[pair], 16)
        outs[g, q_step, :, 128 * pair:128 * pair + 128] = (normed[16:] * gain_tile + query_base[g, pair]).astype(bf16)
        key_inv[g, pair] = inv_std[:16]
        key_norm[g, pair] = normed[:16]
        d_norm[g, pair] = (normed[:16] * gain_tile + key_base[g, pair]) * (2.0 * gain_tile)
        yield

    def stage_back(g, pair, j, q_step, live):
        d_val = d_norm[g, pair]
        normed = key_norm[g, pair]
        mean_d = side_sums(d_val) * (1 / 64)
        mean_dn = side_sums(d_val * normed) * (1 / 64)
        d_val = key_inv[g, pair] * (d_val - mean_d - normed * mean_dn)
        d_two[g, pair] = rows(*split3(d_val))
        total = d_val[:8] + d_val[8:]
        for shift in (4, 2, 1):
            total = total + pltpu.roll(total, shift, 0)
        b2[g, pair] = b2[g, pair] - jnp.where(low[:8], live * rate[2 * pair], live * rate[2 * pair + 1]) * total
        yield

    def six_left(parts):
        return rows(parts[0], parts[0], parts[0], parts[1], parts[1], parts[2])

    def six_right(ref, g, pair, height, side):
        at = [part * height + side for part in range(3)]
        term = [lanes(ref[g, pair, 0, a:a + 16], ref[g, pair, 1, a:a + 16]) for a in at]
        return rows(term[0], term[1], term[2], term[0], term[1], term[0])

    def both_rates(first, second):
        return rows(jnp.full((64, 256), first, f32), jnp.full((64, 256), second, f32))

    def stage_second(g, pair, j, q_step, live):
        dp = d_two[g, pair]
        lhs = rows(*by_side(dp[:16]), *by_side(dp[16:32]), *by_side(dp[32:]))
        top = dot_nn(lanes(lhs, lhs), states(w2_parts, g, pair, 0, 256))
        yield
        low_terms = dot_nn(lhs[:32], states(w2_parts, g, pair, 256, 384))
        yield
        d_hidden = (sum3(top, 32) + low_terms) * slope[g, pair]
        for tile in range(2):
            d_one[g, pair, tile] = tile_parts(d_hidden, tile)
        yield

    def stage_second_update(g, pair, j, q_step, live):
        dp = d_two[g, pair]
        turned = six_left([dp[:16], dp[16:32], dp[32:]]).T
        yield
        grads = []
        for side in range(2):
            grads.append(dot_nn(turned[64 * side:64 * side + 64], six_right(act, g, pair, 64, 32 * side)))
            yield
        scale = [0.25 * live * rate[2 * pair + side] for side in range(2)]
        new = w2[g, pair] - both_rates(*scale) * rows(*grads)
        w2[g, pair] = new
        for tile in range(2):
            w2_parts[g, pair, tile] = tile_parts(new, tile)
        yield

    def stage_first_update(g, pair, j, q_step, live):
        turned = key_parts[g, pair].T
        yield
        grads = []
        for side in range(2):
            grads.append(dot_nn(rows(turned[64 * side:64 * side + 64], count_rows), six_right(d_one, g, pair, 32, 16 * side)))
            yield
        scale = [live * rate[2 * pair + side] for side in range(2)]
        new = w1[g, pair] - both_rates(*scale) * rows(grads[0][:64], grads[1][:64])
        w1[g, pair] = new
        for tile in range(2):
            w1_parts[g, pair, tile] = tile_parts(new, tile)
        offset = b1[g, pair]
        b1[g, pair] = rows(offset[:8] - scale[0] * grads[0][64:72], offset[8:] - scale[1] * grads[1][64:72])
        yield

    units = [(g, pair) for g in range(seqs) for pair in range(heads // 2)]
    batches = len(units) // BATCH
    stages = {'A': (0, stage_hidden), 'B': (1, stage_out), 'C': (2, stage_norm), 'D': (3, stage_back), 'E': (4, stage_second),
              'G': (4, stage_second_update), 'F': (5, stage_first_update)}

    def run_turn(turn, step, skip):
        running = {}
        for name in ORDER:
            for unit in range(BATCH):
                delay, stage = stages[name]
                j, batch = divmod(turn - delay, batches)
                if skip(j, delay):
                    continue
                if (name, unit) not in running:
                    g, pair = units[batch * BATCH + unit]
                    running[name, unit] = stage(g, pair, j, jnp.maximum(step + j - 1, 0), jnp.where(step + j >= 0, 1.0, 0.0) if j < 0 else 1.0)
                next(running[name, unit])
        for stage in running.values():
            next(stage, None)

    def body(step, last=False):
        shift_in()
        projection = project(jnp.minimum(step + ahead, steps - ahead)) if not last else iter(())
        count = 0
        for turn in range(batches * (1 if last else ahead)):
            run_turn(turn, step, lambda j, delay: last and j >= 0 and delay >= 3)
            if count >= PROJECT_FROM and (count - PROJECT_FROM) % PROJECT_EVERY == 0:
                next(projection, None)
            count += 1
        for _ in projection:
            pass

    def wait_ahead(step):
        for j in range(ahead):
            wait_tokens(step + j)

    wait_ahead(0)
    for _ in project(0):
        pass

    def loop_body(turn, carry):
        step = turn * ahead

        @pl.when(step + ahead < steps)
        def _():
            wait_ahead(step + ahead)

        @pl.when((step == 6) & (lax.rem(me, 2) == 1))
        def _():
            send_far()

        for j in range(ahead):
            row = step - 2 - ahead + j

            @pl.when(row >= 0)
            def _():
                send_out(row)

        body(step)
        return carry

    lax.fori_loop(0, steps // ahead, loop_body, 0)
    for j in range(ahead):
        send_out(jnp.int32(steps - 2 - ahead + j))
    body(jnp.int32(steps), last=True)
    send_out(jnp.int32(steps - 2))
    for turn in range(batches, batches + 2):
        run_turn(turn, jnp.int32(steps), lambda j, delay: j != 0 or delay > 2)
    w_keep.wait()
    w_swap.wait()

    @pl.loop(0, own_steps)
    def _(chunk):
        token_copy(0, near, chunk).wait_send()
        token_copy(1, far_a, chunk).wait_send()
        token_copy(2, far_b, chunk).wait_send()

    send_out(jnp.int32(steps - 1))

    def out_wait(src, dst, send, recv):
        return pltpu.make_async_remote_copy(src, dst, send, recv, device_id={'heads': other_row}, device_id_type=mesh_ids)

    def landed(row_at, place):
        return o_full.at[pl.ds(seqs * place, seqs), :, pl.ds(width * row_at, width)]

    away = steps - own_steps
    whole = outs.at[:, pl.ds(0, away)]
    out_wait(whole, whole, out_send.at[0], out_recv.at[0, 0]).wait_send()
    out_wait(outs, outs, out_send.at[1], out_recv.at[0, 0]).wait_send()
    for row_at in range(2):
        for place in range(parts_of_seq):
            spot = landed(row_at, place)
            mine = (row_axis == row_at) & (me == place)

            @pl.when(mine)
            def _():
                pltpu.make_async_copy(spot, spot, own_sem).wait()

            @pl.when(jnp.logical_not(mine))
            def _():
                out_wait(spot, spot, out_send.at[0], out_recv.at[row_at, place]).wait_recv()


def run_layer(tokens, theta_k, theta_q, theta_v, w_out, w1, w2t, b1, b2, gain, bias, rate, parts_of_seq):
    num_seqs, own_len, model_dim = tokens.shape
    seqs = num_seqs // parts_of_seq
    steps = own_len * parts_of_seq // MINI_BATCH
    heads = w1.shape[0]
    width = theta_k.shape[1]
    vmem = pl.BlockSpec(memory_space=pltpu.VMEM)
    smem = pl.BlockSpec(memory_space=pltpu.SMEM)
    hbm = pl.BlockSpec(memory_space=pl.ANY)
    each = [((128, 256), f32), ((128, 256), f32), ((2, 384, 128), bf16), ((2, 384, 128), bf16), ((16, 256), f32),
            ((2, 192, 128), bf16), ((32, 256), f32), ((2, 96, 128), bf16),
            ((8, 128), f32), ((96, 128), bf16), ((16, 128), f32), ((16, 128), f32), ((32, 128), f32),
            ((16, 128), f32), ((16, 128), f32), ((16, 128), f32), ((48, 128), bf16)]
    scratch = [pltpu.VMEM((seqs, heads // 2) + shape, dtype) for shape, dtype in each]
    scratch += [pltpu.VMEM((heads // 2, 8, 128), f32)] * 2
    scratch += [pltpu.VMEM((seqs, steps, MINI_BATCH, model_dim), bf16), pltpu.VMEM((seqs, steps, MINI_BATCH, width), bf16)]
    ahead = AHEAD
    several = pltpu.VMEM((ahead, seqs, MINI_BATCH, width), f32)
    scratch += [several] * 3 + [pltpu.VMEM((seqs, MINI_BATCH, width), f32)] + [several] * 3
    own_steps = steps // parts_of_seq
    dma = pltpu.SemaphoreType.DMA
    scratch += [dma((3, own_steps)), dma((steps,)), dma((2,)), dma((2, parts_of_seq)), dma, dma, dma, dma]
    return pl.pallas_call(
        functools.partial(layer_kernel, steps, seqs, heads, ahead, parts_of_seq),
        out_shape=(jax.ShapeDtypeStruct((num_seqs, own_len, 2 * width), bf16), jax.ShapeDtypeStruct((2 * width, model_dim), bf16)),
        in_specs=[hbm] + [vmem] * 3 + [hbm] + [vmem] * 6 + [smem],
        out_specs=(hbm, hbm),
        scratch_shapes=scratch,
        compiler_params=pltpu.CompilerParams(vmem_limit_bytes=60 * 2 ** 20, collective_id=0, has_side_effects=True),
    )(tokens, theta_k, theta_q, theta_v, w_out, w1, w2t, b1, b2, gain, bias, rate)


def solution(mesh):
    parts_of_seq = mesh.shape['seq']

    def local_fn(tokens, theta_q, theta_k, theta_v, w_out, w_one, b_one, w_two, b_two, ln_gain, ln_bias, inner_lr):
        outs, w_full = run_layer(tokens, theta_k, theta_q, theta_v, w_out, w_one, jnp.swapaxes(w_two, 1, 2), b_one, b_two, ln_gain, ln_bias, inner_lr, parts_of_seq)
        return jnp.einsum('bte,ed->btd', outs, w_full, preferred_element_type=f32).astype(bf16)

    arg_specs = (P('data', 'seq', None), P(None, 'heads'), P(None, 'heads'), P(None, 'heads'), P('heads', None), P('heads', None, None), P('heads', None), P('heads', None, None), P('heads', None), P('heads', None), P('heads', None), P('heads'))
    return jax.shard_map(local_fn, mesh=mesh, in_specs=arg_specs, out_specs=P('data', 'seq', None), check_vma=False)
```

```python
import functools

import jax
import jax.numpy as jnp
from jax import lax
from jax.experimental import pallas as pl
from jax.experimental.pallas import tpu as pltpu
from jax.sharding import PartitionSpec as P

MINI_BATCH = 16
AHEAD = 2
BATCH = 2
ORDER = 'MCDGFAABEBAEABEGGGFFF'
PROJECT_EVERY = 1
PROJECT_FROM = 0
LN_EPS = 1e-6
GELU_C0 = 0.7978845608028654
GELU_C1 = 0.044715
f32 = jnp.float32
bf16 = jnp.bfloat16


def split3(val):
    high = val.astype(bf16)
    rest = val - high.astype(f32)
    mid = rest.astype(bf16)
    return high, mid, (rest - mid.astype(f32)).astype(bf16)


def dot_nn(lhs, rhs):
    return lax.dot_general(lhs, rhs, (((1,), (0,)), ((), ())), preferred_element_type=f32)


def dot_nt(lhs, rhs):
    return lax.dot_general(lhs, rhs, (((1,), (1,)), ((), ())), preferred_element_type=f32)


def dot_tn(lhs, rhs):
    return lax.dot_general(lhs, rhs, (((0,), (0,)), ((), ())), preferred_element_type=f32)


def rows(*parts):
    return jnp.concatenate(parts, 0)


def lanes(*parts):
    return jnp.concatenate(parts, 1)


def rep8(val, count):
    return rows(*([val] * (count // 8)))


def sum3(val, count):
    return val[0:count] + val[count:2 * count] + val[2 * count:3 * count]


def twice_gelu_and_slope(z_val):
    square = z_val * z_val
    tanh_val = jnp.tanh(z_val * (GELU_C0 + (GELU_C0 * GELU_C1) * square))
    plus = 1.0 + tanh_val
    slope = plus + (1.0 - tanh_val * tanh_val) * (z_val * (GELU_C0 + (3 * GELU_C0 * GELU_C1) * square))
    return z_val * plus, slope


def tile_parts(val, tile):
    return rows(*split3(val[:, 128 * tile:128 * tile + 128]))


def eight_rows(row, twice):
    row = lanes(row, row) if twice else row
    return jnp.broadcast_to(row, (8, row.shape[1]))


def layer_kernel(steps, seqs, heads, ahead, parts_of_seq, tokens, theta_k, theta_q, theta_v, w_out, w1_in, w2_in, b1_in, b2_in, gain_in, bias_in, rate_in,
                 o_full, w_full,
                 w1, w2, w1_parts, w2_parts, b1, act, slope, d_one, b2, key_parts, key_base, query_base, z_two, key_norm, key_inv, d_norm, d_two, gain_pair, bias_pair,
                 tok, outs, k_now, v_now, q_now, q_last, k_new, v_new, q_new,
                 tok_send, tok_recv, half_recv, pass_recv, out_send, out_recv, own_sem, w_send, w_recv, w_own):
    low = lax.broadcasted_iota(jnp.int32, (16, 128), 1) < 64
    pad128 = jnp.zeros((128, 256), bf16)
    low_tall = lax.broadcasted_iota(jnp.int32, (32, 128), 1) < 64
    count_rows = jnp.where(lax.broadcasted_iota(jnp.int32, (16, 96), 1) < 48, 1.0, 0.0).astype(bf16)
    width = 64 * heads
    own_steps = steps // parts_of_seq
    row_axis = lax.axis_index('heads')
    me = lax.axis_index('seq')
    other_row = 1 - row_axis
    mesh_ids = pl.DeviceIdType.MESH

    def other_core(place):
        return place + 1 - 2 * lax.rem(place, 2)

    near = other_core(me)
    far_a = lax.rem(me + 2, 4)
    far_b = other_core(far_a)

    barrier = pltpu.get_barrier_semaphore()
    for shift_row in range(2):
        for shift in range(parts_of_seq):
            if shift_row or shift:
                pl.semaphore_signal(barrier, inc=1, device_id={'heads': lax.rem(row_axis + shift_row, 2), 'seq': lax.rem(me + shift, parts_of_seq)}, device_id_type=mesh_ids)
    pl.semaphore_wait(barrier, 2 * parts_of_seq - 1)

    half = seqs // 2
    my_half = pl.ds(half * row_axis, half)
    far_from = (1 - me // 2) * (steps // 2)

    def remote(src, dst, send, recv, **device):
        return pltpu.make_async_remote_copy(src, dst, send, recv, device_id=device, device_id_type=mesh_ids)

    def near_tokens(chunk):
        at = me * own_steps + chunk
        return tokens.at[pl.ds(seqs * me, seqs), pl.ds(MINI_BATCH * chunk, MINI_BATCH)], tok.at[:, at], tok_recv.at[at]

    def send_near(turn):
        for j in range(ahead):
            chunk = ahead * (turn - (own_steps // ahead) * me + 4) + j

            @pl.when((chunk >= 0) & (chunk < own_steps))
            def _():
                pltpu.make_async_copy(*near_tokens(chunk)).start()
                at = me * own_steps + chunk
                src = tokens.at[pl.ds(seqs * near, seqs), pl.ds(MINI_BATCH * chunk, MINI_BATCH)]
                remote(src, tok.at[:, at], tok_send.at[0], tok_recv.at[at], seq=near).start()

    def send_far(turn):
        for j in range(ahead):
            chunk = ahead * (turn - 4 * me + 3) + j

            @pl.when((chunk >= 0) & (chunk < own_steps))
            def _():
                at = me * own_steps + chunk
                for dest in (far_a, far_b):
                    src = tokens.at[pl.ds(seqs * dest + half * row_axis, half), pl.ds(MINI_BATCH * chunk, MINI_BATCH)]
                    remote(src, tok.at[my_half, at], tok_send.at[1], half_recv.at[lax.rem(at, steps // 2)], seq=dest).start()

    def pass_on(step):
        spot = tok.at[my_half, step]
        slot = step - far_from
        remote(spot, spot, tok_send.at[2], half_recv.at[slot], heads=other_row).wait_recv()
        remote(spot, spot, tok_send.at[2], pass_recv.at[slot], heads=other_row).start()

    def pass_ahead(step):
        @pl.when((step >= far_from) & (step < far_from + steps // 2))
        def _():
            pass_on(step)

    def wait_tokens(step):
        is_far = (step >= far_from) & (step < far_from + steps // 2)

        @pl.when(is_far)
        def _():
            spot = tok.at[my_half, step]
            remote(spot, spot, tok_send.at[2], pass_recv.at[step - far_from], heads=other_row).wait_recv()

        @pl.when(jnp.logical_not(is_far))
        def _():
            remote(tok.at[:, step], tok.at[:, step], tok_send.at[0], tok_recv.at[step], seq=near).wait_recv()

    for turn in range(3):
        send_far(jnp.int32(turn - 3))
    for turn in range(4):
        send_near(jnp.int32(turn - 4))

    my_w_rows = w_full.at[pl.ds(pl.multiple_of(row_axis * width, width), width)]
    w_swap = pltpu.make_async_remote_copy(w_out, my_w_rows, w_send, w_recv, device_id={'heads': other_row}, device_id_type=mesh_ids)
    w_keep = pltpu.make_async_copy(w_out, my_w_rows, w_own)
    w_keep.start()

    @pl.when(me < 2)
    def _():
        w_swap.start()


    def out_rows(step, count):
        return pl.ds(pl.multiple_of(MINI_BATCH * step, MINI_BATCH), MINI_BATCH * count)

    def send_out(step, count):
        owner = step // own_steps
        src = outs.at[:, out_rows(step, count)]
        dst = o_full.at[pl.ds(seqs * me, seqs), out_rows(lax.rem(step, own_steps), count), pl.ds(pl.multiple_of(width * row_axis, width), width)]
        remote(src, dst, out_send.at[1], out_recv.at[row_axis, me], heads=other_row, seq=owner).start()

        @pl.when(owner != me)
        def _():
            remote(src, dst, out_send.at[0], out_recv.at[row_axis, me], seq=owner).start()

        @pl.when(owner == me)
        def _():
            pltpu.make_async_copy(src, dst, own_sem).start()

    for pair in range(heads // 2):
        even, odd = 2 * pair, 2 * pair + 1

        def pair_row(source):
            return jnp.broadcast_to(lanes(source[even:even + 1], source[odd:odd + 1]), (8, 128))

        gain_pair[pair] = pair_row(gain_in)
        bias_pair[pair] = pair_row(bias_in)
        offset = pair_row(b2_in)
        hidden_offset = rows(eight_rows(b1_in[even:even + 1], False), eight_rows(b1_in[odd:odd + 1], False))
        first = rows(w1_in[even], w1_in[odd])
        second = rows(0.5 * w2_in[even], 0.5 * w2_in[odd])
        for g in range(seqs):
            w1[g, pair] = first
            w2[g, pair] = second
            b1[g, pair] = hidden_offset
            b2[g, pair] = offset
        for tile in range(2):
            first_parts, second_parts = tile_parts(first, tile), tile_parts(second, tile)
            for g in range(seqs):
                w1_parts[g, pair, tile] = first_parts
                w2_parts[g, pair, tile] = second_parts
    q_last[...] = jnp.zeros(q_last.shape, f32)

    @pl.loop(0, seqs)
    def _(g):
        for ref in (act, slope, d_one, key_parts, key_base, query_base, z_two, key_norm, key_inv, d_norm, d_two):
            ref[g] = jnp.zeros(ref.shape[1:], ref.dtype)

    rate = [rate_in[h] * (1 / MINI_BATCH) for h in range(heads)]

    def both(unit):
        return [2 * pair + side for pair in unit for side in range(2)]

    def project(step):
        for theta, target in ((theta_k, k_new), (theta_q, q_new), (theta_v, v_new)):
            for col in range(0, width, 256):
                toks = tok[:, pl.ds(step, ahead)].reshape(seqs * ahead * MINI_BATCH, tok.shape[3])
                found = dot_nn(toks, theta[:, col:col + 256]).reshape(seqs, ahead, MINI_BATCH, 256)
                for j in range(ahead):
                    target[j, :, :, col:col + 256] = found[:, j]
                yield

    def shift_in():
        k_now[...] = k_new[...]
        v_now[...] = v_new[...]
        q_now[0] = q_last[...]
        for j in range(1, ahead):
            q_now[j] = q_new[j - 1]
        q_last[...] = q_new[ahead - 1]

    def states(ref, g, pair, first, last):
        return lanes(ref[g, pair, 0, first:last], ref[g, pair, 1, first:last])

    def by_side(val):
        keep = lax.broadcasted_iota(jnp.int32, val.shape, 1) < 64
        zero = jnp.zeros(val.shape, val.dtype)
        return [jnp.where(keep, val, zero), jnp.where(keep, zero, val)]

    def side_sums(val):
        keep = low if val.shape[0] == 16 else low_tall
        return jnp.where(keep, jnp.sum(jnp.where(keep, val, 0.0), 1, keepdims=True), jnp.sum(jnp.where(keep, 0.0, val), 1, keepdims=True))

    def stage_hidden(g, pair, j, q_step, live):
        cols = slice(128 * pair, 128 * pair + 128)
        key_tile = k_now[j, g, :, cols]
        query_tile = q_now[j, g, :, cols]
        bias_tile = rep8(bias_pair[pair], 16)
        query_base[g, pair] = query_tile + bias_tile
        key_base[g, pair] = (key_tile + bias_tile) - v_now[j, g, :, cols]
        kp = split3(key_tile)
        qp = split3(query_tile)
        key_parts[g, pair] = six_left(kp)
        lhs = rows(*by_side(rows(kp[0], qp[0])), *by_side(rows(kp[1], qp[1])), *by_side(rows(kp[2], qp[2])))
        yield
        top = dot_nn(lanes(lhs, lhs), states(w1_parts, g, pair, 0, 256))
        yield
        low_terms = dot_nn(lhs[:64], states(w1_parts, g, pair, 256, 384))
        yield
        offset = b1[g, pair]
        z_one = sum3(top, 64) + low_terms + rows(rep8(offset[:8], 32), rep8(offset[8:], 32))
        hidden, slope_val = twice_gelu_and_slope(z_one)
        slope[g, pair] = rows(slope_val[:16], slope_val[32:48])
        for tile in range(2):
            act[g, pair, tile] = tile_parts(hidden, tile)
        yield

    def stage_out(g, pair, j, q_step, live):
        acts = lanes(act[g, pair, 0], act[g, pair, 1])
        top = dot_nt(acts, states(w2_parts, g, pair, 0, 256))
        yield
        low_terms = dot_nt(acts[:64], rows(states(w2_parts, g, pair, 256, 384), pad128))
        yield
        total = sum3(top, 64) + low_terms
        total = total[:, :128] + total[:, 128:]
        z_two[g, pair] = jnp.where(low_tall, total[:32], total[32:]) + rep8(b2[g, pair], 32)
        yield

    def stage_center(g, pair, j, q_step, live):
        z_val = z_two[g, pair]
        z_two[g, pair] = z_val - side_sums(z_val) * (1 / 64)
        yield

    def stage_norm(g, pair, j, q_step, live):
        z_val = z_two[g, pair]
        inv_std = lax.rsqrt(side_sums(z_val * z_val) * (1 / 64) + LN_EPS)
        normed = z_val * inv_std
        gain_tile = rep8(gain_pair[pair], 16)
        outs[g, out_rows(q_step, 1), 128 * pair:128 * pair + 128] = (normed[16:] * gain_tile + query_base[g, pair]).astype(bf16)
        key_inv[g, pair] = inv_std[:16]
        key_norm[g, pair] = normed[:16]
        d_norm[g, pair] = (normed[:16] * gain_tile + key_base[g, pair]) * (2.0 * gain_tile)
        yield

    def stage_back(g, pair, j, q_step, live):
        d_val = d_norm[g, pair]
        normed = key_norm[g, pair]
        mean_d = side_sums(d_val) * (1 / 64)
        mean_dn = side_sums(d_val * normed) * (1 / 64)
        d_val = key_inv[g, pair] * (d_val - mean_d - normed * mean_dn)
        d_two[g, pair] = rows(*split3(d_val))
        total = d_val[:8] + d_val[8:]
        for shift in (4, 2, 1):
            total = total + pltpu.roll(total, shift, 0)
        b2[g, pair] = b2[g, pair] - jnp.where(low[:8], live * rate[2 * pair], live * rate[2 * pair + 1]) * total
        yield

    def six_left(parts):
        return rows(parts[0], parts[0], parts[0], parts[1], parts[1], parts[2])

    def six_right(ref, g, pair, height, side):
        at = [part * height + side for part in range(3)]
        term = [lanes(ref[g, pair, 0, a:a + 16], ref[g, pair, 1, a:a + 16]) for a in at]
        return rows(term[0], term[1], term[2], term[0], term[1], term[0])

    def both_rates(first, second):
        return rows(jnp.full((64, 256), first, f32), jnp.full((64, 256), second, f32))

    def stage_second(g, pair, j, q_step, live):
        dp = d_two[g, pair]
        lhs = rows(*by_side(dp[:16]), *by_side(dp[16:32]), *by_side(dp[32:]))
        top = dot_nn(lanes(lhs, lhs), states(w2_parts, g, pair, 0, 256))
        yield
        low_terms = dot_nn(lhs[:32], states(w2_parts, g, pair, 256, 384))
        yield
        d_hidden = (sum3(top, 32) + low_terms) * slope[g, pair]
        for tile in range(2):
            d_one[g, pair, tile] = tile_parts(d_hidden, tile)
        yield

    def stage_second_update(g, pair, j, q_step, live):
        dp = d_two[g, pair]
        turned = six_left([dp[:16], dp[16:32], dp[32:]]).T
        yield
        grads = []
        for side in range(2):
            grads.append(dot_nn(turned[64 * side:64 * side + 64], six_right(act, g, pair, 64, 32 * side)))
            yield
        scale = [0.25 * live * rate[2 * pair + side] for side in range(2)]
        new = w2[g, pair] - both_rates(*scale) * rows(*grads)
        w2[g, pair] = new
        for tile in range(2):
            w2_parts[g, pair, tile] = tile_parts(new, tile)
        yield

    def stage_first_update(g, pair, j, q_step, live):
        turned = key_parts[g, pair].T
        yield
        grads = []
        for side in range(2):
            grads.append(dot_nn(rows(turned[64 * side:64 * side + 64], count_rows), six_right(d_one, g, pair, 32, 16 * side)))
            yield
        scale = [live * rate[2 * pair + side] for side in range(2)]
        new = w1[g, pair] - both_rates(*scale) * rows(grads[0][:64], grads[1][:64])
        w1[g, pair] = new
        for tile in range(2):
            w1_parts[g, pair, tile] = tile_parts(new, tile)
        offset = b1[g, pair]
        b1[g, pair] = rows(offset[:8] - scale[0] * grads[0][64:72], offset[8:] - scale[1] * grads[1][64:72])
        yield

    units = [(g, pair) for g in range(seqs) for pair in range(heads // 2)]
    batches = len(units) // BATCH
    stages = {'A': (0, stage_hidden), 'B': (1, stage_out), 'M': (2, stage_center), 'C': (3, stage_norm), 'D': (4, stage_back),
              'E': (5, stage_second), 'G': (5, stage_second_update), 'F': (6, stage_first_update)}

    def run_turn(turn, step, skip):
        running = {}
        for name in ORDER:
            for unit in range(BATCH):
                delay, stage = stages[name]
                j, batch = divmod(turn - delay, batches)
                if skip(j, delay):
                    continue
                if (name, unit) not in running:
                    g, pair = units[batch * BATCH + unit]
                    running[name, unit] = stage(g, pair, j, jnp.maximum(step + j - 1, 0), jnp.where(step + j >= 0, 1.0, 0.0) if j < 0 else 1.0)
                next(running[name, unit])
        for stage in running.values():
            next(stage, None)

    def body(step, last=False):
        shift_in()
        projection = project(jnp.minimum(step + ahead, steps - ahead)) if not last else iter(())
        count = 0
        for turn in range(batches * (1 if last else ahead)):
            run_turn(turn, step, lambda j, delay: last and j >= 0 and delay > 3)
            if count >= PROJECT_FROM and (count - PROJECT_FROM) % PROJECT_EVERY == 0:
                next(projection, None)
            count += 1
        for _ in projection:
            pass

    def wait_ahead(step):
        for j in range(ahead):
            wait_tokens(step + j)

    for j in range(2 * ahead):
        pass_ahead(jnp.int32(j))
    wait_ahead(0)
    for _ in project(0):
        pass

    def loop_body(turn, carry):
        step = turn * ahead

        for j in range(ahead):
            pass_ahead(step + 2 * ahead + j)
        send_far(turn)
        send_near(turn)

        @pl.when((me >= 2) & (turn == steps // (2 * ahead)))
        def _():
            w_swap.start()


        @pl.when(step + ahead < steps)
        def _():
            wait_ahead(step + ahead)

        @pl.when(turn >= 2)
        def _():
            send_out(step - 2 * ahead, ahead)

        body(step)
        return carry

    lax.fori_loop(0, steps // ahead, loop_body, 0)
    send_out(jnp.int32(steps - 2 * ahead), ahead)
    body(jnp.int32(steps), last=True)
    send_out(jnp.int32(steps - 2), 1)
    for turn in range(batches, batches + 3):
        run_turn(turn, jnp.int32(steps), lambda j, delay: j != 0 or delay > 3)
    w_keep.wait()
    w_swap.wait()
    quarter = tok.at[:, pl.ds(0, own_steps)]
    for slot in range(3):
        remote(quarter, quarter, tok_send.at[slot], pass_recv.at[0], heads=other_row).wait_send()
    send_out(jnp.int32(steps - 1), 1)

    def rows_of(count):
        return outs.at[:, pl.ds(0, count * MINI_BATCH)]

    def done(count, send, recv):
        return remote(rows_of(count), rows_of(count), send, recv, heads=other_row)

    done(steps - own_steps, out_send.at[0], out_recv.at[0, 0]).wait_send()
    done(steps, out_send.at[1], out_recv.at[0, 0]).wait_send()
    pltpu.make_async_copy(rows_of(own_steps), rows_of(own_steps), own_sem).wait()
    for place in range(parts_of_seq):
        done(own_steps, out_send.at[0], out_recv.at[other_row, place]).wait_recv()

        @pl.when(me != place)
        def _():
            done(own_steps, out_send.at[0], out_recv.at[row_axis, place]).wait_recv()


def run_layer(tokens, theta_k, theta_q, theta_v, w_out, w1, w2t, b1, b2, gain, bias, rate, parts_of_seq):
    num_seqs, own_len, model_dim = tokens.shape
    seqs = num_seqs // parts_of_seq
    steps = own_len * parts_of_seq // MINI_BATCH
    heads = w1.shape[0]
    width = theta_k.shape[1]
    vmem = pl.BlockSpec(memory_space=pltpu.VMEM)
    smem = pl.BlockSpec(memory_space=pltpu.SMEM)
    hbm = pl.BlockSpec(memory_space=pl.ANY)
    each = [((128, 256), f32), ((128, 256), f32), ((2, 384, 128), bf16), ((2, 384, 128), bf16), ((16, 256), f32),
            ((2, 192, 128), bf16), ((32, 256), f32), ((2, 96, 128), bf16),
            ((8, 128), f32), ((96, 128), bf16), ((16, 128), f32), ((16, 128), f32), ((32, 128), f32),
            ((16, 128), f32), ((16, 128), f32), ((16, 128), f32), ((48, 128), bf16)]
    scratch = [pltpu.VMEM((seqs, heads // 2) + shape, dtype) for shape, dtype in each]
    scratch += [pltpu.VMEM((heads // 2, 8, 128), f32)] * 2
    scratch += [pltpu.VMEM((seqs, steps, MINI_BATCH, model_dim), bf16), pltpu.VMEM((seqs, steps * MINI_BATCH, width), bf16)]
    ahead = AHEAD
    several = pltpu.VMEM((ahead, seqs, MINI_BATCH, width), f32)
    scratch += [several] * 3 + [pltpu.VMEM((seqs, MINI_BATCH, width), f32)] + [several] * 3
    own_steps = steps // parts_of_seq
    dma = pltpu.SemaphoreType.DMA
    scratch += [dma((3,)), dma((steps,)), dma((steps // 2,)), dma((steps // 2,)), dma((2,)), dma((2, parts_of_seq)), dma, dma, dma, dma]
    return pl.pallas_call(
        functools.partial(layer_kernel, steps, seqs, heads, ahead, parts_of_seq),
        out_shape=(jax.ShapeDtypeStruct((num_seqs, own_len, 2 * width), bf16), jax.ShapeDtypeStruct((2 * width, model_dim), bf16)),
        in_specs=[hbm] + [vmem] * 3 + [hbm] + [vmem] * 6 + [smem],
        out_specs=(hbm, hbm),
        scratch_shapes=scratch,
        compiler_params=pltpu.CompilerParams(vmem_limit_bytes=60 * 2 ** 20, collective_id=0, has_side_effects=True),
    )(tokens, theta_k, theta_q, theta_v, w_out, w1, w2t, b1, b2, gain, bias, rate)


def solution(mesh):
    parts_of_seq = mesh.shape['seq']

    def local_fn(tokens, theta_q, theta_k, theta_v, w_out, w_one, b_one, w_two, b_two, ln_gain, ln_bias, inner_lr):
        outs, w_full = run_layer(tokens, theta_k, theta_q, theta_v, w_out, w_one, jnp.swapaxes(w_two, 1, 2), b_one, b_two, ln_gain, ln_bias, inner_lr, parts_of_seq)
        return jnp.einsum('bte,ed->btd', outs, w_full, preferred_element_type=f32).astype(bf16)

    arg_specs = (P('data', 'seq', None), P(None, 'heads'), P(None, 'heads'), P(None, 'heads'), P('heads', None), P('heads', None, None), P('heads', None), P('heads', None, None), P('heads', None), P('heads', None), P('heads', None), P('heads'))
    return jax.shard_map(local_fn, mesh=mesh, in_specs=arg_specs, out_specs=P('data', 'seq', None), check_vma=False)
```

```python
import functools

import jax
import jax.numpy as jnp
from jax import lax
from jax.experimental import pallas as pl
from jax.experimental.pallas import tpu as pltpu
from jax.sharding import PartitionSpec as P

MINI_BATCH = 16
AHEAD = 2
BATCH = 2
ORDER = 'MCDGFAABEBAEABEGGGFFF'
PROJECT_EVERY = 1
PROJECT_FROM = 0
LN_EPS = 1e-6
GELU_C0 = 0.7978845608028654
GELU_C1 = 0.044715
f32 = jnp.float32
bf16 = jnp.bfloat16


def split3(val):
    high = val.astype(bf16)
    rest = val - high.astype(f32)
    mid = rest.astype(bf16)
    return high, mid, (rest - mid.astype(f32)).astype(bf16)


def dot_nn(lhs, rhs):
    return lax.dot_general(lhs, rhs, (((1,), (0,)), ((), ())), preferred_element_type=f32)


def dot_nt(lhs, rhs):
    return lax.dot_general(lhs, rhs, (((1,), (1,)), ((), ())), preferred_element_type=f32)


def dot_tn(lhs, rhs):
    return lax.dot_general(lhs, rhs, (((0,), (0,)), ((), ())), preferred_element_type=f32)


def rows(*parts):
    return jnp.concatenate(parts, 0)


def lanes(*parts):
    return jnp.concatenate(parts, 1)


def rep8(val, count):
    return rows(*([val] * (count // 8)))


def sum3(val, count):
    return val[0:count] + val[count:2 * count] + val[2 * count:3 * count]


def twice_gelu_and_slope(z_val):
    square = z_val * z_val
    tanh_val = jnp.tanh(z_val * (GELU_C0 + (GELU_C0 * GELU_C1) * square))
    plus = 1.0 + tanh_val
    slope = plus + (1.0 - tanh_val * tanh_val) * (z_val * (GELU_C0 + (3 * GELU_C0 * GELU_C1) * square))
    return z_val * plus, slope


def tile_parts(val, tile):
    return rows(*split3(val[:, 128 * tile:128 * tile + 128]))


def eight_rows(row, twice):
    row = lanes(row, row) if twice else row
    return jnp.broadcast_to(row, (8, row.shape[1]))


def layer_kernel(steps, seqs, heads, ahead, parts_of_seq, tokens, w_out, theta_k_at, theta_q_at, theta_v_at, w1_at, w2_at, b1_at, b2_at, gain_at, bias_at, rate_in,
                 o_full, w_full, y_early, theta_k, theta_q, theta_v, w1_in, w2_in, b1_in, b2_in, gain_in, bias_in,
                 w1, w2, w1_parts, w2_parts, b1, act, slope, d_one, b2, key_parts, key_base, query_base, z_two, key_norm, key_inv, d_norm, d_two, gain_pair, bias_pair,
                 tok, outs, k_now, v_now, q_now, q_last, k_new, v_new, q_new,
                 load_sem, tok_send, own_recv, near_recv, half_recv, pass_recv, out_send, out_recv, own_sem, w_send, w_recv, w_own,
                 w_all, o_block, y_block, o_sem, y_sem):
    low = lax.broadcasted_iota(jnp.int32, (16, 128), 1) < 64
    pad128 = jnp.zeros((128, 256), bf16)
    low_tall = lax.broadcasted_iota(jnp.int32, (32, 128), 1) < 64
    count_rows = jnp.where(lax.broadcasted_iota(jnp.int32, (16, 96), 1) < 48, 1.0, 0.0).astype(bf16)
    width = 64 * heads
    own_steps = steps // parts_of_seq
    early_steps = 2 * own_steps // 3
    row_axis = lax.axis_index('heads')
    me = lax.axis_index('seq')
    other_row = 1 - row_axis
    mesh_ids = pl.DeviceIdType.MESH

    def other_core(place):
        return place + 1 - 2 * lax.rem(place, 2)

    near = other_core(me)
    far_a = lax.rem(me + 2, 4)
    far_b = other_core(far_a)

    barrier = pltpu.get_barrier_semaphore()
    for shift_row in range(2):
        for shift in range(parts_of_seq):
            if shift_row or shift:
                pl.semaphore_signal(barrier, inc=1, device_id={'heads': lax.rem(row_axis + shift_row, 2), 'seq': lax.rem(me + shift, parts_of_seq)}, device_id_type=mesh_ids)
    pl.semaphore_wait(barrier, 2 * parts_of_seq - 1)

    half = seqs // 2
    my_half = pl.ds(half * row_axis, half)
    far_from = (1 - me // 2) * (steps // 2)

    def remote(src, dst, send, recv, **device):
        return pltpu.make_async_remote_copy(src, dst, send, recv, device_id=device, device_id_type=mesh_ids)

    pair_rows = ahead * MINI_BATCH
    own_turns = own_steps // ahead
    far_turns = 2 * own_turns
    far_turn = far_turns * (1 - me // 2)

    def tok_rows(turn, count=1):
        return pl.ds(pl.multiple_of(pair_rows * turn, pair_rows), pair_rows * count)

    def send_far(turn):
        piece = turn - 4 * me + 3

        @pl.when((piece >= 0) & (piece < own_turns))
        def _():
            at = me * own_turns + piece
            for dest in (far_a, far_b):
                src = tokens.at[pl.ds(seqs * dest + half * row_axis, half), tok_rows(piece)]
                remote(src, tok.at[my_half, tok_rows(at)], tok_send.at[1], half_recv.at[lax.rem(at, far_turns)], seq=dest).start()

    def is_far(turn):
        return (turn >= far_turn) & (turn < far_turn + far_turns)

    def pass_on(turn):
        @pl.when(is_far(turn))
        def _():
            spot = tok.at[my_half, tok_rows(turn)]
            slot = turn - far_turn
            remote(spot, spot, tok_send.at[2], half_recv.at[slot], heads=other_row).wait_recv()
            remote(spot, spot, tok_send.at[2], pass_recv.at[slot], heads=other_row).start()

    def wait_tokens(turn):
        @pl.when(is_far(turn))
        def _():
            spot = tok.at[my_half, tok_rows(turn)]
            remote(spot, spot, tok_send.at[2], pass_recv.at[turn - far_turn], heads=other_row).wait_recv()

        @pl.when(lax.rem(turn, own_turns) == 0)
        def _():
            spot = tok.at[:, tok_rows(turn, own_turns)]

            @pl.when(turn // own_turns == me)
            def _():
                pltpu.make_async_copy(spot, spot, own_recv).wait()

            @pl.when(turn // own_turns == near)
            def _():
                remote(spot, spot, tok_send.at[0], near_recv, seq=near).wait_recv()

    for turn in range(3):
        send_far(jnp.int32(turn - 3))
    own_block = tok.at[:, tok_rows(me * own_turns, own_turns)]
    pltpu.make_async_copy(tokens.at[pl.ds(seqs * me, seqs)], own_block, own_recv).start()
    remote(tokens.at[pl.ds(seqs * near, seqs)], own_block, tok_send.at[0], near_recv, seq=near).start()
    loads = [pltpu.make_async_copy(src, dst, load_sem.at[i]) for i, (src, dst) in enumerate((
        (w1_at, w1_in), (w2_at, w2_in), (b1_at, b1_in), (b2_at, b2_in), (gain_at, gain_in), (bias_at, bias_in),
        (theta_k_at, theta_k), (theta_q_at, theta_q), (theta_v_at, theta_v)))]
    for load in loads:
        load.start()

    my_w_rows = w_full.at[pl.ds(pl.multiple_of(row_axis * width, width), width)]
    w_swap = pltpu.make_async_remote_copy(w_out, my_w_rows, w_send, w_recv, device_id={'heads': other_row}, device_id_type=mesh_ids)
    w_keep = pltpu.make_async_copy(w_out, my_w_rows, w_own)
    w_keep.start()
    w_rows = width // 8

    def send_w(turn):
        piece = turn - 2

        @pl.when((piece >= 0) & (piece < 8))
        def _():
            spot = pl.ds(pl.multiple_of(w_rows * piece, w_rows), w_rows)
            remote(w_out.at[spot], my_w_rows.at[spot], w_send, w_recv, heads=other_row).start()


    def out_rows(step, count):
        return pl.ds(pl.multiple_of(MINI_BATCH * step, MINI_BATCH), MINI_BATCH * count)

    def out_copy(step, count):
        place = pl.ds(seqs * me, seqs), out_rows(lax.rem(step, own_steps), count), pl.ds(pl.multiple_of(width * row_axis, width), width)
        late = (lax.rem(step, own_steps) >= early_steps).astype(jnp.int32)
        return outs.at[:, out_rows(step, count)], o_full.at[place], step // own_steps, late

    def send_row(step, count):
        src, dst, owner, late = out_copy(step, count)

        @pl.when(owner != me)
        def _():
            remote(src, dst, out_send.at[0], out_recv.at[row_axis, me, late], seq=owner).start()

        @pl.when(owner == me)
        def _():
            pltpu.make_async_copy(src, dst, own_sem.at[late]).start()

    def send_across(step, count):
        src, dst, owner, late = out_copy(step, count)
        remote(src, dst, out_send.at[1], out_recv.at[row_axis, me, late], heads=other_row, seq=owner).start()

    for load in loads:
        load.wait()
    for pair in range(heads // 2):
        even, odd = 2 * pair, 2 * pair + 1

        def pair_row(source):
            return jnp.broadcast_to(lanes(source[even:even + 1], source[odd:odd + 1]), (8, 128))

        gain_pair[pair] = pair_row(gain_in)
        bias_pair[pair] = pair_row(bias_in)
        offset = pair_row(b2_in)
        hidden_offset = rows(eight_rows(b1_in[even:even + 1], False), eight_rows(b1_in[odd:odd + 1], False))
        first = rows(w1_in[even], w1_in[odd])
        second = rows(0.5 * w2_in[even], 0.5 * w2_in[odd])
        for g in range(seqs):
            w1[g, pair] = first
            w2[g, pair] = second
            b1[g, pair] = hidden_offset
            b2[g, pair] = offset
        for tile in range(2):
            first_parts, second_parts = tile_parts(first, tile), tile_parts(second, tile)
            for g in range(seqs):
                w1_parts[g, pair, tile] = first_parts
                w2_parts[g, pair, tile] = second_parts
    q_last[...] = jnp.zeros(q_last.shape, f32)

    @pl.loop(0, seqs)
    def _(g):
        for ref in (act, slope, d_one, key_parts, key_base, query_base, z_two, key_norm, key_inv, d_norm, d_two):
            ref[g] = jnp.zeros(ref.shape[1:], ref.dtype)

    rate = [rate_in[h] * (1 / MINI_BATCH) for h in range(heads)]

    def both(unit):
        return [2 * pair + side for pair in unit for side in range(2)]

    def project(turn):
        for theta, target in ((theta_k, k_new), (theta_q, q_new), (theta_v, v_new)):
            for col in range(0, width, 256):
                toks = tok[:, tok_rows(turn)].reshape(seqs * pair_rows, tok.shape[2])
                found = dot_nn(toks, theta[:, col:col + 256]).reshape(seqs, ahead, MINI_BATCH, 256)
                for j in range(ahead):
                    target[j, :, :, col:col + 256] = found[:, j]
                yield

    def shift_in():
        k_now[...] = k_new[...]
        v_now[...] = v_new[...]
        q_now[0] = q_last[...]
        for j in range(1, ahead):
            q_now[j] = q_new[j - 1]
        q_last[...] = q_new[ahead - 1]

    def states(ref, g, pair, first, last):
        return lanes(ref[g, pair, 0, first:last], ref[g, pair, 1, first:last])

    def by_side(val):
        keep = lax.broadcasted_iota(jnp.int32, val.shape, 1) < 64
        zero = jnp.zeros(val.shape, val.dtype)
        return [jnp.where(keep, val, zero), jnp.where(keep, zero, val)]

    def side_sums(val):
        keep = low if val.shape[0] == 16 else low_tall
        return jnp.where(keep, jnp.sum(jnp.where(keep, val, 0.0), 1, keepdims=True), jnp.sum(jnp.where(keep, 0.0, val), 1, keepdims=True))

    def stage_hidden(g, pair, j, q_step, live):
        cols = slice(128 * pair, 128 * pair + 128)
        key_tile = k_now[j, g, :, cols]
        query_tile = q_now[j, g, :, cols]
        bias_tile = rep8(bias_pair[pair], 16)
        query_base[g, pair] = query_tile + bias_tile
        key_base[g, pair] = (key_tile + bias_tile) - v_now[j, g, :, cols]
        kp = split3(key_tile)
        qp = split3(query_tile)
        key_parts[g, pair] = six_left(kp)
        lhs = rows(*by_side(rows(kp[0], qp[0])), *by_side(rows(kp[1], qp[1])), *by_side(rows(kp[2], qp[2])))
        yield
        top = dot_nn(lanes(lhs, lhs), states(w1_parts, g, pair, 0, 256))
        yield
        low_terms = dot_nn(lhs[:64], states(w1_parts, g, pair, 256, 384))
        yield
        offset = b1[g, pair]
        z_one = sum3(top, 64) + low_terms + rows(rep8(offset[:8], 32), rep8(offset[8:], 32))
        hidden, slope_val = twice_gelu_and_slope(z_one)
        slope[g, pair] = rows(slope_val[:16], slope_val[32:48])
        for tile in range(2):
            act[g, pair, tile] = tile_parts(hidden, tile)
        yield

    def stage_out(g, pair, j, q_step, live):
        acts = lanes(act[g, pair, 0], act[g, pair, 1])
        top = dot_nt(acts, states(w2_parts, g, pair, 0, 256))
        yield
        low_terms = dot_nt(acts[:64], rows(states(w2_parts, g, pair, 256, 384), pad128))
        yield
        total = sum3(top, 64) + low_terms
        total = total[:, :128] + total[:, 128:]
        z_two[g, pair] = jnp.where(low_tall, total[:32], total[32:]) + rep8(b2[g, pair], 32)
        yield

    def stage_center(g, pair, j, q_step, live):
        z_val = z_two[g, pair]
        z_two[g, pair] = z_val - side_sums(z_val) * (1 / 64)
        yield

    def stage_norm(g, pair, j, q_step, live):
        z_val = z_two[g, pair]
        inv_std = lax.rsqrt(side_sums(z_val * z_val) * (1 / 64) + LN_EPS)
        normed = z_val * inv_std
        gain_tile = rep8(gain_pair[pair], 16)
        outs[g, out_rows(q_step, 1), 128 * pair:128 * pair + 128] = (normed[16:] * gain_tile + query_base[g, pair]).astype(bf16)
        key_inv[g, pair] = inv_std[:16]
        key_norm[g, pair] = normed[:16]
        d_norm[g, pair] = (normed[:16] * gain_tile + key_base[g, pair]) * (2.0 * gain_tile)
        yield

    def stage_back(g, pair, j, q_step, live):
        d_val = d_norm[g, pair]
        normed = key_norm[g, pair]
        mean_d = side_sums(d_val) * (1 / 64)
        mean_dn = side_sums(d_val * normed) * (1 / 64)
        d_val = key_inv[g, pair] * (d_val - mean_d - normed * mean_dn)
        d_two[g, pair] = rows(*split3(d_val))
        total = d_val[:8] + d_val[8:]
        for shift in (4, 2, 1):
            total = total + pltpu.roll(total, shift, 0)
        b2[g, pair] = b2[g, pair] - jnp.where(low[:8], live * rate[2 * pair], live * rate[2 * pair + 1]) * total
        yield

    def six_left(parts):
        return rows(parts[0], parts[0], parts[0], parts[1], parts[1], parts[2])

    def six_right(ref, g, pair, height, side):
        at = [part * height + side for part in range(3)]
        term = [lanes(ref[g, pair, 0, a:a + 16], ref[g, pair, 1, a:a + 16]) for a in at]
        return rows(term[0], term[1], term[2], term[0], term[1], term[0])

    def both_rates(first, second):
        return rows(jnp.full((64, 256), first, f32), jnp.full((64, 256), second, f32))

    def stage_second(g, pair, j, q_step, live):
        dp = d_two[g, pair]
        lhs = rows(*by_side(dp[:16]), *by_side(dp[16:32]), *by_side(dp[32:]))
        top = dot_nn(lanes(lhs, lhs), states(w2_parts, g, pair, 0, 256))
        yield
        low_terms = dot_nn(lhs[:32], states(w2_parts, g, pair, 256, 384))
        yield
        d_hidden = (sum3(top, 32) + low_terms) * slope[g, pair]
        for tile in range(2):
            d_one[g, pair, tile] = tile_parts(d_hidden, tile)
        yield

    def stage_second_update(g, pair, j, q_step, live):
        dp = d_two[g, pair]
        turned = six_left([dp[:16], dp[16:32], dp[32:]]).T
        yield
        grads = []
        for side in range(2):
            grads.append(dot_nn(turned[64 * side:64 * side + 64], six_right(act, g, pair, 64, 32 * side)))
            yield
        scale = [0.25 * live * rate[2 * pair + side] for side in range(2)]
        new = w2[g, pair] - both_rates(*scale) * rows(*grads)
        w2[g, pair] = new
        for tile in range(2):
            w2_parts[g, pair, tile] = tile_parts(new, tile)
        yield

    def stage_first_update(g, pair, j, q_step, live):
        turned = key_parts[g, pair].T
        yield
        grads = []
        for side in range(2):
            grads.append(dot_nn(rows(turned[64 * side:64 * side + 64], count_rows), six_right(d_one, g, pair, 32, 16 * side)))
            yield
        scale = [live * rate[2 * pair + side] for side in range(2)]
        new = w1[g, pair] - both_rates(*scale) * rows(grads[0][:64], grads[1][:64])
        w1[g, pair] = new
        for tile in range(2):
            w1_parts[g, pair, tile] = tile_parts(new, tile)
        offset = b1[g, pair]
        b1[g, pair] = rows(offset[:8] - scale[0] * grads[0][64:72], offset[8:] - scale[1] * grads[1][64:72])
        yield

    units = [(g, pair) for g in range(seqs) for pair in range(heads // 2)]
    batches = len(units) // BATCH
    delays = (0, 1, 2, 3, 5, 5, 6, 6)
    stages = {name: (delay, stage) for name, delay, stage in zip('ABMCDEGF', delays, (
        stage_hidden, stage_out, stage_center, stage_norm, stage_back, stage_second, stage_second_update, stage_first_update))}

    def run_turn(turn, step, skip):
        running = {}
        for name in ORDER:
            for unit in range(BATCH):
                delay, stage = stages[name]
                j, batch = divmod(turn - delay, batches)
                if skip(j, delay):
                    continue
                if (name, unit) not in running:
                    g, pair = units[batch * BATCH + unit]
                    running[name, unit] = stage(g, pair, j, jnp.maximum(step + j - 1, 0), jnp.where(step + j >= 0, 1.0, 0.0) if j < 0 else 1.0)
                next(running[name, unit])
        for stage in running.values():
            next(stage, None)

    def body(step, next_turn=None):
        last = next_turn is None
        shift_in()
        projection = iter(()) if last else project(next_turn)
        count = 0
        for turn in range(batches * (1 if last else ahead)):
            run_turn(turn, step, lambda j, delay: last and j >= 0 and delay > 3)
            if count >= PROJECT_FROM and (count - PROJECT_FROM) % PROJECT_EVERY == 0:
                next(projection, None)
            count += 1
        for _ in projection:
            pass

    pass_on(jnp.int32(0))
    pass_on(jnp.int32(1))
    turns = steps // ahead
    half_turns = turns // 2

    def loop_body(turn, carry):
        step = turn * ahead
        pass_on(turn + 2)
        send_far(turn)

        @pl.when(turn <= 1)
        def _():
            wait_tokens(turn)
            for _ in project(turn):
                pass

        @pl.when((turn >= 1) & (turn + 1 < turns))
        def _():
            wait_tokens(turn + 1)

        send_w(turn)

        @pl.when(turn >= 2)
        def _():
            send_row(step - 2 * ahead, ahead)

        @pl.when((turn >= 2) & ((me < 2) | (turn >= half_turns + 2)))
        def _():
            send_across(step - 2 * ahead, ahead)

        @pl.when((turn >= half_turns) & (me >= 2))
        def _():
            send_across(step - half_turns * ahead, ahead)

        body(step, lax.rem(turn + jnp.minimum(turn, 1), turns))
        return carry

    lax.fori_loop(0, turns, loop_body, 0)
    send_row(jnp.int32(steps - 2 * ahead), ahead)
    send_across(jnp.int32(steps - 2 * ahead), ahead)
    body(jnp.int32(steps))
    send_row(jnp.int32(steps - 2), 1)
    send_across(jnp.int32(steps - 2), 1)
    for turn in range(batches, batches + 3):
        run_turn(turn, jnp.int32(steps), lambda j, delay: j != 0 or delay > 3)
    quarter = tok.at[:, tok_rows(0, own_turns)]
    for slot in range(3):
        remote(quarter, quarter, tok_send.at[slot], pass_recv.at[0], heads=other_row).wait_send()
    send_row(jnp.int32(steps - 1), 1)
    send_across(jnp.int32(steps - 1), 1)

    def rows_of(count):
        return outs.at[:, pl.ds(0, count * MINI_BATCH)]

    def done(count, send, recv):
        return remote(rows_of(count), rows_of(count), send, recv, heads=other_row)

    def arrive(late, count):
        pltpu.make_async_copy(rows_of(count), rows_of(count), own_sem.at[late]).wait()
        for place in range(parts_of_seq):
            done(count, out_send.at[0], out_recv.at[other_row, place, late]).wait_recv()

            @pl.when(me != place)
            def _():
                done(count, out_send.at[0], out_recv.at[row_axis, place, late]).wait_recv()

    w_keep.wait()
    w_swap.wait()
    w_load = pltpu.make_async_copy(w_full, w_all, w_own)
    w_load.start()
    arrive(0, early_steps)

    def fetch(block):
        rows_at = pl.ds(two * block, two), pl.ds(0, early_steps * MINI_BATCH)
        return pltpu.make_async_copy(o_full.at[rows_at], o_block.at[lax.rem(block, 2)], o_sem.at[lax.rem(block, 2)])

    def put(block):
        return pltpu.make_async_copy(y_block.at[lax.rem(block, 2)], y_early.at[pl.ds(two * block, two)], y_sem.at[lax.rem(block, 2)])

    two = 2
    blocks = parts_of_seq * seqs // two
    fetch(jnp.int32(0)).start()
    w_load.wait()

    def early_block(block, carry):
        @pl.when(block + 1 < blocks)
        def _():
            fetch(block + 1).start()

        @pl.when(block >= 2)
        def _():
            put(block - 2).wait()

        fetch(block).wait()
        slot = lax.rem(block, 2)
        val = o_block[slot].reshape(two * early_steps * MINI_BATCH, 2 * width)
        for col in range(0, w_all.shape[1], 256):
            y_block[slot, :, :, col:col + 256] = dot_nn(val, w_all[:, col:col + 256]).astype(bf16).reshape(two, early_steps * MINI_BATCH, 256)
        put(block).start()
        return carry

    lax.fori_loop(0, blocks, early_block, 0)
    put(jnp.int32(blocks - 2)).wait()
    put(jnp.int32(blocks - 1)).wait()
    done(steps - own_steps, out_send.at[0], out_recv.at[0, 0, 0]).wait_send()
    done(steps, out_send.at[1], out_recv.at[0, 0, 0]).wait_send()
    arrive(1, own_steps - early_steps)


def late_kernel(y_early, outs, w_full, y_ref, w_all, o_late, y_late, y_kept, in_sem, out_sem, w_sem):
    num_seqs, late = o_late.shape[:2]
    early = y_kept.shape[1]
    group = num_seqs // 4
    early_rows, late_rows = pl.ds(0, early), pl.ds(early, late)
    w_load = pltpu.make_async_copy(w_full, w_all, w_sem)
    w_load.start()

    def some(part):
        return pl.ds(group * part, group)

    late_in = [pltpu.make_async_copy(outs.at[some(i), late_rows], o_late.at[some(i)], in_sem.at[0, i]) for i in range(4)]
    early_in = [pltpu.make_async_copy(y_early.at[some(i)], y_kept.at[some(i)], in_sem.at[1, i]) for i in range(4)]
    late_out = [pltpu.make_async_copy(y_late.at[some(i)], y_ref.at[some(i), late_rows], out_sem.at[0, i]) for i in range(4)]
    early_out = [pltpu.make_async_copy(y_kept.at[some(i)], y_ref.at[some(i), early_rows], out_sem.at[1, i]) for i in range(4)]
    for copy in late_in + early_in:
        copy.start()
    w_load.wait()
    for i in range(4):
        late_in[i].wait()
        val = o_late[some(i)].reshape(group * late, o_late.shape[2])
        for col in range(0, w_all.shape[1], 256):
            y_late[some(i), :, col:col + 256] = dot_nn(val, w_all[:, col:col + 256]).astype(bf16).reshape(group, late, 256)
        early_in[i].wait()
        early_out[i].start()
        late_out[i].start()
    for copy in early_out + late_out:
        copy.wait()


def finish(outs, w_full, y_early):
    num_seqs, own_len, width = outs.shape
    early, model_dim = y_early.shape[1:]
    late = own_len - early
    hbm = pl.BlockSpec(memory_space=pl.ANY)
    dma = pltpu.SemaphoreType.DMA
    return pl.pallas_call(
        late_kernel,
        out_shape=jax.ShapeDtypeStruct((num_seqs, own_len, model_dim), bf16),
        in_specs=[hbm] * 3,
        out_specs=hbm,
        scratch_shapes=[pltpu.VMEM((width, model_dim), bf16), pltpu.VMEM((num_seqs, late, width), bf16), pltpu.VMEM((num_seqs, late, model_dim), bf16),
                        pltpu.VMEM((num_seqs, early, model_dim), bf16), dma((2, 4)), dma((2, 4)), dma],
        compiler_params=pltpu.CompilerParams(vmem_limit_bytes=60 * 2 ** 20),
    )(y_early, outs, w_full)


def run_layer(tokens, theta_k, theta_q, theta_v, w_out, w1, w2t, b1, b2, gain, bias, rate, parts_of_seq):
    num_seqs, own_len, model_dim = tokens.shape
    seqs = num_seqs // parts_of_seq
    steps = own_len * parts_of_seq // MINI_BATCH
    heads = w1.shape[0]
    width = theta_k.shape[1]
    smem = pl.BlockSpec(memory_space=pltpu.SMEM)
    hbm = pl.BlockSpec(memory_space=pl.ANY)
    each = [((128, 256), f32), ((128, 256), f32), ((2, 384, 128), bf16), ((2, 384, 128), bf16), ((16, 256), f32),
            ((2, 192, 128), bf16), ((32, 256), f32), ((2, 96, 128), bf16),
            ((8, 128), f32), ((96, 128), bf16), ((16, 128), f32), ((16, 128), f32), ((32, 128), f32),
            ((16, 128), f32), ((16, 128), f32), ((16, 128), f32), ((48, 128), bf16)]
    scratch = [pltpu.VMEM(val.shape, val.dtype) for val in (theta_k, theta_q, theta_v, w1, w2t, b1, b2, gain, bias)]
    scratch += [pltpu.VMEM((seqs, heads // 2) + shape, dtype) for shape, dtype in each]
    scratch += [pltpu.VMEM((heads // 2, 8, 128), f32)] * 2
    scratch += [pltpu.VMEM((seqs, steps * MINI_BATCH, model_dim), bf16), pltpu.VMEM((seqs, steps * MINI_BATCH, width), bf16)]
    ahead = AHEAD
    several = pltpu.VMEM((ahead, seqs, MINI_BATCH, width), f32)
    scratch += [several] * 3 + [pltpu.VMEM((seqs, MINI_BATCH, width), f32)] + [several] * 3
    own_steps = steps // parts_of_seq
    dma = pltpu.SemaphoreType.DMA
    half_turns = steps // (2 * AHEAD)
    scratch += [dma((9,)), dma((3,)), dma, dma, dma((half_turns,)), dma((half_turns,)), dma((2,)), dma((2, parts_of_seq, 2)), dma((2,)), dma, dma, dma]
    early = 2 * own_len // 3
    scratch += [pltpu.VMEM((2 * width, model_dim), bf16), pltpu.VMEM((2, 2, early, 2 * width), bf16), pltpu.VMEM((2, 2, early, model_dim), bf16), dma((2,)), dma((2,))]
    return pl.pallas_call(
        functools.partial(layer_kernel, steps, seqs, heads, ahead, parts_of_seq),
        out_shape=(jax.ShapeDtypeStruct((num_seqs, own_len, 2 * width), bf16), jax.ShapeDtypeStruct((2 * width, model_dim), bf16),
                   jax.ShapeDtypeStruct((num_seqs, early, model_dim), bf16)),
        in_specs=[hbm] * 11 + [smem],
        out_specs=(hbm, hbm, hbm),
        scratch_shapes=scratch,
        compiler_params=pltpu.CompilerParams(vmem_limit_bytes=60 * 2 ** 20, collective_id=0, has_side_effects=True),
    )(tokens, w_out, theta_k, theta_q, theta_v, w1, w2t, b1, b2, gain, bias, rate)


def solution(mesh):
    parts_of_seq = mesh.shape['seq']

    def local_fn(tokens, theta_q, theta_k, theta_v, w_out, w_one, b_one, w_two, b_two, ln_gain, ln_bias, inner_lr):
        outs, w_full, y_early = run_layer(tokens, theta_k, theta_q, theta_v, w_out, w_one, jnp.swapaxes(w_two, 1, 2), b_one, b_two, ln_gain, ln_bias, inner_lr, parts_of_seq)
        return finish(outs, w_full, y_early)

    arg_specs = (P('data', 'seq', None), P(None, 'heads'), P(None, 'heads'), P(None, 'heads'), P('heads', None), P('heads', None, None), P('heads', None), P('heads', None, None), P('heads', None), P('heads', None), P('heads', None), P('heads'))
    return jax.shard_map(local_fn, mesh=mesh, in_specs=arg_specs, out_specs=P('data', 'seq', None), check_vma=False)
```

```python
import functools

import jax
import jax.numpy as jnp
from jax import lax
from jax.experimental import pallas as pl
from jax.experimental.pallas import tpu as pltpu
from jax.sharding import PartitionSpec as P

MINI_BATCH = 16
AHEAD = 2
BATCH = 2
ORDER = 'MCDGFAABEBAEABEGGGFFF'
PROJECT_EVERY = 1
PROJECT_FROM = 0
FAR0, FAR1, FAR2, PA, WT, P0 = -3, 4, -4, 4, 10, 2
LN_EPS = 1e-6
GELU_C0 = 0.7978845608028654
GELU_C1 = 0.044715
f32 = jnp.float32
bf16 = jnp.bfloat16


def split3(val):
    high = val.astype(bf16)
    rest = val - high.astype(f32)
    mid = rest.astype(bf16)
    return high, mid, (rest - mid.astype(f32)).astype(bf16)


def dot_nn(lhs, rhs):
    return lax.dot_general(lhs, rhs, (((1,), (0,)), ((), ())), preferred_element_type=f32)


def dot_nt(lhs, rhs):
    return lax.dot_general(lhs, rhs, (((1,), (1,)), ((), ())), preferred_element_type=f32)


def dot_tn(lhs, rhs):
    return lax.dot_general(lhs, rhs, (((0,), (0,)), ((), ())), preferred_element_type=f32)


def rows(*parts):
    return jnp.concatenate(parts, 0)


def lanes(*parts):
    return jnp.concatenate(parts, 1)


def rep8(val, count):
    return rows(*([val] * (count // 8)))


def sum3(val, count):
    return val[0:count] + val[count:2 * count] + val[2 * count:3 * count]


def twice_gelu_and_slope(z_val):
    square = z_val * z_val
    tanh_val = jnp.tanh(z_val * (GELU_C0 + (GELU_C0 * GELU_C1) * square))
    plus = 1.0 + tanh_val
    slope = plus + (1.0 - tanh_val * tanh_val) * (z_val * (GELU_C0 + (3 * GELU_C0 * GELU_C1) * square))
    return z_val * plus, slope


def tile_parts(val, tile):
    return rows(*split3(val[:, 128 * tile:128 * tile + 128]))


def eight_rows(row, twice):
    row = lanes(row, row) if twice else row
    return jnp.broadcast_to(row, (8, row.shape[1]))


def layer_kernel(steps, seqs, heads, ahead, parts_of_seq, tokens, w_out, theta_k_at, theta_q_at, theta_v_at, w1_at, w2_at, b1_at, b2_at, gain_at, bias_at, rate_in,
                 o_full, w_full, y_early, theta_k, theta_q, theta_v, w1_in, w2_in,
                 w1, w2, w1_parts, w2_parts, b1, act, slope, d_one, b2, key_parts, key_base, query_base, z_two, key_norm, key_inv, d_norm, d_two, gain_pair, bias_pair,
                 tok, outs, k_now, v_now, q_now, q_last, k_new, v_new, q_new,
                 load_sem, tok_send, own_recv, near_recv, half_recv, pass_recv, out_send, out_recv, own_sem, w_send, w_recv, w_own,
                 w_all, o_block, y_block, o_sem, y_sem, b1_in, b2_in, gain_in, bias_in):
    low = lax.broadcasted_iota(jnp.int32, (16, 128), 1) < 64
    pad128 = jnp.zeros((128, 256), bf16)
    low_tall = lax.broadcasted_iota(jnp.int32, (32, 128), 1) < 64
    count_rows = jnp.where(lax.broadcasted_iota(jnp.int32, (16, 96), 1) < 48, 1.0, 0.0).astype(bf16)
    width = 64 * heads
    own_steps = steps // parts_of_seq
    early_steps = 2 * own_steps // 3
    row_axis = lax.axis_index('heads')
    me = lax.axis_index('seq')
    other_row = 1 - row_axis
    mesh_ids = pl.DeviceIdType.MESH

    def other_core(place):
        return place + 1 - 2 * lax.rem(place, 2)

    near = other_core(me)
    far_a = lax.rem(me + 2, 4)
    far_b = other_core(far_a)

    barrier = pltpu.get_barrier_semaphore()
    for shift_row in range(2):
        for shift in range(parts_of_seq):
            if shift_row or shift:
                pl.semaphore_signal(barrier, inc=1, device_id={'heads': lax.rem(row_axis + shift_row, 2), 'seq': lax.rem(me + shift, parts_of_seq)}, device_id_type=mesh_ids)
    pl.semaphore_wait(barrier, 2 * parts_of_seq - 1)

    half = seqs // 2
    my_half = pl.ds(half * row_axis, half)
    far_from = (1 - me // 2) * (steps // 2)

    def remote(src, dst, send, recv, **device):
        return pltpu.make_async_remote_copy(src, dst, send, recv, device_id=device, device_id_type=mesh_ids)

    pair_rows = ahead * MINI_BATCH
    own_turns = own_steps // ahead
    far_turns = 2 * own_turns
    far_turn = far_turns * (1 - me // 2)

    def tok_rows(turn, count=1):
        return pl.ds(pl.multiple_of(pair_rows * turn, pair_rows), pair_rows * count)

    def send_far(turn):
        piece = turn - FAR0 - FAR1 * me - FAR2 * (me // 2)

        @pl.when((piece >= 0) & (piece < own_turns))
        def _():
            at = me * own_turns + piece
            for dest in (far_a, far_b):
                src = tokens.at[pl.ds(seqs * dest + half * row_axis, half), tok_rows(piece)]
                remote(src, tok.at[my_half, tok_rows(at)], tok_send.at[1], half_recv.at[lax.rem(at, far_turns)], seq=dest).start()

    def is_far(turn):
        return (turn >= far_turn) & (turn < far_turn + far_turns)

    def pass_on(turn):
        @pl.when(is_far(turn))
        def _():
            spot = tok.at[my_half, tok_rows(turn)]
            slot = turn - far_turn
            remote(spot, spot, tok_send.at[2], half_recv.at[slot], heads=other_row).wait_recv()
            remote(spot, spot, tok_send.at[2], pass_recv.at[slot], heads=other_row).start()

    def wait_tokens(turn):
        @pl.when(is_far(turn))
        def _():
            spot = tok.at[my_half, tok_rows(turn)]
            remote(spot, spot, tok_send.at[2], pass_recv.at[turn - far_turn], heads=other_row).wait_recv()

        @pl.when(lax.rem(turn, own_turns) == 0)
        def _():
            spot = tok.at[:, tok_rows(turn, own_turns)]

            @pl.when(turn // own_turns == me)
            def _():
                pltpu.make_async_copy(spot, spot, own_recv).wait()

            @pl.when(turn // own_turns == near)
            def _():
                remote(spot, spot, tok_send.at[0], near_recv, seq=near).wait_recv()

    for turn in range(FAR0, 0):
        send_far(jnp.int32(turn))
    own_block = tok.at[:, tok_rows(me * own_turns, own_turns)]
    pltpu.make_async_copy(tokens.at[pl.ds(seqs * me, seqs)], own_block, own_recv).start()
    remote(tokens.at[pl.ds(seqs * near, seqs)], own_block, tok_send.at[0], near_recv, seq=near).start()
    loads = [pltpu.make_async_copy(src, dst, load_sem.at[i]) for i, (src, dst) in enumerate((
        (w1_at, w1_in), (w2_at, w2_in), (b1_at, b1_in), (b2_at, b2_in), (gain_at, gain_in), (bias_at, bias_in),
        (theta_k_at, theta_k), (theta_q_at, theta_q), (theta_v_at, theta_v)))]
    for load in loads:
        load.start()

    my_w_rows = w_full.at[pl.ds(pl.multiple_of(row_axis * width, width), width)]
    w_swap = pltpu.make_async_remote_copy(w_out, my_w_rows, w_send, w_recv, device_id={'heads': other_row}, device_id_type=mesh_ids)
    w_keep = pltpu.make_async_copy(w_out, my_w_rows, w_own)
    w_keep.start()

    @pl.when(me < 2)
    def _():
        w_swap.start()

    def out_rows(step, count):
        return pl.ds(pl.multiple_of(MINI_BATCH * step, MINI_BATCH), MINI_BATCH * count)

    def out_copy(step, count):
        place = pl.ds(seqs * me, seqs), out_rows(lax.rem(step, own_steps), count), pl.ds(pl.multiple_of(width * row_axis, width), width)
        late = (lax.rem(step, own_steps) >= early_steps).astype(jnp.int32)
        return outs.at[:, out_rows(step, count)], o_full.at[place], step // own_steps, late

    def send_row(step, count):
        src, dst, owner, late = out_copy(step, count)

        @pl.when(owner != me)
        def _():
            remote(src, dst, out_send.at[0], out_recv.at[row_axis, me, late], seq=owner).start()

        @pl.when(owner == me)
        def _():
            pltpu.make_async_copy(src, dst, own_sem.at[late]).start()

    def send_across(step, count):
        src, dst, owner, late = out_copy(step, count)
        remote(src, dst, out_send.at[1], out_recv.at[row_axis, me, late], heads=other_row, seq=owner).start()

    for load in loads:
        load.wait()
    for pair in range(heads // 2):
        even, odd = 2 * pair, 2 * pair + 1

        def pair_row(source):
            return jnp.broadcast_to(lanes(source[even:even + 1], source[odd:odd + 1]), (8, 128))

        gain_pair[pair] = pair_row(gain_in)
        bias_pair[pair] = pair_row(bias_in)
        offset = pair_row(b2_in)
        hidden_offset = rows(eight_rows(b1_in[even:even + 1], False), eight_rows(b1_in[odd:odd + 1], False))
        first = rows(w1_in[even], w1_in[odd])
        second = rows(0.5 * w2_in[even], 0.5 * w2_in[odd])
        for g in range(seqs):
            w1[g, pair] = first
            w2[g, pair] = second
            b1[g, pair] = hidden_offset
            b2[g, pair] = offset
        for tile in range(2):
            first_parts, second_parts = tile_parts(first, tile), tile_parts(second, tile)
            for g in range(seqs):
                w1_parts[g, pair, tile] = first_parts
                w2_parts[g, pair, tile] = second_parts
    q_last[...] = jnp.zeros(q_last.shape, f32)

    @pl.loop(0, seqs)
    def _(g):
        for ref in (act, slope, d_one, key_parts, key_base, query_base, z_two, key_norm, key_inv, d_norm, d_two):
            ref[g] = jnp.zeros(ref.shape[1:], ref.dtype)

    rate = [rate_in[h] * (1 / MINI_BATCH) for h in range(heads)]

    def both(unit):
        return [2 * pair + side for pair in unit for side in range(2)]

    def project(turn):
        for theta, target in ((theta_k, k_new), (theta_q, q_new), (theta_v, v_new)):
            for col in range(0, width, 256):
                toks = tok[:, tok_rows(turn)].reshape(seqs * pair_rows, tok.shape[2])
                found = dot_nn(toks, theta[:, col:col + 256]).reshape(seqs, ahead, MINI_BATCH, 256)
                for j in range(ahead):
                    target[j, :, :, col:col + 256] = found[:, j]
                yield

    def shift_in():
        k_now[...] = k_new[...]
        v_now[...] = v_new[...]
        q_now[0] = q_last[...]
        for j in range(1, ahead):
            q_now[j] = q_new[j - 1]
        q_last[...] = q_new[ahead - 1]

    def states(ref, g, pair, first, last):
        return lanes(ref[g, pair, 0, first:last], ref[g, pair, 1, first:last])

    def by_side(val):
        keep = lax.broadcasted_iota(jnp.int32, val.shape, 1) < 64
        zero = jnp.zeros(val.shape, val.dtype)
        return [jnp.where(keep, val, zero), jnp.where(keep, zero, val)]

    def side_sums(val):
        keep = low if val.shape[0] == 16 else low_tall
        return jnp.where(keep, jnp.sum(jnp.where(keep, val, 0.0), 1, keepdims=True), jnp.sum(jnp.where(keep, 0.0, val), 1, keepdims=True))

    def stage_hidden(g, pair, j, q_step, live):
        cols = slice(128 * pair, 128 * pair + 128)
        key_tile = k_now[j, g, :, cols]
        query_tile = q_now[j, g, :, cols]
        bias_tile = rep8(bias_pair[pair], 16)
        query_base[g, pair] = query_tile + bias_tile
        key_base[g, pair] = (key_tile + bias_tile) - v_now[j, g, :, cols]
        kp = split3(key_tile)
        qp = split3(query_tile)
        key_parts[g, pair] = six_left(kp)
        lhs = rows(*by_side(rows(kp[0], qp[0])), *by_side(rows(kp[1], qp[1])), *by_side(rows(kp[2], qp[2])))
        yield
        top = dot_nn(lanes(lhs, lhs), states(w1_parts, g, pair, 0, 256))
        yield
        low_terms = dot_nn(lhs[:64], states(w1_parts, g, pair, 256, 384))
        yield
        offset = b1[g, pair]
        z_one = sum3(top, 64) + low_terms + rows(rep8(offset[:8], 32), rep8(offset[8:], 32))
        hidden, slope_val = twice_gelu_and_slope(z_one)
        slope[g, pair] = rows(slope_val[:16], slope_val[32:48])
        for tile in range(2):
            act[g, pair, tile] = tile_parts(hidden, tile)
        yield

    def stage_out(g, pair, j, q_step, live):
        acts = lanes(act[g, pair, 0], act[g, pair, 1])
        top = dot_nt(acts, states(w2_parts, g, pair, 0, 256))
        yield
        low_terms = dot_nt(acts[:64], rows(states(w2_parts, g, pair, 256, 384), pad128))
        yield
        total = sum3(top, 64) + low_terms
        total = total[:, :128] + total[:, 128:]
        z_two[g, pair] = jnp.where(low_tall, total[:32], total[32:]) + rep8(b2[g, pair], 32)
        yield

    def stage_center(g, pair, j, q_step, live):
        z_val = z_two[g, pair]
        z_two[g, pair] = z_val - side_sums(z_val) * (1 / 64)
        yield

    def stage_norm(g, pair, j, q_step, live):
        z_val = z_two[g, pair]
        inv_std = lax.rsqrt(side_sums(z_val * z_val) * (1 / 64) + LN_EPS)
        normed = z_val * inv_std
        gain_tile = rep8(gain_pair[pair], 16)
        outs[g, out_rows(q_step, 1), 128 * pair:128 * pair + 128] = (normed[16:] * gain_tile + query_base[g, pair]).astype(bf16)
        key_inv[g, pair] = inv_std[:16]
        key_norm[g, pair] = normed[:16]
        d_norm[g, pair] = (normed[:16] * gain_tile + key_base[g, pair]) * (2.0 * gain_tile)
        yield

    def stage_back(g, pair, j, q_step, live):
        d_val = d_norm[g, pair]
        normed = key_norm[g, pair]
        mean_d = side_sums(d_val) * (1 / 64)
        mean_dn = side_sums(d_val * normed) * (1 / 64)
        d_val = key_inv[g, pair] * (d_val - mean_d - normed * mean_dn)
        d_two[g, pair] = rows(*split3(d_val))
        total = d_val[:8] + d_val[8:]
        for shift in (4, 2, 1):
            total = total + pltpu.roll(total, shift, 0)
        b2[g, pair] = b2[g, pair] - jnp.where(low[:8], live * rate[2 * pair], live * rate[2 * pair + 1]) * total
        yield

    def six_left(parts):
        return rows(parts[0], parts[0], parts[0], parts[1], parts[1], parts[2])

    def six_right(ref, g, pair, height, side):
        at = [part * height + side for part in range(3)]
        term = [lanes(ref[g, pair, 0, a:a + 16], ref[g, pair, 1, a:a + 16]) for a in at]
        return rows(term[0], term[1], term[2], term[0], term[1], term[0])

    def both_rates(first, second):
        return rows(jnp.full((64, 256), first, f32), jnp.full((64, 256), second, f32))

    def stage_second(g, pair, j, q_step, live):
        dp = d_two[g, pair]
        lhs = rows(*by_side(dp[:16]), *by_side(dp[16:32]), *by_side(dp[32:]))
        top = dot_nn(lanes(lhs, lhs), states(w2_parts, g, pair, 0, 256))
        yield
        low_terms = dot_nn(lhs[:32], states(w2_parts, g, pair, 256, 384))
        yield
        d_hidden = (sum3(top, 32) + low_terms) * slope[g, pair]
        for tile in range(2):
            d_one[g, pair, tile] = tile_parts(d_hidden, tile)
        yield

    def stage_second_update(g, pair, j, q_step, live):
        dp = d_two[g, pair]
        turned = six_left([dp[:16], dp[16:32], dp[32:]]).T
        yield
        grads = []
        for side in range(2):
            grads.append(dot_nn(turned[64 * side:64 * side + 64], six_right(act, g, pair, 64, 32 * side)))
            yield
        scale = [0.25 * live * rate[2 * pair + side] for side in range(2)]
        new = w2[g, pair] - both_rates(*scale) * rows(*grads)
        w2[g, pair] = new
        for tile in range(2):
            w2_parts[g, pair, tile] = tile_parts(new, tile)
        yield

    def stage_first_update(g, pair, j, q_step, live):
        turned = key_parts[g, pair].T
        yield
        grads = []
        for side in range(2):
            grads.append(dot_nn(rows(turned[64 * side:64 * side + 64], count_rows), six_right(d_one, g, pair, 32, 16 * side)))
            yield
        scale = [live * rate[2 * pair + side] for side in range(2)]
        new = w1[g, pair] - both_rates(*scale) * rows(grads[0][:64], grads[1][:64])
        w1[g, pair] = new
        for tile in range(2):
            w1_parts[g, pair, tile] = tile_parts(new, tile)
        offset = b1[g, pair]
        b1[g, pair] = rows(offset[:8] - scale[0] * grads[0][64:72], offset[8:] - scale[1] * grads[1][64:72])
        yield

    units = [(g, pair) for g in range(seqs) for pair in range(heads // 2)]
    batches = len(units) // BATCH
    delays = (0, 1, 2, 3, 5, 5, 6, 6)
    stages = {name: (delay, stage) for name, delay, stage in zip('ABMCDEGF', delays, (
        stage_hidden, stage_out, stage_center, stage_norm, stage_back, stage_second, stage_second_update, stage_first_update))}

    def run_turn(turn, step, skip):
        running = {}
        for name in ORDER:
            for unit in range(BATCH):
                delay, stage = stages[name]
                j, batch = divmod(turn - delay, batches)
                if skip(j, delay):
                    continue
                if (name, unit) not in running:
                    g, pair = units[batch * BATCH + unit]
                    running[name, unit] = stage(g, pair, j, jnp.maximum(step + j - 1, 0), jnp.where(step + j >= 0, 1.0, 0.0) if j < 0 else 1.0)
                next(running[name, unit])
        for stage in running.values():
            next(stage, None)

    def body(step, next_turn=None):
        last = next_turn is None
        shift_in()
        projection = iter(()) if last else project(next_turn)
        count = 0
        for turn in range(batches * (1 if last else ahead)):
            run_turn(turn, step, lambda j, delay: last and j >= 0 and delay > 3)
            if count >= PROJECT_FROM and (count - PROJECT_FROM) % PROJECT_EVERY == 0:
                next(projection, None)
            count += 1
        for _ in projection:
            pass

    for turn in range(P0):
        pass_on(jnp.int32(turn))
    turns = steps // ahead
    half_turns = turns // 2

    def loop_body(turn, carry):
        step = turn * ahead
        pass_on(turn + P0 + PA * (1 - me // 2))
        send_far(turn)

        @pl.when(turn <= 1)
        def _():
            wait_tokens(turn)
            for _ in project(turn):
                pass

        @pl.when((turn >= 1) & (turn + 1 < turns))
        def _():
            wait_tokens(turn + 1)

        @pl.when((me >= 2) & (turn == WT))
        def _():
            w_swap.start()

        @pl.when(turn >= 2)
        def _():
            send_row(step - 2 * ahead, ahead)

        @pl.when((turn >= 2) & ((me < 2) | (turn >= half_turns + 2)))
        def _():
            send_across(step - 2 * ahead, ahead)

        @pl.when((turn >= half_turns) & (me >= 2))
        def _():
            send_across(step - half_turns * ahead, ahead)

        body(step, lax.rem(turn + jnp.minimum(turn, 1), turns))
        return carry

    lax.fori_loop(0, turns, loop_body, 0)
    send_row(jnp.int32(steps - 2 * ahead), ahead)
    send_across(jnp.int32(steps - 2 * ahead), ahead)
    body(jnp.int32(steps))
    send_row(jnp.int32(steps - 2), 1)
    send_across(jnp.int32(steps - 2), 1)
    for turn in range(batches, batches + 3):
        run_turn(turn, jnp.int32(steps), lambda j, delay: j != 0 or delay > 3)
    quarter = tok.at[:, tok_rows(0, own_turns)]
    for slot in range(3):
        remote(quarter, quarter, tok_send.at[slot], pass_recv.at[0], heads=other_row).wait_send()
    send_row(jnp.int32(steps - 1), 1)
    send_across(jnp.int32(steps - 1), 1)

    def rows_of(count):
        return outs.at[:, pl.ds(0, count * MINI_BATCH)]

    def done(count, send, recv):
        return remote(rows_of(count), rows_of(count), send, recv, heads=other_row)

    def arrive(late, count):
        pltpu.make_async_copy(rows_of(count), rows_of(count), own_sem.at[late]).wait()
        for place in range(parts_of_seq):
            done(count, out_send.at[0], out_recv.at[other_row, place, late]).wait_recv()

            @pl.when(me != place)
            def _():
                done(count, out_send.at[0], out_recv.at[row_axis, place, late]).wait_recv()

    w_keep.wait()
    w_swap.wait()
    w_load = pltpu.make_async_copy(w_full, w_all, w_own)
    w_load.start()
    arrive(0, early_steps)

    def fetch(block):
        rows_at = pl.ds(two * block, two), pl.ds(0, early_steps * MINI_BATCH)
        return pltpu.make_async_copy(o_full.at[rows_at], o_block.at[lax.rem(block, 2)], o_sem.at[lax.rem(block, 2)])

    def put(block):
        return pltpu.make_async_copy(y_block.at[lax.rem(block, 2)], y_early.at[pl.ds(two * block, two)], y_sem.at[lax.rem(block, 2)])

    two = 2
    blocks = parts_of_seq * seqs // two
    fetch(jnp.int32(0)).start()
    w_load.wait()

    def early_block(block, carry):
        @pl.when(block + 1 < blocks)
        def _():
            fetch(block + 1).start()

        @pl.when(block >= 2)
        def _():
            put(block - 2).wait()

        fetch(block).wait()
        slot = lax.rem(block, 2)
        val = o_block[slot].reshape(two * early_steps * MINI_BATCH, 2 * width)
        for col in range(0, w_all.shape[1], 256):
            y_block[slot, :, :, col:col + 256] = dot_nn(val, w_all[:, col:col + 256]).astype(bf16).reshape(two, early_steps * MINI_BATCH, 256)
        put(block).start()
        return carry

    lax.fori_loop(0, blocks, early_block, 0)
    put(jnp.int32(blocks - 2)).wait()
    put(jnp.int32(blocks - 1)).wait()
    done(steps - own_steps, out_send.at[0], out_recv.at[0, 0, 0]).wait_send()
    done(steps, out_send.at[1], out_recv.at[0, 0, 0]).wait_send()
    arrive(1, own_steps - early_steps)


def late_kernel(y_early, outs, w_full, y_ref, w_all, o_late, y_late, y_kept, in_sem, out_sem, w_sem):
    num_seqs, late = o_late.shape[:2]
    early = y_kept.shape[1]
    group = num_seqs // 4
    early_rows, late_rows = pl.ds(0, early), pl.ds(early, late)
    w_load = pltpu.make_async_copy(w_full, w_all, w_sem)
    w_load.start()

    def some(part):
        return pl.ds(group * part, group)

    late_in = [pltpu.make_async_copy(outs.at[some(i), late_rows], o_late.at[some(i)], in_sem.at[0, i]) for i in range(4)]
    early_in = [pltpu.make_async_copy(y_early.at[some(i)], y_kept.at[some(i)], in_sem.at[1, i]) for i in range(4)]
    late_out = [pltpu.make_async_copy(y_late.at[some(i)], y_ref.at[some(i), late_rows], out_sem.at[0, i]) for i in range(4)]
    early_out = [pltpu.make_async_copy(y_kept.at[some(i)], y_ref.at[some(i), early_rows], out_sem.at[1, i]) for i in range(4)]
    for copy in late_in + early_in:
        copy.start()
    w_load.wait()
    for i in range(4):
        late_in[i].wait()
        val = o_late[some(i)].reshape(group * late, o_late.shape[2])
        for col in range(0, w_all.shape[1], 256):
            y_late[some(i), :, col:col + 256] = dot_nn(val, w_all[:, col:col + 256]).astype(bf16).reshape(group, late, 256)
        early_in[i].wait()
        early_out[i].start()
        late_out[i].start()
    for copy in early_out + late_out:
        copy.wait()


def finish(outs, w_full, y_early):
    num_seqs, own_len, width = outs.shape
    early, model_dim = y_early.shape[1:]
    late = own_len - early
    hbm = pl.BlockSpec(memory_space=pl.ANY)
    dma = pltpu.SemaphoreType.DMA
    return pl.pallas_call(
        late_kernel,
        out_shape=jax.ShapeDtypeStruct((num_seqs, own_len, model_dim), bf16),
        in_specs=[hbm] * 3,
        out_specs=hbm,
        scratch_shapes=[pltpu.VMEM((width, model_dim), bf16), pltpu.VMEM((num_seqs, late, width), bf16), pltpu.VMEM((num_seqs, late, model_dim), bf16),
                        pltpu.VMEM((num_seqs, early, model_dim), bf16), dma((2, 4)), dma((2, 4)), dma],
        compiler_params=pltpu.CompilerParams(vmem_limit_bytes=60 * 2 ** 20),
    )(y_early, outs, w_full)


def run_layer(tokens, theta_k, theta_q, theta_v, w_out, w1, w2t, b1, b2, gain, bias, rate, parts_of_seq):
    num_seqs, own_len, model_dim = tokens.shape
    seqs = num_seqs // parts_of_seq
    steps = own_len * parts_of_seq // MINI_BATCH
    heads = w1.shape[0]
    width = theta_k.shape[1]
    smem = pl.BlockSpec(memory_space=pltpu.SMEM)
    hbm = pl.BlockSpec(memory_space=pl.ANY)
    each = [((128, 256), f32), ((128, 256), f32), ((2, 384, 128), bf16), ((2, 384, 128), bf16), ((16, 256), f32),
            ((2, 192, 128), bf16), ((32, 256), f32), ((2, 96, 128), bf16),
            ((8, 128), f32), ((96, 128), bf16), ((16, 128), f32), ((16, 128), f32), ((32, 128), f32),
            ((16, 128), f32), ((16, 128), f32), ((16, 128), f32), ((48, 128), bf16)]
    scratch = [pltpu.VMEM(val.shape, val.dtype) for val in (theta_k, theta_q, theta_v, w1, w2t)]
    scratch += [pltpu.VMEM((seqs, heads // 2) + shape, dtype) for shape, dtype in each]
    scratch += [pltpu.VMEM((heads // 2, 8, 128), f32)] * 2
    scratch += [pltpu.VMEM((seqs, steps * MINI_BATCH, model_dim), bf16), pltpu.VMEM((seqs, steps * MINI_BATCH, width), bf16)]
    ahead = AHEAD
    several = pltpu.VMEM((ahead, seqs, MINI_BATCH, width), f32)
    scratch += [several] * 3 + [pltpu.VMEM((seqs, MINI_BATCH, width), f32)] + [several] * 3
    own_steps = steps // parts_of_seq
    dma = pltpu.SemaphoreType.DMA
    half_turns = steps // (2 * AHEAD)
    scratch += [dma((9,)), dma((3,)), dma, dma, dma((half_turns,)), dma((half_turns,)), dma((2,)), dma((2, parts_of_seq, 2)), dma((2,)), dma, dma, dma]
    early = 2 * own_len // 3
    scratch += [pltpu.VMEM((2 * width, model_dim), bf16), pltpu.VMEM((2, 2, early, 2 * width), bf16), pltpu.VMEM((2, 2, early, model_dim), bf16), dma((2,)), dma((2,))]
    scratch += [pltpu.VMEM(val.shape, val.dtype) for val in (b1, b2, gain, bias)]
    return pl.pallas_call(
        functools.partial(layer_kernel, steps, seqs, heads, ahead, parts_of_seq),
        out_shape=(jax.ShapeDtypeStruct((num_seqs, own_len, 2 * width), bf16), jax.ShapeDtypeStruct((2 * width, model_dim), bf16),
                   jax.ShapeDtypeStruct((num_seqs, early, model_dim), bf16)),
        in_specs=[hbm] * 11 + [smem],
        out_specs=(hbm, hbm, hbm),
        scratch_shapes=scratch,
        compiler_params=pltpu.CompilerParams(vmem_limit_bytes=60 * 2 ** 20, collective_id=0, has_side_effects=True),
    )(tokens, w_out, theta_k, theta_q, theta_v, w1, w2t, b1, b2, gain, bias, rate)


def solution(mesh):
    parts_of_seq = mesh.shape['seq']

    def local_fn(tokens, theta_q, theta_k, theta_v, w_out, w_one, b_one, w_two, b_two, ln_gain, ln_bias, inner_lr):
        outs, w_full, y_early = run_layer(tokens, theta_k, theta_q, theta_v, w_out, w_one, jnp.swapaxes(w_two, 1, 2), b_one, b_two, ln_gain, ln_bias, inner_lr, parts_of_seq)
        return finish(outs, w_full, y_early)

    arg_specs = (P('data', 'seq', None), P(None, 'heads'), P(None, 'heads'), P(None, 'heads'), P('heads', None), P('heads', None, None), P('heads', None), P('heads', None, None), P('heads', None), P('heads', None), P('heads', None), P('heads'))
    return jax.shard_map(local_fn, mesh=mesh, in_specs=arg_specs, out_specs=P('data', 'seq', None), check_vma=False)
```

```python
import functools

import jax
import jax.numpy as jnp
from jax import lax
from jax.experimental import pallas as pl
from jax.experimental.pallas import tpu as pltpu
from jax.sharding import PartitionSpec as P

MINI_BATCH = 16
AHEAD = 2
BATCH = 2
ORDER = 'MCDGFAABEBAEABEGGGFFF'
PROJECT_EVERY = 1
PROJECT_FROM = 0
FAR0, FAR1, FAR2, PA, WT, P0 = -3, 6, -9, 5, 10, 2
WHOLE = 2
LN_EPS = 1e-6
GELU_C0 = 0.7978845608028654
GELU_C1 = 0.044715
f32 = jnp.float32
bf16 = jnp.bfloat16


def split3(val):
    high = val.astype(bf16)
    rest = val - high.astype(f32)
    mid = rest.astype(bf16)
    return high, mid, (rest - mid.astype(f32)).astype(bf16)


def dot_nn(lhs, rhs):
    return lax.dot_general(lhs, rhs, (((1,), (0,)), ((), ())), preferred_element_type=f32)


def dot_nt(lhs, rhs):
    return lax.dot_general(lhs, rhs, (((1,), (1,)), ((), ())), preferred_element_type=f32)


def dot_tn(lhs, rhs):
    return lax.dot_general(lhs, rhs, (((0,), (0,)), ((), ())), preferred_element_type=f32)


def rows(*parts):
    return jnp.concatenate(parts, 0)


def lanes(*parts):
    return jnp.concatenate(parts, 1)


def rep8(val, count):
    return rows(*([val] * (count // 8)))


def sum3(val, count):
    return val[0:count] + val[count:2 * count] + val[2 * count:3 * count]


def twice_gelu_and_slope(z_val):
    square = z_val * z_val
    tanh_val = jnp.tanh(z_val * (GELU_C0 + (GELU_C0 * GELU_C1) * square))
    plus = 1.0 + tanh_val
    slope = plus + (1.0 - tanh_val * tanh_val) * (z_val * (GELU_C0 + (3 * GELU_C0 * GELU_C1) * square))
    return z_val * plus, slope


def tile_parts(val, tile):
    return rows(*split3(val[:, 128 * tile:128 * tile + 128]))


def eight_rows(row, twice):
    row = lanes(row, row) if twice else row
    return jnp.broadcast_to(row, (8, row.shape[1]))


def layer_kernel(steps, seqs, heads, ahead, parts_of_seq, tokens, w_out, theta_k_at, theta_q_at, theta_v_at, w1_at, w2_at, b1_at, b2_at, gain_at, bias_at, rate_in,
                 o_full, w_full, y_early, theta_k, theta_q, theta_v, w1_in, w2_in,
                 w1, w2, w1_parts, w2_parts, b1, act, slope, d_one, b2, key_parts, key_base, query_base, z_two, key_norm, key_inv, d_norm, d_two, gain_pair, bias_pair,
                 tok, outs, k_now, v_now, q_now, q_last, k_new, v_new, q_new,
                 load_sem, tok_send, own_recv, near_recv, half_recv, pass_recv, whole_recv, out_send, out_recv, own_sem, w_send, w_recv, w_own,
                 w_all, o_block, y_block, o_sem, y_sem, b1_in, b2_in, gain_in, bias_in):
    low = lax.broadcasted_iota(jnp.int32, (16, 128), 1) < 64
    pad128 = jnp.zeros((128, 256), bf16)
    low_tall = lax.broadcasted_iota(jnp.int32, (32, 128), 1) < 64
    count_rows = jnp.where(lax.broadcasted_iota(jnp.int32, (16, 96), 1) < 48, 1.0, 0.0).astype(bf16)
    width = 64 * heads
    own_steps = steps // parts_of_seq
    early_steps = 2 * own_steps // 3
    row_axis = lax.axis_index('heads')
    me = lax.axis_index('seq')
    other_row = 1 - row_axis
    mesh_ids = pl.DeviceIdType.MESH

    def other_core(place):
        return place + 1 - 2 * lax.rem(place, 2)

    near = other_core(me)

    barrier = pltpu.get_barrier_semaphore()
    for shift_row in range(2):
        for shift in range(parts_of_seq):
            if shift_row or shift:
                pl.semaphore_signal(barrier, inc=1, device_id={'heads': lax.rem(row_axis + shift_row, 2), 'seq': lax.rem(me + shift, parts_of_seq)}, device_id_type=mesh_ids)
    pl.semaphore_wait(barrier, 2 * parts_of_seq - 1)

    half = seqs // 2
    my_half = pl.ds(half * row_axis, half)
    far_from = (1 - me // 2) * (steps // 2)

    def remote(src, dst, send, recv, **device):
        return pltpu.make_async_remote_copy(src, dst, send, recv, device_id=device, device_id_type=mesh_ids)

    pair_rows = ahead * MINI_BATCH
    own_turns = own_steps // ahead
    far_turns = 2 * own_turns
    far_turn = far_turns * (1 - me // 2)

    def tok_rows(turn, count=1):
        return pl.ds(pl.multiple_of(pair_rows * turn, pair_rows), pair_rows * count)

    def is_whole(turn):
        return (turn >= WHOLE) & (turn < WHOLE + 2)

    def send_far(turn):
        piece = turn - FAR0 - FAR1 * me - FAR2 * (me // 2)

        @pl.when((piece >= 0) & (piece < own_turns))
        def _():
            at = me * own_turns + piece
            whole = is_whole(at)

            @pl.loop(0, 2)
            def _(core):
                dest = 2 * (1 - me // 2) + core

                @pl.when(whole)
                def _():
                    src = tokens.at[pl.ds(seqs * dest, seqs), tok_rows(piece)]
                    remote(src, tok.at[:, tok_rows(at)], tok_send.at[1], whole_recv.at[at - WHOLE], seq=dest).start()

                @pl.when(jnp.logical_not(whole))
                def _():
                    src = tokens.at[pl.ds(seqs * dest + half * row_axis, half), tok_rows(piece)]
                    remote(src, tok.at[my_half, tok_rows(at)], tok_send.at[1], half_recv.at[lax.rem(at, far_turns)], seq=dest).start()

    def is_far(turn):
        return (turn >= far_turn) & (turn < far_turn + far_turns)

    def pass_on(turn):
        @pl.when(is_far(turn) & jnp.logical_not(is_whole(turn)))
        def _():
            spot = tok.at[my_half, tok_rows(turn)]
            slot = turn - far_turn
            remote(spot, spot, tok_send.at[2], half_recv.at[slot], heads=other_row).wait_recv()
            remote(spot, spot, tok_send.at[2], pass_recv.at[slot], heads=other_row).start()

    def wait_tokens(turn):
        @pl.when(is_far(turn) & is_whole(turn))
        def _():
            spot = tok.at[:, tok_rows(turn)]
            remote(spot, spot, tok_send.at[1], whole_recv.at[turn - WHOLE], heads=other_row).wait_recv()

        @pl.when(is_far(turn) & jnp.logical_not(is_whole(turn)))
        def _():
            spot = tok.at[my_half, tok_rows(turn)]
            remote(spot, spot, tok_send.at[2], pass_recv.at[turn - far_turn], heads=other_row).wait_recv()

        @pl.when(lax.rem(turn, own_turns) == 0)
        def _():
            spot = tok.at[:, tok_rows(turn, own_turns)]

            @pl.when(turn // own_turns == me)
            def _():
                pltpu.make_async_copy(spot, spot, own_recv).wait()

            @pl.when(turn // own_turns == near)
            def _():
                remote(spot, spot, tok_send.at[0], near_recv, seq=near).wait_recv()

    for turn in range(FAR0, 0):
        send_far(jnp.int32(turn))
    own_block = tok.at[:, tok_rows(me * own_turns, own_turns)]
    pltpu.make_async_copy(tokens.at[pl.ds(seqs * me, seqs)], own_block, own_recv).start()
    remote(tokens.at[pl.ds(seqs * near, seqs)], own_block, tok_send.at[0], near_recv, seq=near).start()
    loads = [pltpu.make_async_copy(src, dst, load_sem.at[i]) for i, (src, dst) in enumerate((
        (w1_at, w1_in), (w2_at, w2_in), (b1_at, b1_in), (b2_at, b2_in), (gain_at, gain_in), (bias_at, bias_in),
        (theta_k_at, theta_k), (theta_q_at, theta_q), (theta_v_at, theta_v)))]
    for load in loads:
        load.start()

    my_w_rows = w_full.at[pl.ds(pl.multiple_of(row_axis * width, width), width)]
    w_swap = pltpu.make_async_remote_copy(w_out, my_w_rows, w_send, w_recv, device_id={'heads': other_row}, device_id_type=mesh_ids)
    w_keep = pltpu.make_async_copy(w_out, my_w_rows, w_own)
    w_keep.start()

    @pl.when(me < 2)
    def _():
        w_swap.start()

    def out_rows(step, count):
        return pl.ds(pl.multiple_of(MINI_BATCH * step, MINI_BATCH), MINI_BATCH * count)

    def out_copy(step, count):
        place = pl.ds(seqs * me, seqs), out_rows(lax.rem(step, own_steps), count), pl.ds(pl.multiple_of(width * row_axis, width), width)
        late = (lax.rem(step, own_steps) >= early_steps).astype(jnp.int32)
        return outs.at[:, out_rows(step, count)], o_full.at[place], step // own_steps, late

    def send_row(step, count):
        src, dst, owner, late = out_copy(step, count)

        @pl.when(owner != me)
        def _():
            remote(src, dst, out_send.at[0], out_recv.at[row_axis, me, late], seq=owner).start()

        @pl.when(owner == me)
        def _():
            pltpu.make_async_copy(src, dst, own_sem.at[late]).start()

    def send_across(step, count):
        src, dst, owner, late = out_copy(step, count)
        remote(src, dst, out_send.at[1], out_recv.at[row_axis, me, late], heads=other_row, seq=owner).start()

    for load in loads:
        load.wait()
    for pair in range(heads // 2):
        even, odd = 2 * pair, 2 * pair + 1

        def pair_row(source):
            return jnp.broadcast_to(lanes(source[even:even + 1], source[odd:odd + 1]), (8, 128))

        gain_pair[pair] = pair_row(gain_in)
        bias_pair[pair] = pair_row(bias_in)
        offset = pair_row(b2_in)
        hidden_offset = rows(eight_rows(b1_in[even:even + 1], False), eight_rows(b1_in[odd:odd + 1], False))
        first = rows(w1_in[even], w1_in[odd])
        second = rows(0.5 * w2_in[even], 0.5 * w2_in[odd])
        for g in range(seqs):
            w1[g, pair] = first
            w2[g, pair] = second
            b1[g, pair] = hidden_offset
            b2[g, pair] = offset
        for tile in range(2):
            first_parts, second_parts = tile_parts(first, tile), tile_parts(second, tile)
            for g in range(seqs):
                w1_parts[g, pair, tile] = first_parts
                w2_parts[g, pair, tile] = second_parts
    q_last[...] = jnp.zeros(q_last.shape, f32)

    @pl.loop(0, seqs)
    def _(g):
        for ref in (act, slope, d_one, key_parts, key_base, query_base, z_two, key_norm, key_inv, d_norm, d_two):
            ref[g] = jnp.zeros(ref.shape[1:], ref.dtype)

    rate = [rate_in[h] * (1 / MINI_BATCH) for h in range(heads)]

    def both(unit):
        return [2 * pair + side for pair in unit for side in range(2)]

    def project(turn):
        for theta, target in ((theta_k, k_new), (theta_q, q_new), (theta_v, v_new)):
            for col in range(0, width, 256):
                toks = tok[:, tok_rows(turn)].reshape(seqs * pair_rows, tok.shape[2])
                found = dot_nn(toks, theta[:, col:col + 256]).reshape(seqs, ahead, MINI_BATCH, 256)
                for j in range(ahead):
                    target[j, :, :, col:col + 256] = found[:, j]
                yield

    def shift_in():
        k_now[...] = k_new[...]
        v_now[...] = v_new[...]
        q_now[0] = q_last[...]
        for j in range(1, ahead):
            q_now[j] = q_new[j - 1]
        q_last[...] = q_new[ahead - 1]

    def states(ref, g, pair, first, last):
        return lanes(ref[g, pair, 0, first:last], ref[g, pair, 1, first:last])

    def by_side(val):
        keep = lax.broadcasted_iota(jnp.int32, val.shape, 1) < 64
        zero = jnp.zeros(val.shape, val.dtype)
        return [jnp.where(keep, val, zero), jnp.where(keep, zero, val)]

    def side_sums(val):
        keep = low if val.shape[0] == 16 else low_tall
        return jnp.where(keep, jnp.sum(jnp.where(keep, val, 0.0), 1, keepdims=True), jnp.sum(jnp.where(keep, 0.0, val), 1, keepdims=True))

    def stage_hidden(g, pair, j, q_step, live):
        cols = slice(128 * pair, 128 * pair + 128)
        key_tile = k_now[j, g, :, cols]
        query_tile = q_now[j, g, :, cols]
        bias_tile = rep8(bias_pair[pair], 16)
        query_base[g, pair] = query_tile + bias_tile
        key_base[g, pair] = (key_tile + bias_tile) - v_now[j, g, :, cols]
        kp = split3(key_tile)
        qp = split3(query_tile)
        key_parts[g, pair] = six_left(kp)
        lhs = rows(*by_side(rows(kp[0], qp[0])), *by_side(rows(kp[1], qp[1])), *by_side(rows(kp[2], qp[2])))
        yield
        top = dot_nn(lanes(lhs, lhs), states(w1_parts, g, pair, 0, 256))
        yield
        low_terms = dot_nn(lhs[:64], states(w1_parts, g, pair, 256, 384))
        yield
        offset = b1[g, pair]
        z_one = sum3(top, 64) + low_terms + rows(rep8(offset[:8], 32), rep8(offset[8:], 32))
        hidden, slope_val = twice_gelu_and_slope(z_one)
        slope[g, pair] = rows(slope_val[:16], slope_val[32:48])
        for tile in range(2):
            act[g, pair, tile] = tile_parts(hidden, tile)
        yield

    def stage_out(g, pair, j, q_step, live):
        acts = lanes(act[g, pair, 0], act[g, pair, 1])
        top = dot_nt(acts, states(w2_parts, g, pair, 0, 256))
        yield
        low_terms = dot_nt(acts[:64], rows(states(w2_parts, g, pair, 256, 384), pad128))
        yield
        total = sum3(top, 64) + low_terms
        total = total[:, :128] + total[:, 128:]
        z_two[g, pair] = jnp.where(low_tall, total[:32], total[32:]) + rep8(b2[g, pair], 32)
        yield

    def stage_center(g, pair, j, q_step, live):
        z_val = z_two[g, pair]
        z_two[g, pair] = z_val - side_sums(z_val) * (1 / 64)
        yield

    def stage_norm(g, pair, j, q_step, live):
        z_val = z_two[g, pair]
        inv_std = lax.rsqrt(side_sums(z_val * z_val) * (1 / 64) + LN_EPS)
        normed = z_val * inv_std
        gain_tile = rep8(gain_pair[pair], 16)
        outs[g, out_rows(q_step, 1), 128 * pair:128 * pair + 128] = (normed[16:] * gain_tile + query_base[g, pair]).astype(bf16)
        key_inv[g, pair] = inv_std[:16]
        key_norm[g, pair] = normed[:16]
        d_norm[g, pair] = (normed[:16] * gain_tile + key_base[g, pair]) * (2.0 * gain_tile)
        yield

    def stage_back(g, pair, j, q_step, live):
        d_val = d_norm[g, pair]
        normed = key_norm[g, pair]
        mean_d = side_sums(d_val) * (1 / 64)
        mean_dn = side_sums(d_val * normed) * (1 / 64)
        d_val = key_inv[g, pair] * (d_val - mean_d - normed * mean_dn)
        d_two[g, pair] = rows(*split3(d_val))
        total = d_val[:8] + d_val[8:]
        for shift in (4, 2, 1):
            total = total + pltpu.roll(total, shift, 0)
        b2[g, pair] = b2[g, pair] - jnp.where(low[:8], live * rate[2 * pair], live * rate[2 * pair + 1]) * total
        yield

    def six_left(parts):
        return rows(parts[0], parts[0], parts[0], parts[1], parts[1], parts[2])

    def six_right(ref, g, pair, height, side):
        at = [part * height + side for part in range(3)]
        term = [lanes(ref[g, pair, 0, a:a + 16], ref[g, pair, 1, a:a + 16]) for a in at]
        return rows(term[0], term[1], term[2], term[0], term[1], term[0])

    def both_rates(first, second):
        return rows(jnp.full((64, 256), first, f32), jnp.full((64, 256), second, f32))

    def stage_second(g, pair, j, q_step, live):
        dp = d_two[g, pair]
        lhs = rows(*by_side(dp[:16]), *by_side(dp[16:32]), *by_side(dp[32:]))
        top = dot_nn(lanes(lhs, lhs), states(w2_parts, g, pair, 0, 256))
        yield
        low_terms = dot_nn(lhs[:32], states(w2_parts, g, pair, 256, 384))
        yield
        d_hidden = (sum3(top, 32) + low_terms) * slope[g, pair]
        for tile in range(2):
            d_one[g, pair, tile] = tile_parts(d_hidden, tile)
        yield

    def stage_second_update(g, pair, j, q_step, live):
        dp = d_two[g, pair]
        turned = six_left([dp[:16], dp[16:32], dp[32:]]).T
        yield
        grads = []
        for side in range(2):
            grads.append(dot_nn(turned[64 * side:64 * side + 64], six_right(act, g, pair, 64, 32 * side)))
            yield
        scale = [0.25 * live * rate[2 * pair + side] for side in range(2)]
        new = w2[g, pair] - both_rates(*scale) * rows(*grads)
        w2[g, pair] = new
        for tile in range(2):
            w2_parts[g, pair, tile] = tile_parts(new, tile)
        yield

    def stage_first_update(g, pair, j, q_step, live):
        turned = key_parts[g, pair].T
        yield
        grads = []
        for side in range(2):
            grads.append(dot_nn(rows(turned[64 * side:64 * side + 64], count_rows), six_right(d_one, g, pair, 32, 16 * side)))
            yield
        scale = [live * rate[2 * pair + side] for side in range(2)]
        new = w1[g, pair] - both_rates(*scale) * rows(grads[0][:64], grads[1][:64])
        w1[g, pair] = new
        for tile in range(2):
            w1_parts[g, pair, tile] = tile_parts(new, tile)
        offset = b1[g, pair]
        b1[g, pair] = rows(offset[:8] - scale[0] * grads[0][64:72], offset[8:] - scale[1] * grads[1][64:72])
        yield

    units = [(g, pair) for g in range(seqs) for pair in range(heads // 2)]
    batches = len(units) // BATCH
    delays = (0, 1, 2, 3, 5, 5, 6, 6)
    stages = {name: (delay, stage) for name, delay, stage in zip('ABMCDEGF', delays, (
        stage_hidden, stage_out, stage_center, stage_norm, stage_back, stage_second, stage_second_update, stage_first_update))}

    def run_turn(turn, step, skip):
        running = {}
        for name in ORDER:
            for unit in range(BATCH):
                delay, stage = stages[name]
                j, batch = divmod(turn - delay, batches)
                if skip(j, delay):
                    continue
                if (name, unit) not in running:
                    g, pair = units[batch * BATCH + unit]
                    running[name, unit] = stage(g, pair, j, jnp.maximum(step + j - 1, 0), jnp.where(step + j >= 0, 1.0, 0.0) if j < 0 else 1.0)
                next(running[name, unit])
        for stage in running.values():
            next(stage, None)

    def body(step, next_turn=None):
        last = next_turn is None
        shift_in()
        projection = iter(()) if last else project(next_turn)
        count = 0
        for turn in range(batches * (1 if last else ahead)):
            run_turn(turn, step, lambda j, delay: last and j >= 0 and delay > 3)
            if count >= PROJECT_FROM and (count - PROJECT_FROM) % PROJECT_EVERY == 0:
                next(projection, None)
            count += 1
        for _ in projection:
            pass

    for turn in range(P0):
        pass_on(jnp.int32(turn))
    turns = steps // ahead
    half_turns = turns // 2

    def loop_body(turn, carry):
        step = turn * ahead
        pass_on(turn + P0 + PA * (1 - me // 2))
        send_far(turn)

        @pl.when(turn <= 1)
        def _():
            wait_tokens(turn)
            for _ in project(turn):
                pass

        @pl.when((turn >= 1) & (turn + 1 < turns))
        def _():
            wait_tokens(turn + 1)

        @pl.when((me >= 2) & (turn == WT))
        def _():
            w_swap.start()

        @pl.when(turn >= 2)
        def _():
            send_row(step - 2 * ahead, ahead)

        @pl.when((turn >= 2) & ((me < 2) | (turn >= half_turns + 2)))
        def _():
            send_across(step - 2 * ahead, ahead)

        @pl.when((turn >= half_turns) & (me >= 2))
        def _():
            send_across(step - half_turns * ahead, ahead)

        body(step, lax.rem(turn + jnp.minimum(turn, 1), turns))
        return carry

    lax.fori_loop(0, turns, loop_body, 0)
    send_row(jnp.int32(steps - 2 * ahead), ahead)
    send_across(jnp.int32(steps - 2 * ahead), ahead)
    body(jnp.int32(steps))
    send_row(jnp.int32(steps - 2), 1)
    send_across(jnp.int32(steps - 2), 1)
    for turn in range(batches, batches + 3):
        run_turn(turn, jnp.int32(steps), lambda j, delay: j != 0 or delay > 3)
    def tokens_sent(slot, count):
        some = tok.at[:, pl.ds(0, count * MINI_BATCH)]
        remote(some, some, tok_send.at[slot], pass_recv.at[0], heads=other_row).wait_send()

    tokens_sent(0, own_steps)
    for slot, more, cond in ((1, 4, me == 0), (2, -2, me >= 2)):
        @pl.when(cond)
        def _():
            tokens_sent(slot, own_steps + more)

        @pl.when(jnp.logical_not(cond))
        def _():
            tokens_sent(slot, own_steps)

    send_row(jnp.int32(steps - 1), 1)
    send_across(jnp.int32(steps - 1), 1)

    def rows_of(count):
        return outs.at[:, pl.ds(0, count * MINI_BATCH)]

    def done(count, send, recv):
        return remote(rows_of(count), rows_of(count), send, recv, heads=other_row)

    def arrive(late, count):
        pltpu.make_async_copy(rows_of(count), rows_of(count), own_sem.at[late]).wait()
        for place in range(parts_of_seq):
            done(count, out_send.at[0], out_recv.at[other_row, place, late]).wait_recv()

            @pl.when(me != place)
            def _():
                done(count, out_send.at[0], out_recv.at[row_axis, place, late]).wait_recv()

    w_keep.wait()
    w_swap.wait()
    w_load = pltpu.make_async_copy(w_full, w_all, w_own)
    w_load.start()
    arrive(0, early_steps)

    def fetch(block):
        rows_at = pl.ds(two * block, two), pl.ds(0, early_steps * MINI_BATCH)
        return pltpu.make_async_copy(o_full.at[rows_at], o_block.at[lax.rem(block, 2)], o_sem.at[lax.rem(block, 2)])

    def put(block):
        return pltpu.make_async_copy(y_block.at[lax.rem(block, 2)], y_early.at[pl.ds(two * block, two)], y_sem.at[lax.rem(block, 2)])

    two = 2
    blocks = parts_of_seq * seqs // two
    fetch(jnp.int32(0)).start()
    w_load.wait()

    def early_block(block, carry):
        @pl.when(block + 1 < blocks)
        def _():
            fetch(block + 1).start()

        @pl.when(block >= 2)
        def _():
            put(block - 2).wait()

        fetch(block).wait()
        slot = lax.rem(block, 2)
        val = o_block[slot].reshape(two * early_steps * MINI_BATCH, 2 * width)
        for col in range(0, w_all.shape[1], 256):
            y_block[slot, :, :, col:col + 256] = dot_nn(val, w_all[:, col:col + 256]).astype(bf16).reshape(two, early_steps * MINI_BATCH, 256)
        put(block).start()
        return carry

    lax.fori_loop(0, blocks, early_block, 0)
    put(jnp.int32(blocks - 2)).wait()
    put(jnp.int32(blocks - 1)).wait()
    done(steps - own_steps, out_send.at[0], out_recv.at[0, 0, 0]).wait_send()
    done(steps, out_send.at[1], out_recv.at[0, 0, 0]).wait_send()
    arrive(1, own_steps - early_steps)


def late_kernel(y_early, outs, w_full, y_ref, w_all, o_late, y_late, y_kept, in_sem, out_sem, w_sem):
    num_seqs, late = o_late.shape[:2]
    early = y_kept.shape[1]
    group = num_seqs // 4
    early_rows, late_rows = pl.ds(0, early), pl.ds(early, late)
    w_load = pltpu.make_async_copy(w_full, w_all, w_sem)
    w_load.start()

    def some(part):
        return pl.ds(group * part, group)

    late_in = [pltpu.make_async_copy(outs.at[some(i), late_rows], o_late.at[some(i)], in_sem.at[0, i]) for i in range(4)]
    early_in = [pltpu.make_async_copy(y_early.at[some(i)], y_kept.at[some(i)], in_sem.at[1, i]) for i in range(4)]
    late_out = [pltpu.make_async_copy(y_late.at[some(i)], y_ref.at[some(i), late_rows], out_sem.at[0, i]) for i in range(4)]
    early_out = [pltpu.make_async_copy(y_kept.at[some(i)], y_ref.at[some(i), early_rows], out_sem.at[1, i]) for i in range(4)]
    for copy in late_in + early_in:
        copy.start()
    w_load.wait()
    for i in range(4):
        late_in[i].wait()
        val = o_late[some(i)].reshape(group * late, o_late.shape[2])
        for col in range(0, w_all.shape[1], 256):
            y_late[some(i), :, col:col + 256] = dot_nn(val, w_all[:, col:col + 256]).astype(bf16).reshape(group, late, 256)
        early_in[i].wait()
        early_out[i].start()
        late_out[i].start()
    for copy in early_out + late_out:
        copy.wait()


def finish(outs, w_full, y_early):
    num_seqs, own_len, width = outs.shape
    early, model_dim = y_early.shape[1:]
    late = own_len - early
    hbm = pl.BlockSpec(memory_space=pl.ANY)
    dma = pltpu.SemaphoreType.DMA
    return pl.pallas_call(
        late_kernel,
        out_shape=jax.ShapeDtypeStruct((num_seqs, own_len, model_dim), bf16),
        in_specs=[hbm] * 3,
        out_specs=hbm,
        scratch_shapes=[pltpu.VMEM((width, model_dim), bf16), pltpu.VMEM((num_seqs, late, width), bf16), pltpu.VMEM((num_seqs, late, model_dim), bf16),
                        pltpu.VMEM((num_seqs, early, model_dim), bf16), dma((2, 4)), dma((2, 4)), dma],
        compiler_params=pltpu.CompilerParams(vmem_limit_bytes=60 * 2 ** 20),
    )(y_early, outs, w_full)


def run_layer(tokens, theta_k, theta_q, theta_v, w_out, w1, w2t, b1, b2, gain, bias, rate, parts_of_seq):
    num_seqs, own_len, model_dim = tokens.shape
    seqs = num_seqs // parts_of_seq
    steps = own_len * parts_of_seq // MINI_BATCH
    heads = w1.shape[0]
    width = theta_k.shape[1]
    smem = pl.BlockSpec(memory_space=pltpu.SMEM)
    hbm = pl.BlockSpec(memory_space=pl.ANY)
    each = [((128, 256), f32), ((128, 256), f32), ((2, 384, 128), bf16), ((2, 384, 128), bf16), ((16, 256), f32),
            ((2, 192, 128), bf16), ((32, 256), f32), ((2, 96, 128), bf16),
            ((8, 128), f32), ((96, 128), bf16), ((16, 128), f32), ((16, 128), f32), ((32, 128), f32),
            ((16, 128), f32), ((16, 128), f32), ((16, 128), f32), ((48, 128), bf16)]
    scratch = [pltpu.VMEM(val.shape, val.dtype) for val in (theta_k, theta_q, theta_v, w1, w2t)]
    scratch += [pltpu.VMEM((seqs, heads // 2) + shape, dtype) for shape, dtype in each]
    scratch += [pltpu.VMEM((heads // 2, 8, 128), f32)] * 2
    scratch += [pltpu.VMEM((seqs, steps * MINI_BATCH, model_dim), bf16), pltpu.VMEM((seqs, steps * MINI_BATCH, width), bf16)]
    ahead = AHEAD
    several = pltpu.VMEM((ahead, seqs, MINI_BATCH, width), f32)
    scratch += [several] * 3 + [pltpu.VMEM((seqs, MINI_BATCH, width), f32)] + [several] * 3
    own_steps = steps // parts_of_seq
    dma = pltpu.SemaphoreType.DMA
    half_turns = steps // (2 * AHEAD)
    scratch += [dma((9,)), dma((3,)), dma, dma, dma((half_turns,)), dma((half_turns,)), dma((2,)), dma((2,)), dma((2, parts_of_seq, 2)), dma((2,)), dma, dma, dma]
    early = 2 * own_len // 3
    scratch += [pltpu.VMEM((2 * width, model_dim), bf16), pltpu.VMEM((2, 2, early, 2 * width), bf16), pltpu.VMEM((2, 2, early, model_dim), bf16), dma((2,)), dma((2,))]
    scratch += [pltpu.VMEM(val.shape, val.dtype) for val in (b1, b2, gain, bias)]
    return pl.pallas_call(
        functools.partial(layer_kernel, steps, seqs, heads, ahead, parts_of_seq),
        out_shape=(jax.ShapeDtypeStruct((num_seqs, own_len, 2 * width), bf16), jax.ShapeDtypeStruct((2 * width, model_dim), bf16),
                   jax.ShapeDtypeStruct((num_seqs, early, model_dim), bf16)),
        in_specs=[hbm] * 11 + [smem],
        out_specs=(hbm, hbm, hbm),
        scratch_shapes=scratch,
        compiler_params=pltpu.CompilerParams(vmem_limit_bytes=60 * 2 ** 20, collective_id=0, has_side_effects=True),
    )(tokens, w_out, theta_k, theta_q, theta_v, w1, w2t, b1, b2, gain, bias, rate)


def solution(mesh):
    parts_of_seq = mesh.shape['seq']

    def local_fn(tokens, theta_q, theta_k, theta_v, w_out, w_one, b_one, w_two, b_two, ln_gain, ln_bias, inner_lr):
        outs, w_full, y_early = run_layer(tokens, theta_k, theta_q, theta_v, w_out, w_one, jnp.swapaxes(w_two, 1, 2), b_one, b_two, ln_gain, ln_bias, inner_lr, parts_of_seq)
        return finish(outs, w_full, y_early)

    arg_specs = (P('data', 'seq', None), P(None, 'heads'), P(None, 'heads'), P(None, 'heads'), P('heads', None), P('heads', None, None), P('heads', None), P('heads', None, None), P('heads', None), P('heads', None), P('heads', None), P('heads'))
    return jax.shard_map(local_fn, mesh=mesh, in_specs=arg_specs, out_specs=P('data', 'seq', None), check_vma=False)
```

```python
import functools

import jax
import jax.numpy as jnp
from jax import lax
from jax.experimental import pallas as pl
from jax.experimental.pallas import tpu as pltpu
from jax.sharding import PartitionSpec as P

MINI_BATCH = 16
AHEAD = 2
BATCH = 2
ORDER = 'MCDGFAABEBAEABEGGGFFF'
PROJECT_EVERY = 1
PROJECT_FROM = 0
FAR0, FAR1, FAR2, PA, WT, P0 = -3, 6, -9, 5, 10, 2
WHOLE = 2
LN_EPS = 1e-6
GELU_C0 = 0.7978845608028654
GELU_C1 = 0.044715
f32 = jnp.float32
bf16 = jnp.bfloat16


def split3(val):
    high = val.astype(bf16)
    rest = val - high.astype(f32)
    mid = rest.astype(bf16)
    return high, mid, (rest - mid.astype(f32)).astype(bf16)


def dot_nn(lhs, rhs):
    return lax.dot_general(lhs, rhs, (((1,), (0,)), ((), ())), preferred_element_type=f32)


def dot_nt(lhs, rhs):
    return lax.dot_general(lhs, rhs, (((1,), (1,)), ((), ())), preferred_element_type=f32)


def dot_tn(lhs, rhs):
    return lax.dot_general(lhs, rhs, (((0,), (0,)), ((), ())), preferred_element_type=f32)


def rows(*parts):
    return jnp.concatenate(parts, 0)


def lanes(*parts):
    return jnp.concatenate(parts, 1)


def rep8(val, count):
    return rows(*([val] * (count // 8)))


def sum3(val, count):
    return val[0:count] + val[count:2 * count] + val[2 * count:3 * count]


def twice_gelu_and_slope(z_val):
    square = z_val * z_val
    tanh_val = jnp.tanh(z_val * (GELU_C0 + (GELU_C0 * GELU_C1) * square))
    plus = 1.0 + tanh_val
    slope = plus + (1.0 - tanh_val * tanh_val) * (z_val * (GELU_C0 + (3 * GELU_C0 * GELU_C1) * square))
    return z_val * plus, slope


def tile_parts(val, tile):
    return rows(*split3(val[:, 128 * tile:128 * tile + 128]))


def eight_rows(row, twice):
    row = lanes(row, row) if twice else row
    return jnp.broadcast_to(row, (8, row.shape[1]))


def layer_kernel(steps, seqs, heads, ahead, parts_of_seq, tokens, w_out, theta_k_at, theta_q_at, theta_v_at, w1_at, w2_at, b1_at, b2_at, gain_at, bias_at, rate_in,
                 o_full, w_full, y_early, theta_k, theta_q, theta_v, w1_in, w2_in,
                 w1, w2, w1_parts, w2_parts, b1, act, slope, d_one, b2, key_parts, key_base, query_base, z_two, key_norm, key_inv, d_norm, d_two, gain_pair, bias_pair,
                 tok, outs, k_now, v_now, q_now, q_last, k_new, v_new, q_new,
                 load_sem, tok_send, own_recv, near_recv, half_recv, pass_recv, whole_recv, out_send, out_recv, own_sem, w_send, w_recv, w_own,
                 w_all, o_block, y_block, o_first, y_first, o_sem, y_sem, b1_in, b2_in, gain_in, bias_in):
    low = lax.broadcasted_iota(jnp.int32, (16, 128), 1) < 64
    pad128 = jnp.zeros((128, 256), bf16)
    low_tall = lax.broadcasted_iota(jnp.int32, (32, 128), 1) < 64
    count_rows = jnp.where(lax.broadcasted_iota(jnp.int32, (16, 96), 1) < 48, 1.0, 0.0).astype(bf16)
    width = 64 * heads
    own_steps = steps // parts_of_seq
    early_steps = 2 * own_steps // 3
    part_steps = own_steps // 3
    part_rows = part_steps * MINI_BATCH
    row_axis = lax.axis_index('heads')
    me = lax.axis_index('seq')
    other_row = 1 - row_axis
    mesh_ids = pl.DeviceIdType.MESH

    def other_core(place):
        return place + 1 - 2 * lax.rem(place, 2)

    near = other_core(me)

    barrier = pltpu.get_barrier_semaphore()
    for shift_row in range(2):
        for shift in range(parts_of_seq):
            if shift_row or shift:
                pl.semaphore_signal(barrier, inc=1, device_id={'heads': lax.rem(row_axis + shift_row, 2), 'seq': lax.rem(me + shift, parts_of_seq)}, device_id_type=mesh_ids)
    pl.semaphore_wait(barrier, 2 * parts_of_seq - 1)

    half = seqs // 2
    my_half = pl.ds(half * row_axis, half)
    far_from = (1 - me // 2) * (steps // 2)

    def remote(src, dst, send, recv, **device):
        return pltpu.make_async_remote_copy(src, dst, send, recv, device_id=device, device_id_type=mesh_ids)

    pair_rows = ahead * MINI_BATCH
    own_turns = own_steps // ahead
    far_turns = 2 * own_turns
    far_turn = far_turns * (1 - me // 2)

    def tok_rows(turn, count=1):
        return pl.ds(pl.multiple_of(pair_rows * turn, pair_rows), pair_rows * count)

    def is_whole(turn):
        return (turn >= WHOLE) & (turn < WHOLE + 2)

    def send_far(turn):
        piece = turn - FAR0 - FAR1 * me - FAR2 * (me // 2)

        @pl.when((piece >= 0) & (piece < own_turns))
        def _():
            at = me * own_turns + piece
            whole = is_whole(at)

            @pl.loop(0, 2)
            def _(core):
                dest = 2 * (1 - me // 2) + core

                @pl.when(whole)
                def _():
                    src = tokens.at[pl.ds(seqs * dest, seqs), tok_rows(piece)]
                    remote(src, tok.at[:, tok_rows(at)], tok_send.at[1], whole_recv.at[at - WHOLE], seq=dest).start()

                @pl.when(jnp.logical_not(whole))
                def _():
                    src = tokens.at[pl.ds(seqs * dest + half * row_axis, half), tok_rows(piece)]
                    remote(src, tok.at[my_half, tok_rows(at)], tok_send.at[1], half_recv.at[lax.rem(at, far_turns)], seq=dest).start()

    def is_far(turn):
        return (turn >= far_turn) & (turn < far_turn + far_turns)

    def pass_on(turn):
        @pl.when(is_far(turn) & jnp.logical_not(is_whole(turn)))
        def _():
            spot = tok.at[my_half, tok_rows(turn)]
            slot = turn - far_turn
            remote(spot, spot, tok_send.at[2], half_recv.at[slot], heads=other_row).wait_recv()
            remote(spot, spot, tok_send.at[2], pass_recv.at[slot], heads=other_row).start()

    def wait_tokens(turn):
        @pl.when(is_far(turn) & is_whole(turn))
        def _():
            spot = tok.at[:, tok_rows(turn)]
            remote(spot, spot, tok_send.at[1], whole_recv.at[turn - WHOLE], heads=other_row).wait_recv()

        @pl.when(is_far(turn) & jnp.logical_not(is_whole(turn)))
        def _():
            spot = tok.at[my_half, tok_rows(turn)]
            remote(spot, spot, tok_send.at[2], pass_recv.at[turn - far_turn], heads=other_row).wait_recv()

        @pl.when(lax.rem(turn, own_turns) == 0)
        def _():
            spot = tok.at[:, tok_rows(turn, own_turns)]

            @pl.when(turn // own_turns == me)
            def _():
                pltpu.make_async_copy(spot, spot, own_recv).wait()

            @pl.when(turn // own_turns == near)
            def _():
                remote(spot, spot, tok_send.at[0], near_recv, seq=near).wait_recv()

    for turn in range(FAR0, 0):
        send_far(jnp.int32(turn))
    own_block = tok.at[:, tok_rows(me * own_turns, own_turns)]
    pltpu.make_async_copy(tokens.at[pl.ds(seqs * me, seqs)], own_block, own_recv).start()
    remote(tokens.at[pl.ds(seqs * near, seqs)], own_block, tok_send.at[0], near_recv, seq=near).start()
    loads = [pltpu.make_async_copy(src, dst, load_sem.at[i]) for i, (src, dst) in enumerate((
        (w1_at, w1_in), (w2_at, w2_in), (b1_at, b1_in), (b2_at, b2_in), (gain_at, gain_in), (bias_at, bias_in),
        (theta_k_at, theta_k), (theta_q_at, theta_q), (theta_v_at, theta_v)))]
    for load in loads:
        load.start()

    my_w_rows = w_full.at[pl.ds(pl.multiple_of(row_axis * width, width), width)]
    w_swap = pltpu.make_async_remote_copy(w_out, my_w_rows, w_send, w_recv, device_id={'heads': other_row}, device_id_type=mesh_ids)
    w_keep = pltpu.make_async_copy(w_out, my_w_rows, w_own)
    w_keep.start()

    @pl.when(me < 2)
    def _():
        w_swap.start()

    def out_rows(step, count):
        return pl.ds(pl.multiple_of(MINI_BATCH * step, MINI_BATCH), MINI_BATCH * count)

    def out_copy(step, count):
        place = pl.ds(seqs * me, seqs), out_rows(lax.rem(step, own_steps), count), pl.ds(pl.multiple_of(width * row_axis, width), width)
        late = lax.rem(step, own_steps) // part_steps
        return outs.at[:, out_rows(step, count)], o_full.at[place], step // own_steps, late

    def send_row(step, count):
        src, dst, owner, late = out_copy(step, count)

        @pl.when(owner != me)
        def _():
            remote(src, dst, out_send.at[0], out_recv.at[row_axis, me, late], seq=owner).start()

        @pl.when(owner == me)
        def _():
            pltpu.make_async_copy(src, dst, own_sem.at[late]).start()

    def send_across(step, count):
        src, dst, owner, late = out_copy(step, count)
        remote(src, dst, out_send.at[1], out_recv.at[row_axis, me, late], heads=other_row, seq=owner).start()

    for load in loads:
        load.wait()
    for pair in range(heads // 2):
        even, odd = 2 * pair, 2 * pair + 1

        def pair_row(source):
            return jnp.broadcast_to(lanes(source[even:even + 1], source[odd:odd + 1]), (8, 128))

        gain_pair[pair] = pair_row(gain_in)
        bias_pair[pair] = pair_row(bias_in)
        offset = pair_row(b2_in)
        hidden_offset = rows(eight_rows(b1_in[even:even + 1], False), eight_rows(b1_in[odd:odd + 1], False))
        first = rows(w1_in[even], w1_in[odd])
        second = rows(0.5 * w2_in[even], 0.5 * w2_in[odd])
        for g in range(seqs):
            w1[g, pair] = first
            w2[g, pair] = second
            b1[g, pair] = hidden_offset
            b2[g, pair] = offset
        for tile in range(2):
            first_parts, second_parts = tile_parts(first, tile), tile_parts(second, tile)
            for g in range(seqs):
                w1_parts[g, pair, tile] = first_parts
                w2_parts[g, pair, tile] = second_parts
    q_last[...] = jnp.zeros(q_last.shape, f32)

    @pl.loop(0, seqs)
    def _(g):
        for ref in (act, slope, d_one, key_parts, key_base, query_base, z_two, key_norm, key_inv, d_norm, d_two):
            ref[g] = jnp.zeros(ref.shape[1:], ref.dtype)

    rate = [rate_in[h] * (1 / MINI_BATCH) for h in range(heads)]

    def both(unit):
        return [2 * pair + side for pair in unit for side in range(2)]

    def project(turn):
        for theta, target in ((theta_k, k_new), (theta_q, q_new), (theta_v, v_new)):
            for col in range(0, width, 256):
                toks = tok[:, tok_rows(turn)].reshape(seqs * pair_rows, tok.shape[2])
                found = dot_nn(toks, theta[:, col:col + 256]).reshape(seqs, ahead, MINI_BATCH, 256)
                for j in range(ahead):
                    target[j, :, :, col:col + 256] = found[:, j]
                yield

    def shift_in():
        k_now[...] = k_new[...]
        v_now[...] = v_new[...]
        q_now[0] = q_last[...]
        for j in range(1, ahead):
            q_now[j] = q_new[j - 1]
        q_last[...] = q_new[ahead - 1]

    def states(ref, g, pair, first, last):
        return lanes(ref[g, pair, 0, first:last], ref[g, pair, 1, first:last])

    def by_side(val):
        keep = lax.broadcasted_iota(jnp.int32, val.shape, 1) < 64
        zero = jnp.zeros(val.shape, val.dtype)
        return [jnp.where(keep, val, zero), jnp.where(keep, zero, val)]

    def side_sums(val):
        keep = low if val.shape[0] == 16 else low_tall
        return jnp.where(keep, jnp.sum(jnp.where(keep, val, 0.0), 1, keepdims=True), jnp.sum(jnp.where(keep, 0.0, val), 1, keepdims=True))

    def stage_hidden(g, pair, j, q_step, live):
        cols = slice(128 * pair, 128 * pair + 128)
        key_tile = k_now[j, g, :, cols]
        query_tile = q_now[j, g, :, cols]
        bias_tile = rep8(bias_pair[pair], 16)
        query_base[g, pair] = query_tile + bias_tile
        key_base[g, pair] = (key_tile + bias_tile) - v_now[j, g, :, cols]
        kp = split3(key_tile)
        qp = split3(query_tile)
        key_parts[g, pair] = six_left(kp)
        lhs = rows(*by_side(rows(kp[0], qp[0])), *by_side(rows(kp[1], qp[1])), *by_side(rows(kp[2], qp[2])))
        yield
        top = dot_nn(lanes(lhs, lhs), states(w1_parts, g, pair, 0, 256))
        yield
        low_terms = dot_nn(lhs[:64], states(w1_parts, g, pair, 256, 384))
        yield
        offset = b1[g, pair]
        z_one = sum3(top, 64) + low_terms + rows(rep8(offset[:8], 32), rep8(offset[8:], 32))
        hidden, slope_val = twice_gelu_and_slope(z_one)
        slope[g, pair] = rows(slope_val[:16], slope_val[32:48])
        for tile in range(2):
            act[g, pair, tile] = tile_parts(hidden, tile)
        yield

    def stage_out(g, pair, j, q_step, live):
        acts = lanes(act[g, pair, 0], act[g, pair, 1])
        top = dot_nt(acts, states(w2_parts, g, pair, 0, 256))
        yield
        low_terms = dot_nt(acts[:64], rows(states(w2_parts, g, pair, 256, 384), pad128))
        yield
        total = sum3(top, 64) + low_terms
        total = total[:, :128] + total[:, 128:]
        z_two[g, pair] = jnp.where(low_tall, total[:32], total[32:]) + rep8(b2[g, pair], 32)
        yield

    def stage_center(g, pair, j, q_step, live):
        z_val = z_two[g, pair]
        z_two[g, pair] = z_val - side_sums(z_val) * (1 / 64)
        yield

    def stage_norm(g, pair, j, q_step, live):
        z_val = z_two[g, pair]
        inv_std = lax.rsqrt(side_sums(z_val * z_val) * (1 / 64) + LN_EPS)
        normed = z_val * inv_std
        gain_tile = rep8(gain_pair[pair], 16)
        outs[g, out_rows(q_step, 1), 128 * pair:128 * pair + 128] = (normed[16:] * gain_tile + query_base[g, pair]).astype(bf16)
        key_inv[g, pair] = inv_std[:16]
        key_norm[g, pair] = normed[:16]
        d_norm[g, pair] = (normed[:16] * gain_tile + key_base[g, pair]) * (2.0 * gain_tile)
        yield

    def stage_back(g, pair, j, q_step, live):
        d_val = d_norm[g, pair]
        normed = key_norm[g, pair]
        mean_d = side_sums(d_val) * (1 / 64)
        mean_dn = side_sums(d_val * normed) * (1 / 64)
        d_val = key_inv[g, pair] * (d_val - mean_d - normed * mean_dn)
        d_two[g, pair] = rows(*split3(d_val))
        total = d_val[:8] + d_val[8:]
        for shift in (4, 2, 1):
            total = total + pltpu.roll(total, shift, 0)
        b2[g, pair] = b2[g, pair] - jnp.where(low[:8], live * rate[2 * pair], live * rate[2 * pair + 1]) * total
        yield

    def six_left(parts):
        return rows(parts[0], parts[0], parts[0], parts[1], parts[1], parts[2])

    def six_right(ref, g, pair, height, side):
        at = [part * height + side for part in range(3)]
        term = [lanes(ref[g, pair, 0, a:a + 16], ref[g, pair, 1, a:a + 16]) for a in at]
        return rows(term[0], term[1], term[2], term[0], term[1], term[0])

    def both_rates(first, second):
        return rows(jnp.full((64, 256), first, f32), jnp.full((64, 256), second, f32))

    def stage_second(g, pair, j, q_step, live):
        dp = d_two[g, pair]
        lhs = rows(*by_side(dp[:16]), *by_side(dp[16:32]), *by_side(dp[32:]))
        top = dot_nn(lanes(lhs, lhs), states(w2_parts, g, pair, 0, 256))
        yield
        low_terms = dot_nn(lhs[:32], states(w2_parts, g, pair, 256, 384))
        yield
        d_hidden = (sum3(top, 32) + low_terms) * slope[g, pair]
        for tile in range(2):
            d_one[g, pair, tile] = tile_parts(d_hidden, tile)
        yield

    def stage_second_update(g, pair, j, q_step, live):
        dp = d_two[g, pair]
        turned = six_left([dp[:16], dp[16:32], dp[32:]]).T
        yield
        grads = []
        for side in range(2):
            grads.append(dot_nn(turned[64 * side:64 * side + 64], six_right(act, g, pair, 64, 32 * side)))
            yield
        scale = [0.25 * live * rate[2 * pair + side] for side in range(2)]
        new = w2[g, pair] - both_rates(*scale) * rows(*grads)
        w2[g, pair] = new
        for tile in range(2):
            w2_parts[g, pair, tile] = tile_parts(new, tile)
        yield

    def stage_first_update(g, pair, j, q_step, live):
        turned = key_parts[g, pair].T
        yield
        grads = []
        for side in range(2):
            grads.append(dot_nn(rows(turned[64 * side:64 * side + 64], count_rows), six_right(d_one, g, pair, 32, 16 * side)))
            yield
        scale = [live * rate[2 * pair + side] for side in range(2)]
        new = w1[g, pair] - both_rates(*scale) * rows(grads[0][:64], grads[1][:64])
        w1[g, pair] = new
        for tile in range(2):
            w1_parts[g, pair, tile] = tile_parts(new, tile)
        offset = b1[g, pair]
        b1[g, pair] = rows(offset[:8] - scale[0] * grads[0][64:72], offset[8:] - scale[1] * grads[1][64:72])
        yield

    units = [(g, pair) for g in range(seqs) for pair in range(heads // 2)]
    batches = len(units) // BATCH
    delays = (0, 1, 2, 3, 5, 5, 6, 6)
    stages = {name: (delay, stage) for name, delay, stage in zip('ABMCDEGF', delays, (
        stage_hidden, stage_out, stage_center, stage_norm, stage_back, stage_second, stage_second_update, stage_first_update))}

    def run_turn(turn, step, skip):
        running = {}
        for name in ORDER:
            for unit in range(BATCH):
                delay, stage = stages[name]
                j, batch = divmod(turn - delay, batches)
                if skip(j, delay):
                    continue
                if (name, unit) not in running:
                    g, pair = units[batch * BATCH + unit]
                    running[name, unit] = stage(g, pair, j, jnp.maximum(step + j - 1, 0), jnp.where(step + j >= 0, 1.0, 0.0) if j < 0 else 1.0)
                next(running[name, unit])
        for stage in running.values():
            next(stage, None)

    def body(step, next_turn=None):
        last = next_turn is None
        shift_in()
        projection = first_rows() if last else project(next_turn)
        count = 0
        for turn in range(batches * (1 if last else ahead)):
            run_turn(turn, step, lambda j, delay: last and j >= 0 and delay > 3)
            if count >= PROJECT_FROM and (count - PROJECT_FROM) % PROJECT_EVERY == 0:
                next(projection, None)
                if last:
                    next(projection, None)
            count += 1
        for _ in projection:
            pass

    for turn in range(P0):
        pass_on(jnp.int32(turn))
    turns = steps // ahead
    def rows_of(count):
        return outs.at[:, pl.ds(0, count * MINI_BATCH)]

    def done(count, send, recv):
        return remote(rows_of(count), rows_of(count), send, recv, heads=other_row)

    def arrive(part):
        pltpu.make_async_copy(rows_of(part_steps), rows_of(part_steps), own_sem.at[part]).wait()

        @pl.loop(0, parts_of_seq)
        def _(place):
            done(part_steps, out_send.at[0], out_recv.at[other_row, place, part]).wait_recv()

            @pl.when(me != place)
            def _():
                done(part_steps, out_send.at[0], out_recv.at[row_axis, place, part]).wait_recv()

    w_load = pltpu.make_async_copy(w_full, w_all, w_own)
    num_seqs = parts_of_seq * seqs
    first_load = pltpu.make_async_copy(o_full.at[:, pl.ds(0, part_rows)], o_first, o_sem.at[0])
    first_put = pltpu.make_async_copy(y_first, y_early.at[:, pl.ds(0, part_rows)], y_sem.at[0])

    def first_rows():
        group = 4
        for at in range(0, num_seqs, group):
            for col in range(0, w_all.shape[1], 256):
                val = o_first[at:at + group].reshape(group * part_rows, 2 * width)
                y_first[at:at + group, :, col:col + 256] = dot_nn(val, w_all[:, col:col + 256]).astype(bf16).reshape(group, part_rows, 256)
                yield

    half_turns = turns // 2

    def loop_body(turn, carry):
        step = turn * ahead
        pass_on(turn + P0 + PA * (1 - me // 2))
        send_far(turn)

        @pl.when(turn == turns - 1)
        def _():
            w_keep.wait()
            w_swap.wait()
            w_load.start()
            arrive(0)
            first_load.start()

        @pl.when(turn <= 1)
        def _():
            wait_tokens(turn)
            for _ in project(turn):
                pass

        @pl.when((turn >= 1) & (turn + 1 < turns))
        def _():
            wait_tokens(turn + 1)

        @pl.when((me >= 2) & (turn == WT))
        def _():
            w_swap.start()

        @pl.when(turn >= 2)
        def _():
            send_row(step - 2 * ahead, ahead)

        @pl.when((turn >= 2) & ((me < 2) | (turn >= half_turns + 2)))
        def _():
            send_across(step - 2 * ahead, ahead)

        @pl.when((turn >= half_turns) & (me >= 2))
        def _():
            send_across(step - half_turns * ahead, ahead)

        body(step, lax.rem(turn + jnp.minimum(turn, 1), turns))
        return carry

    lax.fori_loop(0, turns, loop_body, 0)
    send_row(jnp.int32(steps - 2 * ahead), ahead)
    send_across(jnp.int32(steps - 2 * ahead), ahead)
    w_load.wait()
    first_load.wait()
    body(jnp.int32(steps))
    send_row(jnp.int32(steps - 2), 1)
    send_across(jnp.int32(steps - 2), 1)
    for turn in range(batches, batches + 3):
        run_turn(turn, jnp.int32(steps), lambda j, delay: j != 0 or delay > 3)
    def tokens_sent(slot, count):
        some = tok.at[:, pl.ds(0, count * MINI_BATCH)]
        remote(some, some, tok_send.at[slot], pass_recv.at[0], heads=other_row).wait_send()

    tokens_sent(0, own_steps)
    for slot, more, cond in ((1, 4, me == 0), (2, -2, me >= 2)):
        @pl.when(cond)
        def _():
            tokens_sent(slot, own_steps + more)

        @pl.when(jnp.logical_not(cond))
        def _():
            tokens_sent(slot, own_steps)

    send_row(jnp.int32(steps - 1), 1)
    send_across(jnp.int32(steps - 1), 1)

    first_put.start()
    arrive(1)
    several = 4
    blocks = num_seqs // several
    second_rows = pl.ds(part_rows, part_rows)

    def fetch(block):
        return pltpu.make_async_copy(o_full.at[pl.ds(several * block, several), second_rows], o_block.at[lax.rem(block, 2)], o_sem.at[lax.rem(block, 2)])

    def put(block):
        return pltpu.make_async_copy(y_block.at[lax.rem(block, 2)], y_early.at[pl.ds(several * block, several), second_rows], y_sem.at[1 + lax.rem(block, 2)])

    fetch(jnp.int32(0)).start()

    def early_block(block, carry):
        @pl.when(block + 1 < blocks)
        def _():
            fetch(block + 1).start()

        @pl.when(block >= 2)
        def _():
            put(block - 2).wait()

        fetch(block).wait()
        slot = lax.rem(block, 2)
        val = o_block[slot].reshape(several * part_rows, 2 * width)
        for col in range(0, w_all.shape[1], 256):
            y_block[slot, :, :, col:col + 256] = dot_nn(val, w_all[:, col:col + 256]).astype(bf16).reshape(several, part_rows, 256)
        put(block).start()
        return carry

    lax.fori_loop(0, blocks, early_block, 0)
    first_put.wait()
    put(jnp.int32(blocks - 2)).wait()
    put(jnp.int32(blocks - 1)).wait()
    done(steps - own_steps, out_send.at[0], out_recv.at[0, 0, 0]).wait_send()
    done(steps, out_send.at[1], out_recv.at[0, 0, 0]).wait_send()
    arrive(2)


def late_kernel(y_early, outs, w_full, y_ref, w_all, o_late, y_late, y_kept, in_sem, out_sem, w_sem):
    num_seqs, late = o_late.shape[:2]
    early = y_kept.shape[1]
    group = num_seqs // 4
    early_rows, late_rows = pl.ds(0, early), pl.ds(early, late)
    w_load = pltpu.make_async_copy(w_full, w_all, w_sem)
    w_load.start()

    def some(part):
        return pl.ds(group * part, group)

    late_in = [pltpu.make_async_copy(outs.at[some(i), late_rows], o_late.at[some(i)], in_sem.at[0, i]) for i in range(4)]
    early_in = [pltpu.make_async_copy(y_early.at[some(i)], y_kept.at[some(i)], in_sem.at[1, i]) for i in range(4)]
    late_out = [pltpu.make_async_copy(y_late.at[some(i)], y_ref.at[some(i), late_rows], out_sem.at[0, i]) for i in range(4)]
    early_out = [pltpu.make_async_copy(y_kept.at[some(i)], y_ref.at[some(i), early_rows], out_sem.at[1, i]) for i in range(4)]
    for copy in late_in + early_in:
        copy.start()
    w_load.wait()
    for i in range(4):
        late_in[i].wait()
        val = o_late[some(i)].reshape(group * late, o_late.shape[2])
        for col in range(0, w_all.shape[1], 256):
            y_late[some(i), :, col:col + 256] = dot_nn(val, w_all[:, col:col + 256]).astype(bf16).reshape(group, late, 256)
        early_in[i].wait()
        early_out[i].start()
        late_out[i].start()
    for copy in early_out + late_out:
        copy.wait()


def finish(outs, w_full, y_early):
    num_seqs, own_len, width = outs.shape
    early, model_dim = y_early.shape[1:]
    late = own_len - early
    hbm = pl.BlockSpec(memory_space=pl.ANY)
    dma = pltpu.SemaphoreType.DMA
    return pl.pallas_call(
        late_kernel,
        out_shape=jax.ShapeDtypeStruct((num_seqs, own_len, model_dim), bf16),
        in_specs=[hbm] * 3,
        out_specs=hbm,
        scratch_shapes=[pltpu.VMEM((width, model_dim), bf16), pltpu.VMEM((num_seqs, late, width), bf16), pltpu.VMEM((num_seqs, late, model_dim), bf16),
                        pltpu.VMEM((num_seqs, early, model_dim), bf16), dma((2, 4)), dma((2, 4)), dma],
        compiler_params=pltpu.CompilerParams(vmem_limit_bytes=60 * 2 ** 20),
    )(y_early, outs, w_full)


def run_layer(tokens, theta_k, theta_q, theta_v, w_out, w1, w2t, b1, b2, gain, bias, rate, parts_of_seq):
    num_seqs, own_len, model_dim = tokens.shape
    seqs = num_seqs // parts_of_seq
    steps = own_len * parts_of_seq // MINI_BATCH
    heads = w1.shape[0]
    width = theta_k.shape[1]
    smem = pl.BlockSpec(memory_space=pltpu.SMEM)
    hbm = pl.BlockSpec(memory_space=pl.ANY)
    each = [((128, 256), f32), ((128, 256), f32), ((2, 384, 128), bf16), ((2, 384, 128), bf16), ((16, 256), f32),
            ((2, 192, 128), bf16), ((32, 256), f32), ((2, 96, 128), bf16),
            ((8, 128), f32), ((96, 128), bf16), ((16, 128), f32), ((16, 128), f32), ((32, 128), f32),
            ((16, 128), f32), ((16, 128), f32), ((16, 128), f32), ((48, 128), bf16)]
    scratch = [pltpu.VMEM(val.shape, val.dtype) for val in (theta_k, theta_q, theta_v, w1, w2t)]
    scratch += [pltpu.VMEM((seqs, heads // 2) + shape, dtype) for shape, dtype in each]
    scratch += [pltpu.VMEM((heads // 2, 8, 128), f32)] * 2
    scratch += [pltpu.VMEM((seqs, steps * MINI_BATCH, model_dim), bf16), pltpu.VMEM((seqs, steps * MINI_BATCH, width), bf16)]
    ahead = AHEAD
    several = pltpu.VMEM((ahead, seqs, MINI_BATCH, width), f32)
    scratch += [several] * 3 + [pltpu.VMEM((seqs, MINI_BATCH, width), f32)] + [several] * 3
    own_steps = steps // parts_of_seq
    dma = pltpu.SemaphoreType.DMA
    half_turns = steps // (2 * AHEAD)
    scratch += [dma((9,)), dma((3,)), dma, dma, dma((half_turns,)), dma((half_turns,)), dma((2,)), dma((2,)), dma((2, parts_of_seq, 3)), dma((3,)), dma, dma, dma]
    early = 2 * own_len // 3
    scratch += [pltpu.VMEM((2 * width, model_dim), bf16), pltpu.VMEM((2, 4, early // 2, 2 * width), bf16), pltpu.VMEM((2, 4, early // 2, model_dim), bf16),
                pltpu.VMEM((num_seqs, early // 2, 2 * width), bf16), pltpu.VMEM((num_seqs, early // 2, model_dim), bf16), dma((2,)), dma((3,))]
    scratch += [pltpu.VMEM(val.shape, val.dtype) for val in (b1, b2, gain, bias)]
    return pl.pallas_call(
        functools.partial(layer_kernel, steps, seqs, heads, ahead, parts_of_seq),
        out_shape=(jax.ShapeDtypeStruct((num_seqs, own_len, 2 * width), bf16), jax.ShapeDtypeStruct((2 * width, model_dim), bf16),
                   jax.ShapeDtypeStruct((num_seqs, early, model_dim), bf16)),
        in_specs=[hbm] * 11 + [smem],
        out_specs=(hbm, hbm, hbm),
        scratch_shapes=scratch,
        compiler_params=pltpu.CompilerParams(vmem_limit_bytes=60 * 2 ** 20, collective_id=0, has_side_effects=True),
    )(tokens, w_out, theta_k, theta_q, theta_v, w1, w2t, b1, b2, gain, bias, rate)


def solution(mesh):
    parts_of_seq = mesh.shape['seq']

    def local_fn(tokens, theta_q, theta_k, theta_v, w_out, w_one, b_one, w_two, b_two, ln_gain, ln_bias, inner_lr):
        outs, w_full, y_early = run_layer(tokens, theta_k, theta_q, theta_v, w_out, w_one, jnp.swapaxes(w_two, 1, 2), b_one, b_two, ln_gain, ln_bias, inner_lr, parts_of_seq)
        return finish(outs, w_full, y_early)

    arg_specs = (P('data', 'seq', None), P(None, 'heads'), P(None, 'heads'), P(None, 'heads'), P('heads', None), P('heads', None, None), P('heads', None), P('heads', None, None), P('heads', None), P('heads', None), P('heads', None), P('heads'))
    return jax.shard_map(local_fn, mesh=mesh, in_specs=arg_specs, out_specs=P('data', 'seq', None), check_vma=False)
```

```python
import functools

import jax
import jax.numpy as jnp
from jax import lax
from jax.experimental import pallas as pl
from jax.experimental.pallas import tpu as pltpu
from jax.sharding import PartitionSpec as P

MINI_BATCH = 16
AHEAD = 2
BATCH = 2
ORDER = 'MCDGFAABEBAEABEGGGFFF'
PROJECT_EVERY = 1
PROJECT_FROM = 0
FAR0, FAR1, FAR2, PA, WT, P0 = -3, 6, -9, 5, 10, 2
WHOLE = 2
KP = 4
LN_EPS = 1e-6
GELU_C0 = 0.7978845608028654
GELU_C1 = 0.044715
f32 = jnp.float32
bf16 = jnp.bfloat16


def split3(val):
    high = val.astype(bf16)
    rest = val - high.astype(f32)
    mid = rest.astype(bf16)
    return high, mid, (rest - mid.astype(f32)).astype(bf16)


def dot_nn(lhs, rhs):
    return lax.dot_general(lhs, rhs, (((1,), (0,)), ((), ())), preferred_element_type=f32)


def dot_nt(lhs, rhs):
    return lax.dot_general(lhs, rhs, (((1,), (1,)), ((), ())), preferred_element_type=f32)


def dot_tn(lhs, rhs):
    return lax.dot_general(lhs, rhs, (((0,), (0,)), ((), ())), preferred_element_type=f32)


def rows(*parts):
    return jnp.concatenate(parts, 0)


def lanes(*parts):
    return jnp.concatenate(parts, 1)


def rep8(val, count):
    return rows(*([val] * (count // 8)))


def sum3(val, count):
    return val[0:count] + val[count:2 * count] + val[2 * count:3 * count]


def twice_gelu_and_slope(z_val):
    square = z_val * z_val
    tanh_val = jnp.tanh(z_val * (GELU_C0 + (GELU_C0 * GELU_C1) * square))
    plus = 1.0 + tanh_val
    slope = plus + (1.0 - tanh_val * tanh_val) * (z_val * (GELU_C0 + (3 * GELU_C0 * GELU_C1) * square))
    return z_val * plus, slope


def tile_parts(val, tile):
    return rows(*split3(val[:, 128 * tile:128 * tile + 128]))


def eight_rows(row, twice):
    row = lanes(row, row) if twice else row
    return jnp.broadcast_to(row, (8, row.shape[1]))


def layer_kernel(steps, seqs, heads, ahead, parts_of_seq, tokens, w_out, theta_k_at, theta_q_at, theta_v_at, w1_at, w2_at, b1_at, b2_at, gain_at, bias_at, rate_in,
                 o_full, w_full, y_early, theta_k, theta_q, theta_v, w1_in, w2_in,
                 w1, w2, w1_parts, w2_parts, b1, act, slope, d_one, b2, key_parts, key_base, query_base, z_two, key_norm, key_inv, d_norm, d_two, gain_pair, bias_pair,
                 tok, outs, k_now, v_now, q_now, q_last, k_new, v_new, q_new,
                 load_sem, tok_send, own_recv, near_recv, half_recv, pass_recv, whole_recv, out_send, out_recv, own_sem, w_send, w_recv, w_own,
                 w_all, o_block, y_block, o_first, y_first, o_sem, y_sem, b1_in, b2_in, gain_in, bias_in):
    low = lax.broadcasted_iota(jnp.int32, (16, 128), 1) < 64
    pad128 = jnp.zeros((128, 256), bf16)
    low_tall = lax.broadcasted_iota(jnp.int32, (32, 128), 1) < 64
    count_rows = jnp.where(lax.broadcasted_iota(jnp.int32, (16, 96), 1) < 48, 1.0, 0.0).astype(bf16)
    width = 64 * heads
    own_steps = steps // parts_of_seq
    early_steps = 2 * own_steps // 3
    part_steps = own_steps // 3
    part_rows = part_steps * MINI_BATCH
    row_axis = lax.axis_index('heads')
    me = lax.axis_index('seq')
    other_row = 1 - row_axis
    mesh_ids = pl.DeviceIdType.MESH

    def other_core(place):
        return place + 1 - 2 * lax.rem(place, 2)

    near = other_core(me)

    barrier = pltpu.get_barrier_semaphore()
    for shift_row in range(2):
        for shift in range(parts_of_seq):
            if shift_row or shift:
                pl.semaphore_signal(barrier, inc=1, device_id={'heads': lax.rem(row_axis + shift_row, 2), 'seq': lax.rem(me + shift, parts_of_seq)}, device_id_type=mesh_ids)
    pl.semaphore_wait(barrier, 2 * parts_of_seq - 1)

    half = seqs // 2
    my_half = pl.ds(half * row_axis, half)
    far_from = (1 - me // 2) * (steps // 2)

    def remote(src, dst, send, recv, **device):
        return pltpu.make_async_remote_copy(src, dst, send, recv, device_id=device, device_id_type=mesh_ids)

    pair_rows = ahead * MINI_BATCH
    own_turns = own_steps // ahead
    far_turns = 2 * own_turns
    far_turn = far_turns * (1 - me // 2)

    def tok_rows(turn, count=1):
        return pl.ds(pl.multiple_of(pair_rows * turn, pair_rows), pair_rows * count)

    def is_whole(turn):
        return (turn >= WHOLE) & (turn < WHOLE + 2)

    def send_far(turn):
        piece = turn - FAR0 - FAR1 * me - FAR2 * (me // 2)

        @pl.when((piece >= 0) & (piece < own_turns))
        def _():
            at = me * own_turns + piece
            whole = is_whole(at)

            @pl.loop(0, 2)
            def _(core):
                dest = 2 * (1 - me // 2) + core

                @pl.when(whole)
                def _():
                    src = tokens.at[pl.ds(seqs * dest, seqs), tok_rows(piece)]
                    remote(src, tok.at[:, tok_rows(at)], tok_send.at[1], whole_recv.at[at - WHOLE], seq=dest).start()

                @pl.when(jnp.logical_not(whole))
                def _():
                    src = tokens.at[pl.ds(seqs * dest + half * row_axis, half), tok_rows(piece)]
                    remote(src, tok.at[my_half, tok_rows(at)], tok_send.at[1], half_recv.at[lax.rem(at, far_turns)], seq=dest).start()

    def is_far(turn):
        return (turn >= far_turn) & (turn < far_turn + far_turns)

    def pass_on(turn):
        @pl.when(is_far(turn) & jnp.logical_not(is_whole(turn)))
        def _():
            spot = tok.at[my_half, tok_rows(turn)]
            slot = turn - far_turn
            remote(spot, spot, tok_send.at[2], half_recv.at[slot], heads=other_row).wait_recv()
            remote(spot, spot, tok_send.at[2], pass_recv.at[slot], heads=other_row).start()

    def wait_tokens(turn):
        @pl.when(is_far(turn) & is_whole(turn))
        def _():
            spot = tok.at[:, tok_rows(turn)]
            remote(spot, spot, tok_send.at[1], whole_recv.at[turn - WHOLE], heads=other_row).wait_recv()

        @pl.when(is_far(turn) & jnp.logical_not(is_whole(turn)))
        def _():
            spot = tok.at[my_half, tok_rows(turn)]
            remote(spot, spot, tok_send.at[2], pass_recv.at[turn - far_turn], heads=other_row).wait_recv()

        @pl.when(lax.rem(turn, own_turns) == 0)
        def _():
            spot = tok.at[:, tok_rows(turn, own_turns)]

            @pl.when(turn // own_turns == me)
            def _():
                pltpu.make_async_copy(spot, spot, own_recv).wait()

            @pl.when(turn // own_turns == near)
            def _():
                remote(spot, spot, tok_send.at[0], near_recv, seq=near).wait_recv()

    for turn in range(FAR0, 0):
        send_far(jnp.int32(turn))
    own_block = tok.at[:, tok_rows(me * own_turns, own_turns)]
    pltpu.make_async_copy(tokens.at[pl.ds(seqs * me, seqs)], own_block, own_recv).start()
    remote(tokens.at[pl.ds(seqs * near, seqs)], own_block, tok_send.at[0], near_recv, seq=near).start()
    loads = [pltpu.make_async_copy(src, dst, load_sem.at[i]) for i, (src, dst) in enumerate((
        (w1_at, w1_in), (w2_at, w2_in), (b1_at, b1_in), (b2_at, b2_in), (gain_at, gain_in), (bias_at, bias_in),
        (theta_k_at, theta_k), (theta_q_at, theta_q), (theta_v_at, theta_v)))]
    for load in loads:
        load.start()

    my_w_rows = w_full.at[pl.ds(pl.multiple_of(row_axis * width, width), width)]
    w_swap = pltpu.make_async_remote_copy(w_out, my_w_rows, w_send, w_recv, device_id={'heads': other_row}, device_id_type=mesh_ids)
    w_keep = pltpu.make_async_copy(w_out, my_w_rows, w_own)
    w_keep.start()

    @pl.when(me < 2)
    def _():
        w_swap.start()

    def out_rows(step, count):
        return pl.ds(pl.multiple_of(MINI_BATCH * step, MINI_BATCH), MINI_BATCH * count)

    def out_copy(step, count):
        place = pl.ds(seqs * me, seqs), out_rows(lax.rem(step, own_steps), count), pl.ds(pl.multiple_of(width * row_axis, width), width)
        late = lax.rem(step, own_steps) // part_steps
        return outs.at[:, out_rows(step, count)], o_full.at[place], step // own_steps, late

    def send_row(step, count):
        src, dst, owner, late = out_copy(step, count)

        @pl.when(owner != me)
        def _():
            remote(src, dst, out_send.at[0], out_recv.at[row_axis, me, late], seq=owner).start()

        @pl.when(owner == me)
        def _():
            pltpu.make_async_copy(src, dst, own_sem.at[late]).start()

    def send_across(step, count):
        src, dst, owner, late = out_copy(step, count)
        remote(src, dst, out_send.at[1], out_recv.at[row_axis, me, late], heads=other_row, seq=owner).start()

    for load in loads:
        load.wait()
    for pair in range(heads // 2):
        even, odd = 2 * pair, 2 * pair + 1

        def pair_row(source):
            return jnp.broadcast_to(lanes(source[even:even + 1], source[odd:odd + 1]), (8, 128))

        gain_pair[pair] = pair_row(gain_in)
        bias_pair[pair] = pair_row(bias_in)
        offset = pair_row(b2_in)
        hidden_offset = rows(eight_rows(b1_in[even:even + 1], False), eight_rows(b1_in[odd:odd + 1], False))
        first = rows(w1_in[even], w1_in[odd])
        second = rows(0.5 * w2_in[even], 0.5 * w2_in[odd])
        for g in range(seqs):
            w1[g, pair] = first
            w2[g, pair] = second
            b1[g, pair] = hidden_offset
            b2[g, pair] = offset
        for tile in range(2):
            first_parts, second_parts = tile_parts(first, tile), tile_parts(second, tile)
            for g in range(seqs):
                w1_parts[g, pair, tile] = first_parts
                w2_parts[g, pair, tile] = second_parts
    q_last[...] = jnp.zeros(q_last.shape, f32)

    @pl.loop(0, seqs)
    def _(g):
        for ref in (act, slope, d_one, key_parts, key_base, query_base, z_two, key_norm, key_inv, d_norm, d_two):
            ref[g] = jnp.zeros(ref.shape[1:], ref.dtype)

    rate = [rate_in[h] * (1 / MINI_BATCH) for h in range(heads)]

    def both(unit):
        return [2 * pair + side for pair in unit for side in range(2)]

    def project(turn):
        for theta, target in ((theta_k, k_new), (theta_q, q_new), (theta_v, v_new)):
            for col in range(0, width, 256):
                toks = tok[:, tok_rows(turn)].reshape(seqs * pair_rows, tok.shape[2])
                found = dot_nn(toks, theta[:, col:col + 256]).reshape(seqs, ahead, MINI_BATCH, 256)
                for j in range(ahead):
                    target[j, :, :, col:col + 256] = found[:, j]
                yield

    def shift_in():
        k_now[...] = k_new[...]
        v_now[...] = v_new[...]
        q_now[0] = q_last[...]
        for j in range(1, ahead):
            q_now[j] = q_new[j - 1]
        q_last[...] = q_new[ahead - 1]

    def states(ref, g, pair, first, last):
        return lanes(ref[g, pair, 0, first:last], ref[g, pair, 1, first:last])

    def by_side(val):
        keep = lax.broadcasted_iota(jnp.int32, val.shape, 1) < 64
        zero = jnp.zeros(val.shape, val.dtype)
        return [jnp.where(keep, val, zero), jnp.where(keep, zero, val)]

    def side_sums(val):
        keep = low if val.shape[0] == 16 else low_tall
        return jnp.where(keep, jnp.sum(jnp.where(keep, val, 0.0), 1, keepdims=True), jnp.sum(jnp.where(keep, 0.0, val), 1, keepdims=True))

    def stage_hidden(g, pair, j, q_step, live):
        cols = slice(128 * pair, 128 * pair + 128)
        key_tile = k_now[j, g, :, cols]
        query_tile = q_now[j, g, :, cols]
        bias_tile = rep8(bias_pair[pair], 16)
        query_base[g, pair] = query_tile + bias_tile
        key_base[g, pair] = (key_tile + bias_tile) - v_now[j, g, :, cols]
        kp = split3(key_tile)
        qp = split3(query_tile)
        key_parts[g, pair] = six_left(kp)
        lhs = rows(*by_side(rows(kp[0], qp[0])), *by_side(rows(kp[1], qp[1])), *by_side(rows(kp[2], qp[2])))
        yield
        top = dot_nn(lanes(lhs, lhs), states(w1_parts, g, pair, 0, 256))
        yield
        low_terms = dot_nn(lhs[:64], states(w1_parts, g, pair, 256, 384))
        yield
        offset = b1[g, pair]
        z_one = sum3(top, 64) + low_terms + rows(rep8(offset[:8], 32), rep8(offset[8:], 32))
        hidden, slope_val = twice_gelu_and_slope(z_one)
        slope[g, pair] = rows(slope_val[:16], slope_val[32:48])
        for tile in range(2):
            act[g, pair, tile] = tile_parts(hidden, tile)
        yield

    def stage_out(g, pair, j, q_step, live):
        acts = lanes(act[g, pair, 0], act[g, pair, 1])
        top = dot_nt(acts, states(w2_parts, g, pair, 0, 256))
        yield
        low_terms = dot_nt(acts[:64], rows(states(w2_parts, g, pair, 256, 384), pad128))
        yield
        total = sum3(top, 64) + low_terms
        total = total[:, :128] + total[:, 128:]
        z_two[g, pair] = jnp.where(low_tall, total[:32], total[32:]) + rep8(b2[g, pair], 32)
        yield

    def stage_center(g, pair, j, q_step, live):
        z_val = z_two[g, pair]
        z_two[g, pair] = z_val - side_sums(z_val) * (1 / 64)
        yield

    def stage_norm(g, pair, j, q_step, live):
        z_val = z_two[g, pair]
        inv_std = lax.rsqrt(side_sums(z_val * z_val) * (1 / 64) + LN_EPS)
        normed = z_val * inv_std
        gain_tile = rep8(gain_pair[pair], 16)
        outs[g, out_rows(q_step, 1), 128 * pair:128 * pair + 128] = (normed[16:] * gain_tile + query_base[g, pair]).astype(bf16)
        key_inv[g, pair] = inv_std[:16]
        key_norm[g, pair] = normed[:16]
        d_norm[g, pair] = (normed[:16] * gain_tile + key_base[g, pair]) * (2.0 * gain_tile)
        yield

    def stage_back(g, pair, j, q_step, live):
        d_val = d_norm[g, pair]
        normed = key_norm[g, pair]
        mean_d = side_sums(d_val) * (1 / 64)
        mean_dn = side_sums(d_val * normed) * (1 / 64)
        d_val = key_inv[g, pair] * (d_val - mean_d - normed * mean_dn)
        d_two[g, pair] = rows(*split3(d_val))
        total = d_val[:8] + d_val[8:]
        for shift in (4, 2, 1):
            total = total + pltpu.roll(total, shift, 0)
        b2[g, pair] = b2[g, pair] - jnp.where(low[:8], live * rate[2 * pair], live * rate[2 * pair + 1]) * total
        yield

    def six_left(parts):
        return rows(parts[0], parts[0], parts[0], parts[1], parts[1], parts[2])

    def six_right(ref, g, pair, height, side):
        at = [part * height + side for part in range(3)]
        term = [lanes(ref[g, pair, 0, a:a + 16], ref[g, pair, 1, a:a + 16]) for a in at]
        return rows(term[0], term[1], term[2], term[0], term[1], term[0])

    def both_rates(first, second):
        return rows(jnp.full((64, 256), first, f32), jnp.full((64, 256), second, f32))

    def stage_second(g, pair, j, q_step, live):
        dp = d_two[g, pair]
        lhs = rows(*by_side(dp[:16]), *by_side(dp[16:32]), *by_side(dp[32:]))
        top = dot_nn(lanes(lhs, lhs), states(w2_parts, g, pair, 0, 256))
        yield
        low_terms = dot_nn(lhs[:32], states(w2_parts, g, pair, 256, 384))
        yield
        d_hidden = (sum3(top, 32) + low_terms) * slope[g, pair]
        for tile in range(2):
            d_one[g, pair, tile] = tile_parts(d_hidden, tile)
        yield

    def stage_second_update(g, pair, j, q_step, live):
        dp = d_two[g, pair]
        turned = six_left([dp[:16], dp[16:32], dp[32:]]).T
        yield
        grads = []
        for side in range(2):
            grads.append(dot_nn(turned[64 * side:64 * side + 64], six_right(act, g, pair, 64, 32 * side)))
            yield
        scale = [0.25 * live * rate[2 * pair + side] for side in range(2)]
        new = w2[g, pair] - both_rates(*scale) * rows(*grads)
        w2[g, pair] = new
        for tile in range(2):
            w2_parts[g, pair, tile] = tile_parts(new, tile)
        yield

    def stage_first_update(g, pair, j, q_step, live):
        turned = key_parts[g, pair].T
        yield
        grads = []
        for side in range(2):
            grads.append(dot_nn(rows(turned[64 * side:64 * side + 64], count_rows), six_right(d_one, g, pair, 32, 16 * side)))
            yield
        scale = [live * rate[2 * pair + side] for side in range(2)]
        new = w1[g, pair] - both_rates(*scale) * rows(grads[0][:64], grads[1][:64])
        w1[g, pair] = new
        for tile in range(2):
            w1_parts[g, pair, tile] = tile_parts(new, tile)
        offset = b1[g, pair]
        b1[g, pair] = rows(offset[:8] - scale[0] * grads[0][64:72], offset[8:] - scale[1] * grads[1][64:72])
        yield

    units = [(g, pair) for g in range(seqs) for pair in range(heads // 2)]
    batches = len(units) // BATCH
    delays = (0, 1, 2, 3, 5, 5, 6, 6)
    stages = {name: (delay, stage) for name, delay, stage in zip('ABMCDEGF', delays, (
        stage_hidden, stage_out, stage_center, stage_norm, stage_back, stage_second, stage_second_update, stage_first_update))}

    def run_turn(turn, step, skip):
        running = {}
        for name in ORDER:
            for unit in range(BATCH):
                delay, stage = stages[name]
                j, batch = divmod(turn - delay, batches)
                if skip(j, delay):
                    continue
                if (name, unit) not in running:
                    g, pair = units[batch * BATCH + unit]
                    running[name, unit] = stage(g, pair, j, jnp.maximum(step + j - 1, 0), jnp.where(step + j >= 0, 1.0, 0.0) if j < 0 else 1.0)
                next(running[name, unit])
        for stage in running.values():
            next(stage, None)

    def body(step, next_turn=None):
        last = next_turn is None
        shift_in()
        projection = first_rows() if last else project(next_turn)
        count = 0
        for turn in range(batches * (1 if last else ahead)):
            run_turn(turn, step, lambda j, delay: last and j >= 0 and delay > 3)
            if count >= PROJECT_FROM and (count - PROJECT_FROM) % PROJECT_EVERY == 0:
                next(projection, None)
                if last:
                    next(projection, None)
            count += 1
        for _ in projection:
            pass

    for turn in range(P0):
        pass_on(jnp.int32(turn))
    turns = steps // ahead
    def rows_of(count):
        return outs.at[:, pl.ds(0, count * MINI_BATCH)]

    def done(count, send, recv):
        return remote(rows_of(count), rows_of(count), send, recv, heads=other_row)

    def arrive(part):
        pltpu.make_async_copy(rows_of(part_steps), rows_of(part_steps), own_sem.at[part]).wait()

        @pl.loop(0, parts_of_seq)
        def _(place):
            done(part_steps, out_send.at[0], out_recv.at[other_row, place, part]).wait_recv()

            @pl.when(me != place)
            def _():
                done(part_steps, out_send.at[0], out_recv.at[row_axis, place, part]).wait_recv()

    w_load = pltpu.make_async_copy(w_full, w_all, w_own)
    num_seqs = parts_of_seq * seqs
    first_load = pltpu.make_async_copy(o_full.at[:, pl.ds(0, part_rows)], o_first, o_sem.at[0])
    first_put = pltpu.make_async_copy(y_first, y_early.at[:, pl.ds(0, part_rows)], y_sem.at[0])

    def first_rows():
        group = 4
        for at in range(0, num_seqs, group):
            for col in range(0, w_all.shape[1], 256):
                val = o_first[at:at + group].reshape(group * part_rows, 2 * width)
                y_first[at:at + group, :, col:col + 256] = dot_nn(val, w_all[:, col:col + 256]).astype(bf16).reshape(group, part_rows, 256)
                yield

    half_turns = turns // 2

    def loop_body(turn, carry):
        step = turn * ahead
        pass_on(turn + P0 + PA * (1 - me // 2))
        send_far(turn)

        @pl.when(turn == turns - 1)
        def _():
            w_keep.wait()
            w_swap.wait()
            w_load.start()
            arrive(0)
            first_load.start()

        @pl.when(turn <= 1)
        def _():
            wait_tokens(turn)
            for _ in project(turn):
                pass

        @pl.when((turn >= 1) & (turn + 1 < turns))
        def _():
            wait_tokens(turn + 1)

        @pl.when((me >= 2) & (turn == WT))
        def _():
            w_swap.start()

        @pl.when(turn >= 2)
        def _():
            send_row(step - 2 * ahead, ahead)

        @pl.when((turn >= 2) & ((me < 2) | (turn >= half_turns + 2)))
        def _():
            send_across(step - 2 * ahead, ahead)

        @pl.when((turn >= half_turns) & (me >= 2))
        def _():
            send_across(step - half_turns * ahead, ahead)

        body(step, lax.rem(turn + jnp.minimum(turn, 1), turns))
        return carry

    lax.fori_loop(0, turns, loop_body, 0)
    send_row(jnp.int32(steps - 2 * ahead), ahead)
    send_across(jnp.int32(steps - 2 * ahead), ahead)
    w_load.wait()
    first_load.wait()
    body(jnp.int32(steps))
    send_row(jnp.int32(steps - 2), 1)
    send_across(jnp.int32(steps - 2), 1)
    for turn in range(batches, batches + 3):
        run_turn(turn, jnp.int32(steps), lambda j, delay: j != 0 or delay > 3)
    def tokens_sent(slot, count):
        some = tok.at[:, pl.ds(0, count * MINI_BATCH)]
        remote(some, some, tok_send.at[slot], pass_recv.at[0], heads=other_row).wait_send()

    tokens_sent(0, own_steps)
    for slot, more, cond in ((1, 4, me == 0), (2, -2, me >= 2)):
        @pl.when(cond)
        def _():
            tokens_sent(slot, own_steps + more)

        @pl.when(jnp.logical_not(cond))
        def _():
            tokens_sent(slot, own_steps)

    send_row(jnp.int32(steps - 1), 1)
    send_across(jnp.int32(steps - 1), 1)

    first_put.start()
    arrive(1)
    several = 4
    blocks = num_seqs // several
    second_rows = pl.ds(part_rows, part_rows)

    def fetch(block):
        return pltpu.make_async_copy(o_full.at[pl.ds(several * block, several), second_rows], o_block.at[lax.rem(block, 2)], o_sem.at[lax.rem(block, 2)])

    def put(block):
        return pltpu.make_async_copy(y_block.at[lax.rem(block, 2)], y_early.at[pl.ds(several * block, several), second_rows], y_sem.at[1 + lax.rem(block, 2)])

    fetch(jnp.int32(0)).start()

    def early_block(block, carry):
        @pl.when(block + 1 < blocks)
        def _():
            fetch(block + 1).start()

        @pl.when(block >= 2)
        def _():
            put(block - 2).wait()

        fetch(block).wait()
        slot = lax.rem(block, 2)
        val = o_block[slot].reshape(several * part_rows, 2 * width)
        for col in range(0, w_all.shape[1], 256):
            y_block[slot, :, :, col:col + 256] = dot_nn(val, w_all[:, col:col + 256]).astype(bf16).reshape(several, part_rows, 256)
        put(block).start()
        return carry

    lax.fori_loop(0, blocks, early_block, 0)
    first_put.wait()
    put(jnp.int32(blocks - 2)).wait()
    put(jnp.int32(blocks - 1)).wait()
    done(steps - own_steps, out_send.at[0], out_recv.at[0, 0, 0]).wait_send()
    done(steps, out_send.at[1], out_recv.at[0, 0, 0]).wait_send()
    arrive(2)


def late_kernel(y_early, outs, w_full, y_ref, w_all, o_late, y_late, y_kept, in_sem, out_sem, w_sem):
    num_seqs, late = o_late.shape[:2]
    early = y_kept.shape[1]
    parts = in_sem.shape[1]
    group = num_seqs // parts
    early_rows, late_rows = pl.ds(0, early), pl.ds(early, late)
    w_cols = [slice(col, col + 256) for col in range(0, w_all.shape[1], 256)]
    w_loads = [pltpu.make_async_copy(w_full.at[:, cols], w_all.at[:, cols], w_sem.at[i]) for i, cols in enumerate(w_cols)]

    def some(part):
        return pl.ds(group * part, group)

    late_in = [pltpu.make_async_copy(outs.at[some(i), late_rows], o_late.at[some(i)], in_sem.at[0, i]) for i in range(parts)]
    early_in = [pltpu.make_async_copy(y_early.at[some(i)], y_kept.at[some(i)], in_sem.at[1, i]) for i in range(parts)]
    late_out = [pltpu.make_async_copy(y_late.at[some(i)], y_ref.at[some(i), late_rows], out_sem.at[0, i]) for i in range(parts)]
    early_out = [pltpu.make_async_copy(y_kept.at[some(i)], y_ref.at[some(i), early_rows], out_sem.at[1, i]) for i in range(parts)]
    for copy in late_in[:1] + w_loads + late_in[1:] + early_in:
        copy.start()
    for i in range(parts):
        late_in[i].wait()
        val = o_late[some(i)].reshape(group * late, o_late.shape[2])
        for cols, w_load in zip(w_cols, w_loads):
            if i == 0:
                w_load.wait()
            y_late[some(i), :, cols] = dot_nn(val, w_all[:, cols]).astype(bf16).reshape(group, late, 256)
        early_in[i].wait()
        early_out[i].start()
        late_out[i].start()
    for copy in early_out + late_out:
        copy.wait()


def finish(outs, w_full, y_early):
    num_seqs, own_len, width = outs.shape
    early, model_dim = y_early.shape[1:]
    late = own_len - early
    hbm = pl.BlockSpec(memory_space=pl.ANY)
    dma = pltpu.SemaphoreType.DMA
    return pl.pallas_call(
        late_kernel,
        out_shape=jax.ShapeDtypeStruct((num_seqs, own_len, model_dim), bf16),
        in_specs=[hbm] * 3,
        out_specs=hbm,
        scratch_shapes=[pltpu.VMEM((width, model_dim), bf16), pltpu.VMEM((num_seqs, late, width), bf16), pltpu.VMEM((num_seqs, late, model_dim), bf16),
                        pltpu.VMEM((num_seqs, early, model_dim), bf16), dma((2, KP)), dma((2, KP)), dma((model_dim // 256,))],
        compiler_params=pltpu.CompilerParams(vmem_limit_bytes=60 * 2 ** 20),
    )(y_early, outs, w_full)


def run_layer(tokens, theta_k, theta_q, theta_v, w_out, w1, w2t, b1, b2, gain, bias, rate, parts_of_seq):
    num_seqs, own_len, model_dim = tokens.shape
    seqs = num_seqs // parts_of_seq
    steps = own_len * parts_of_seq // MINI_BATCH
    heads = w1.shape[0]
    width = theta_k.shape[1]
    smem = pl.BlockSpec(memory_space=pltpu.SMEM)
    hbm = pl.BlockSpec(memory_space=pl.ANY)
    each = [((128, 256), f32), ((128, 256), f32), ((2, 384, 128), bf16), ((2, 384, 128), bf16), ((16, 256), f32),
            ((2, 192, 128), bf16), ((32, 256), f32), ((2, 96, 128), bf16),
            ((8, 128), f32), ((96, 128), bf16), ((16, 128), f32), ((16, 128), f32), ((32, 128), f32),
            ((16, 128), f32), ((16, 128), f32), ((16, 128), f32), ((48, 128), bf16)]
    scratch = [pltpu.VMEM(val.shape, val.dtype) for val in (theta_k, theta_q, theta_v, w1, w2t)]
    scratch += [pltpu.VMEM((seqs, heads // 2) + shape, dtype) for shape, dtype in each]
    scratch += [pltpu.VMEM((heads // 2, 8, 128), f32)] * 2
    scratch += [pltpu.VMEM((seqs, steps * MINI_BATCH, model_dim), bf16), pltpu.VMEM((seqs, steps * MINI_BATCH, width), bf16)]
    ahead = AHEAD
    several = pltpu.VMEM((ahead, seqs, MINI_BATCH, width), f32)
    scratch += [several] * 3 + [pltpu.VMEM((seqs, MINI_BATCH, width), f32)] + [several] * 3
    own_steps = steps // parts_of_seq
    dma = pltpu.SemaphoreType.DMA
    half_turns = steps // (2 * AHEAD)
    scratch += [dma((9,)), dma((3,)), dma, dma, dma((half_turns,)), dma((half_turns,)), dma((2,)), dma((2,)), dma((2, parts_of_seq, 3)), dma((3,)), dma, dma, dma]
    early = 2 * own_len // 3
    scratch += [pltpu.VMEM((2 * width, model_dim), bf16), pltpu.VMEM((2, 4, early // 2, 2 * width), bf16), pltpu.VMEM((2, 4, early // 2, model_dim), bf16),
                pltpu.VMEM((num_seqs, early // 2, 2 * width), bf16), pltpu.VMEM((num_seqs, early // 2, model_dim), bf16), dma((2,)), dma((3,))]
    scratch += [pltpu.VMEM(val.shape, val.dtype) for val in (b1, b2, gain, bias)]
    return pl.pallas_call(
        functools.partial(layer_kernel, steps, seqs, heads, ahead, parts_of_seq),
        out_shape=(jax.ShapeDtypeStruct((num_seqs, own_len, 2 * width), bf16), jax.ShapeDtypeStruct((2 * width, model_dim), bf16),
                   jax.ShapeDtypeStruct((num_seqs, early, model_dim), bf16)),
        in_specs=[hbm] * 11 + [smem],
        out_specs=(hbm, hbm, hbm),
        scratch_shapes=scratch,
        compiler_params=pltpu.CompilerParams(vmem_limit_bytes=60 * 2 ** 20, collective_id=0, has_side_effects=True),
    )(tokens, w_out, theta_k, theta_q, theta_v, w1, w2t, b1, b2, gain, bias, rate)


def solution(mesh):
    parts_of_seq = mesh.shape['seq']

    def local_fn(tokens, theta_q, theta_k, theta_v, w_out, w_one, b_one, w_two, b_two, ln_gain, ln_bias, inner_lr):
        outs, w_full, y_early = run_layer(tokens, theta_k, theta_q, theta_v, w_out, w_one, jnp.swapaxes(w_two, 1, 2), b_one, b_two, ln_gain, ln_bias, inner_lr, parts_of_seq)
        return finish(outs, w_full, y_early)

    arg_specs = (P('data', 'seq', None), P(None, 'heads'), P(None, 'heads'), P(None, 'heads'), P('heads', None), P('heads', None, None), P('heads', None), P('heads', None, None), P('heads', None), P('heads', None), P('heads', None), P('heads'))
    return jax.shard_map(local_fn, mesh=mesh, in_specs=arg_specs, out_specs=P('data', 'seq', None), check_vma=False)
```

```python
import functools

import jax
import jax.numpy as jnp
from jax import lax
from jax.experimental import pallas as pl
from jax.experimental.pallas import tpu as pltpu
from jax.sharding import PartitionSpec as P

MINI_BATCH = 16
AHEAD = 2
BATCH = 2
ORDER = 'MCDGFAABEBAEABEGGGFFF'
PROJECT_EVERY = 1
PROJECT_FROM = 0
FAR0, FAR1, FAR2, PA, WT, P0 = -3, 6, -9, 5, 10, 2
WHOLE = 2
KP = 4
LN_EPS = 1e-6
GELU_C0 = 0.7978845608028654
GELU_C1 = 0.044715
f32 = jnp.float32
bf16 = jnp.bfloat16


def split3(val):
    high = val.astype(bf16)
    rest = val - high.astype(f32)
    mid = rest.astype(bf16)
    return high, mid, (rest - mid.astype(f32)).astype(bf16)


def dot_nn(lhs, rhs):
    return lax.dot_general(lhs, rhs, (((1,), (0,)), ((), ())), preferred_element_type=f32)


def dot_nt(lhs, rhs):
    return lax.dot_general(lhs, rhs, (((1,), (1,)), ((), ())), preferred_element_type=f32)


def dot_tn(lhs, rhs):
    return lax.dot_general(lhs, rhs, (((0,), (0,)), ((), ())), preferred_element_type=f32)


def rows(*parts):
    return jnp.concatenate(parts, 0)


def lanes(*parts):
    return jnp.concatenate(parts, 1)


def rep8(val, count):
    return rows(*([val] * (count // 8)))


def sum3(val, count):
    return val[0:count] + val[count:2 * count] + val[2 * count:3 * count]


def twice_gelu_and_slope(z_val):
    square = z_val * z_val
    tanh_val = jnp.tanh(z_val * (GELU_C0 + (GELU_C0 * GELU_C1) * square))
    plus = 1.0 + tanh_val
    slope = plus + (1.0 - tanh_val * tanh_val) * (z_val * (GELU_C0 + (3 * GELU_C0 * GELU_C1) * square))
    return z_val * plus, slope


def tile_parts(val, tile):
    return rows(*split3(val[:, 128 * tile:128 * tile + 128]))


def eight_rows(row, twice):
    row = lanes(row, row) if twice else row
    return jnp.broadcast_to(row, (8, row.shape[1]))


def layer_kernel(steps, seqs, heads, ahead, parts_of_seq, tokens, w_out, theta_k_at, theta_q_at, theta_v_at, w1_at, w2_at, b1_at, b2_at, gain_at, bias_at, rate_in,
                 o_full, w_full, y_early, theta_k, theta_q, theta_v, w1_in, w2_in,
                 w1, w2, w1_parts, w2_parts, b1, act, slope, d_one, b2, key_parts, key_base, query_base, z_two, key_norm, key_inv, d_norm, d_two, gain_pair, bias_pair,
                 tok, outs, k_now, v_now, q_now, q_last, k_new, v_new, q_new,
                 load_sem, tok_send, own_recv, near_recv, half_recv, pass_recv, whole_recv, out_send, out_recv, own_sem, w_send, w_recv, w_own,
                 w_all, o_block, y_block, o_first, y_first, o_sem, y_sem, b1_in, b2_in, gain_in, bias_in):
    low = lax.broadcasted_iota(jnp.int32, (16, 128), 1) < 64
    pad128 = jnp.zeros((128, 256), bf16)
    low_tall = lax.broadcasted_iota(jnp.int32, (32, 128), 1) < 64
    count_rows = jnp.where(lax.broadcasted_iota(jnp.int32, (16, 96), 1) < 48, 1.0, 0.0).astype(bf16)
    width = 64 * heads
    own_steps = steps // parts_of_seq
    early_steps = 2 * own_steps // 3
    part_steps = own_steps // 3
    part_rows = part_steps * MINI_BATCH
    row_axis = lax.axis_index('heads')
    me = lax.axis_index('seq')
    other_row = 1 - row_axis
    mesh_ids = pl.DeviceIdType.MESH

    def other_core(place):
        return place + 1 - 2 * lax.rem(place, 2)

    near = other_core(me)

    barrier = pltpu.get_barrier_semaphore()
    for shift_row in range(2):
        for shift in range(parts_of_seq):
            if shift_row or shift:
                pl.semaphore_signal(barrier, inc=1, device_id={'heads': lax.rem(row_axis + shift_row, 2), 'seq': lax.rem(me + shift, parts_of_seq)}, device_id_type=mesh_ids)
    pl.semaphore_wait(barrier, 2 * parts_of_seq - 1)

    half = seqs // 2
    my_half = pl.ds(half * row_axis, half)
    far_from = (1 - me // 2) * (steps // 2)

    def remote(src, dst, send, recv, **device):
        return pltpu.make_async_remote_copy(src, dst, send, recv, device_id=device, device_id_type=mesh_ids)

    pair_rows = ahead * MINI_BATCH
    own_turns = own_steps // ahead
    far_turns = 2 * own_turns
    far_turn = far_turns * (1 - me // 2)

    def tok_rows(turn, count=1):
        return pl.ds(pl.multiple_of(pair_rows * turn, pair_rows), pair_rows * count)

    def is_whole(turn):
        return (turn >= WHOLE) & (turn < WHOLE + 2)

    def send_far(turn):
        piece = turn - FAR0 - FAR1 * me - FAR2 * (me // 2)

        @pl.when((piece >= 0) & (piece < own_turns))
        def _():
            at = me * own_turns + piece
            whole = is_whole(at)

            @pl.loop(0, 2)
            def _(core):
                dest = 2 * (1 - me // 2) + core

                @pl.when(whole)
                def _():
                    src = tokens.at[pl.ds(seqs * dest, seqs), tok_rows(piece)]
                    remote(src, tok.at[:, tok_rows(at)], tok_send.at[1], whole_recv.at[at - WHOLE], seq=dest).start()

                @pl.when(jnp.logical_not(whole))
                def _():
                    src = tokens.at[pl.ds(seqs * dest + half * row_axis, half), tok_rows(piece)]
                    remote(src, tok.at[my_half, tok_rows(at)], tok_send.at[1], half_recv.at[lax.rem(at, far_turns)], seq=dest).start()

    def is_far(turn):
        return (turn >= far_turn) & (turn < far_turn + far_turns)

    def pass_on(turn):
        @pl.when(is_far(turn) & jnp.logical_not(is_whole(turn)))
        def _():
            spot = tok.at[my_half, tok_rows(turn)]
            slot = turn - far_turn
            remote(spot, spot, tok_send.at[2], half_recv.at[slot], heads=other_row).wait_recv()
            remote(spot, spot, tok_send.at[2], pass_recv.at[slot], heads=other_row).start()

    def wait_tokens(turn):
        @pl.when(is_far(turn) & is_whole(turn))
        def _():
            spot = tok.at[:, tok_rows(turn)]
            remote(spot, spot, tok_send.at[1], whole_recv.at[turn - WHOLE], heads=other_row).wait_recv()

        @pl.when(is_far(turn) & jnp.logical_not(is_whole(turn)))
        def _():
            spot = tok.at[my_half, tok_rows(turn)]
            remote(spot, spot, tok_send.at[2], pass_recv.at[turn - far_turn], heads=other_row).wait_recv()

        @pl.when(lax.rem(turn, own_turns) == 0)
        def _():
            spot = tok.at[:, tok_rows(turn, own_turns)]

            @pl.when(turn // own_turns == me)
            def _():
                pltpu.make_async_copy(spot, spot, own_recv).wait()

            @pl.when(turn // own_turns == near)
            def _():
                remote(spot, spot, tok_send.at[0], near_recv, seq=near).wait_recv()

    for turn in range(FAR0, 0):
        send_far(jnp.int32(turn))
    own_block = tok.at[:, tok_rows(me * own_turns, own_turns)]
    pltpu.make_async_copy(tokens.at[pl.ds(seqs * me, seqs)], own_block, own_recv).start()
    remote(tokens.at[pl.ds(seqs * near, seqs)], own_block, tok_send.at[0], near_recv, seq=near).start()
    loads = [pltpu.make_async_copy(src, dst, load_sem.at[i]) for i, (src, dst) in enumerate((
        (w1_at, w1_in), (w2_at, w2_in), (b1_at, b1_in), (b2_at, b2_in), (gain_at, gain_in), (bias_at, bias_in),
        (theta_k_at, theta_k), (theta_q_at, theta_q), (theta_v_at, theta_v)))]
    for load in loads:
        load.start()

    my_w_rows = w_full.at[pl.ds(pl.multiple_of(row_axis * width, width), width)]
    w_swap = pltpu.make_async_remote_copy(w_out, my_w_rows, w_send, w_recv, device_id={'heads': other_row}, device_id_type=mesh_ids)
    w_keep = pltpu.make_async_copy(w_out, my_w_rows, w_own)
    w_keep.start()

    @pl.when(me < 2)
    def _():
        w_swap.start()

    def out_rows(step, count):
        return pl.ds(pl.multiple_of(MINI_BATCH * step, MINI_BATCH), MINI_BATCH * count)

    def out_copy(step, count):
        place = pl.ds(seqs * me, seqs), out_rows(lax.rem(step, own_steps), count), pl.ds(pl.multiple_of(width * row_axis, width), width)
        late = lax.rem(step, own_steps) // part_steps
        return outs.at[:, out_rows(step, count)], o_full.at[place], step // own_steps, late

    def send_row(step, count):
        src, dst, owner, late = out_copy(step, count)

        @pl.when(owner != me)
        def _():
            remote(src, dst, out_send.at[0], out_recv.at[row_axis, me, late], seq=owner).start()

        @pl.when(owner == me)
        def _():
            pltpu.make_async_copy(src, dst, own_sem.at[late]).start()

    def send_across(step, count):
        src, dst, owner, late = out_copy(step, count)
        remote(src, dst, out_send.at[1], out_recv.at[row_axis, me, late], heads=other_row, seq=owner).start()

    for load in loads:
        load.wait()
    for pair in range(heads // 2):
        even, odd = 2 * pair, 2 * pair + 1

        def pair_row(source):
            return jnp.broadcast_to(lanes(source[even:even + 1], source[odd:odd + 1]), (8, 128))

        gain_pair[pair] = pair_row(gain_in)
        bias_pair[pair] = pair_row(bias_in)
        offset = pair_row(b2_in)
        hidden_offset = rows(eight_rows(b1_in[even:even + 1], False), eight_rows(b1_in[odd:odd + 1], False))
        first = rows(w1_in[even], w1_in[odd])
        second = rows(0.5 * w2_in[even], 0.5 * w2_in[odd])
        for g in range(seqs):
            w1[g, pair] = first
            w2[g, pair] = second
            b1[g, pair] = hidden_offset
            b2[g, pair] = offset
        for tile in range(2):
            first_parts, second_parts = tile_parts(first, tile), tile_parts(second, tile)
            for g in range(seqs):
                w1_parts[g, pair, tile] = first_parts
                w2_parts[g, pair, tile] = second_parts
    q_last[...] = jnp.zeros(q_last.shape, f32)

    @pl.loop(0, seqs)
    def _(g):
        for ref in (act, slope, d_one, key_parts, key_base, query_base, z_two, key_norm, key_inv, d_norm, d_two):
            ref[g] = jnp.zeros(ref.shape[1:], ref.dtype)

    rate = [rate_in[h] * (1 / MINI_BATCH) for h in range(heads)]

    def both(unit):
        return [2 * pair + side for pair in unit for side in range(2)]

    def project(turn):
        for theta, target in ((theta_k, k_new), (theta_q, q_new), (theta_v, v_new)):
            for col in range(0, width, 256):
                toks = tok[:, tok_rows(turn)].reshape(seqs * pair_rows, tok.shape[2])
                found = dot_nn(toks, theta[:, col:col + 256]).reshape(seqs, ahead, MINI_BATCH, 256)
                for j in range(ahead):
                    target[j, :, :, col:col + 256] = found[:, j]
                yield

    def shift_in():
        k_now[...] = k_new[...]
        v_now[...] = v_new[...]
        q_now[0] = q_last[...]
        for j in range(1, ahead):
            q_now[j] = q_new[j - 1]
        q_last[...] = q_new[ahead - 1]

    def states(ref, g, pair, first, last):
        return lanes(ref[g, pair, 0, first:last], ref[g, pair, 1, first:last])

    def by_side(val):
        keep = lax.broadcasted_iota(jnp.int32, val.shape, 1) < 64
        zero = jnp.zeros(val.shape, val.dtype)
        return [jnp.where(keep, val, zero), jnp.where(keep, zero, val)]

    def side_sums(val):
        keep = low if val.shape[0] == 16 else low_tall
        return jnp.where(keep, jnp.sum(jnp.where(keep, val, 0.0), 1, keepdims=True), jnp.sum(jnp.where(keep, 0.0, val), 1, keepdims=True))

    def stage_hidden(g, pair, j, q_step, live):
        cols = slice(128 * pair, 128 * pair + 128)
        key_tile = k_now[j, g, :, cols]
        query_tile = q_now[j, g, :, cols]
        bias_tile = rep8(bias_pair[pair], 16)
        query_base[g, pair] = query_tile + bias_tile
        key_base[g, pair] = (key_tile + bias_tile) - v_now[j, g, :, cols]
        kp = split3(key_tile)
        qp = split3(query_tile)
        key_parts[g, pair] = six_left(kp)
        lhs = rows(*by_side(rows(kp[0], qp[0])), *by_side(rows(kp[1], qp[1])), *by_side(rows(kp[2], qp[2])))
        yield
        top = dot_nn(lanes(lhs, lhs), states(w1_parts, g, pair, 0, 256))
        yield
        low_terms = dot_nn(lhs[:64], states(w1_parts, g, pair, 256, 384))
        yield
        offset = b1[g, pair]
        z_one = sum3(top, 64) + low_terms + rows(rep8(offset[:8], 32), rep8(offset[8:], 32))
        hidden, slope_val = twice_gelu_and_slope(z_one)
        slope[g, pair] = rows(slope_val[:16], slope_val[32:48])
        for tile in range(2):
            act[g, pair, tile] = tile_parts(hidden, tile)
        yield

    def stage_out(g, pair, j, q_step, live):
        acts = lanes(act[g, pair, 0], act[g, pair, 1])
        top = dot_nt(acts, states(w2_parts, g, pair, 0, 256))
        yield
        low_terms = dot_nt(acts[:64], rows(states(w2_parts, g, pair, 256, 384), pad128))
        yield
        total = sum3(top, 64) + low_terms
        total = total[:, :128] + total[:, 128:]
        z_two[g, pair] = jnp.where(low_tall, total[:32], total[32:]) + rep8(b2[g, pair], 32)
        yield

    def stage_center(g, pair, j, q_step, live):
        z_val = z_two[g, pair]
        z_two[g, pair] = z_val - side_sums(z_val) * (1 / 64)
        yield

    def stage_norm(g, pair, j, q_step, live):
        z_val = z_two[g, pair]
        inv_std = lax.rsqrt(side_sums(z_val * z_val) * (1 / 64) + LN_EPS)
        normed = z_val * inv_std
        gain_tile = rep8(gain_pair[pair], 16)
        outs[g, out_rows(q_step, 1), 128 * pair:128 * pair + 128] = (normed[16:] * gain_tile + query_base[g, pair]).astype(bf16)
        key_inv[g, pair] = inv_std[:16]
        key_norm[g, pair] = normed[:16]
        d_norm[g, pair] = (normed[:16] * gain_tile + key_base[g, pair]) * (2.0 * gain_tile)
        yield

    def stage_back(g, pair, j, q_step, live):
        d_val = d_norm[g, pair]
        normed = key_norm[g, pair]
        mean_d = side_sums(d_val) * (1 / 64)
        mean_dn = side_sums(d_val * normed) * (1 / 64)
        d_val = key_inv[g, pair] * (d_val - mean_d - normed * mean_dn)
        d_two[g, pair] = rows(*split3(d_val))
        total = d_val[:8] + d_val[8:]
        for shift in (4, 2, 1):
            total = total + pltpu.roll(total, shift, 0)
        b2[g, pair] = b2[g, pair] - jnp.where(low[:8], live * rate[2 * pair], live * rate[2 * pair + 1]) * total
        yield

    def six_left(parts):
        return rows(parts[0], parts[0], parts[0], parts[1], parts[1], parts[2])

    def six_right(ref, g, pair, height, side):
        at = [part * height + side for part in range(3)]
        term = [lanes(ref[g, pair, 0, a:a + 16], ref[g, pair, 1, a:a + 16]) for a in at]
        return rows(term[0], term[1], term[2], term[0], term[1], term[0])

    def both_rates(first, second):
        return rows(jnp.full((64, 256), first, f32), jnp.full((64, 256), second, f32))

    def stage_second(g, pair, j, q_step, live):
        dp = d_two[g, pair]
        lhs = rows(*by_side(dp[:16]), *by_side(dp[16:32]), *by_side(dp[32:]))
        top = dot_nn(lanes(lhs, lhs), states(w2_parts, g, pair, 0, 256))
        yield
        low_terms = dot_nn(lhs[:32], states(w2_parts, g, pair, 256, 384))
        yield
        d_hidden = (sum3(top, 32) + low_terms) * slope[g, pair]
        for tile in range(2):
            d_one[g, pair, tile] = tile_parts(d_hidden, tile)
        yield

    def stage_second_update(g, pair, j, q_step, live):
        dp = d_two[g, pair]
        turned = six_left([dp[:16], dp[16:32], dp[32:]]).T
        yield
        grads = []
        for side in range(2):
            grads.append(dot_nn(turned[64 * side:64 * side + 64], six_right(act, g, pair, 64, 32 * side)))
            yield
        scale = [0.25 * live * rate[2 * pair + side] for side in range(2)]
        new = w2[g, pair] - both_rates(*scale) * rows(*grads)
        w2[g, pair] = new
        for tile in range(2):
            w2_parts[g, pair, tile] = tile_parts(new, tile)
        yield

    def stage_first_update(g, pair, j, q_step, live):
        turned = key_parts[g, pair].T
        yield
        grads = []
        for side in range(2):
            grads.append(dot_nn(rows(turned[64 * side:64 * side + 64], count_rows), six_right(d_one, g, pair, 32, 16 * side)))
            yield
        scale = [live * rate[2 * pair + side] for side in range(2)]
        new = w1[g, pair] - both_rates(*scale) * rows(grads[0][:64], grads[1][:64])
        w1[g, pair] = new
        for tile in range(2):
            w1_parts[g, pair, tile] = tile_parts(new, tile)
        offset = b1[g, pair]
        b1[g, pair] = rows(offset[:8] - scale[0] * grads[0][64:72], offset[8:] - scale[1] * grads[1][64:72])
        yield

    units = [(g, pair) for g in range(seqs) for pair in range(heads // 2)]
    batches = len(units) // BATCH
    delays = (0, 1, 2, 3, 5, 5, 6, 6)
    stages = {name: (delay, stage) for name, delay, stage in zip('ABMCDEGF', delays, (
        stage_hidden, stage_out, stage_center, stage_norm, stage_back, stage_second, stage_second_update, stage_first_update))}

    def run_turn(turn, step, skip):
        running = {}
        for name in ORDER:
            for unit in range(BATCH):
                delay, stage = stages[name]
                j, batch = divmod(turn - delay, batches)
                if skip(j, delay):
                    continue
                if (name, unit) not in running:
                    g, pair = units[batch * BATCH + unit]
                    running[name, unit] = stage(g, pair, j, jnp.maximum(step + j - 1, 0), jnp.where(step + j >= 0, 1.0, 0.0) if j < 0 else 1.0)
                next(running[name, unit])
        for stage in running.values():
            next(stage, None)

    def body(step, next_turn=None):
        last = next_turn is None
        shift_in()
        projection = first_rows() if last else project(next_turn)
        count = 0
        for turn in range(batches * (1 if last else ahead)):
            run_turn(turn, step, lambda j, delay: last and j >= 0 and delay > 3)
            if count >= PROJECT_FROM and (count - PROJECT_FROM) % PROJECT_EVERY == 0:
                next(projection, None)
                if last:
                    next(projection, None)
            count += 1
        for _ in projection:
            pass

    for turn in range(P0):
        pass_on(jnp.int32(turn))
    turns = steps // ahead
    def rows_of(count):
        return outs.at[:, pl.ds(0, count * MINI_BATCH)]

    def done(count, send, recv):
        return remote(rows_of(count), rows_of(count), send, recv, heads=other_row)

    def arrive(part):
        pltpu.make_async_copy(rows_of(part_steps), rows_of(part_steps), own_sem.at[part]).wait()

        @pl.loop(0, parts_of_seq)
        def _(place):
            done(part_steps, out_send.at[0], out_recv.at[other_row, place, part]).wait_recv()

            @pl.when(me != place)
            def _():
                done(part_steps, out_send.at[0], out_recv.at[row_axis, place, part]).wait_recv()

    w_load = pltpu.make_async_copy(w_full, w_all, w_own)
    num_seqs = parts_of_seq * seqs
    first_load = pltpu.make_async_copy(o_full.at[:, pl.ds(0, part_rows)], o_first, o_sem.at[0])
    first_put = pltpu.make_async_copy(y_first, y_early.at[:, pl.ds(0, part_rows)], y_sem.at[0])

    def first_rows():
        group = 4
        for at in range(0, num_seqs, group):
            for col in range(0, w_all.shape[1], 256):
                val = o_first[at:at + group].reshape(group * part_rows, 2 * width)
                y_first[at:at + group, :, col:col + 256] = dot_nn(val, w_all[:, col:col + 256]).astype(bf16).reshape(group, part_rows, 256)
                yield

    half_turns = turns // 2

    def loop_body(turn, carry):
        step = turn * ahead
        pass_on(turn + P0 + PA * (1 - me // 2))
        send_far(turn)

        @pl.when(turn == turns - 1)
        def _():
            w_keep.wait()
            w_swap.wait()
            w_load.start()
            arrive(0)
            first_load.start()

        @pl.when(turn <= 1)
        def _():
            wait_tokens(turn)
            for _ in project(turn):
                pass

        @pl.when((turn >= 1) & (turn + 1 < turns))
        def _():
            wait_tokens(turn + 1)

        @pl.when((me >= 2) & (turn == WT))
        def _():
            w_swap.start()

        @pl.when(turn >= 2)
        def _():
            send_row(step - 2 * ahead, ahead)

        @pl.when((turn >= 2) & ((me < 2) | (turn >= half_turns + 2)))
        def _():
            send_across(step - 2 * ahead, ahead)

        @pl.when((turn >= half_turns) & (me >= 2))
        def _():
            send_across(step - half_turns * ahead, ahead)

        body(step, lax.rem(turn + jnp.minimum(turn, 1), turns))
        return carry

    lax.fori_loop(0, turns, loop_body, 0)
    send_row(jnp.int32(steps - 2 * ahead), ahead)
    send_across(jnp.int32(steps - 2 * ahead), ahead)
    w_load.wait()
    first_load.wait()
    body(jnp.int32(steps))
    send_row(jnp.int32(steps - 2), 1)
    send_across(jnp.int32(steps - 2), 1)
    arrive(1)
    several = 4
    blocks = num_seqs // several
    second_rows = pl.ds(part_rows, part_rows)

    def fetch(block):
        return pltpu.make_async_copy(o_full.at[pl.ds(several * block, several), second_rows], o_block.at[lax.rem(block, 2)], o_sem.at[lax.rem(block, 2)])

    def put(block):
        return pltpu.make_async_copy(y_block.at[lax.rem(block, 2)], y_early.at[pl.ds(several * block, several), second_rows], y_sem.at[1 + lax.rem(block, 2)])

    fetch(jnp.int32(0)).start()

    for turn in range(batches, batches + 3):
        run_turn(turn, jnp.int32(steps), lambda j, delay: j != 0 or delay > 3)
    def tokens_sent(slot, count):
        some = tok.at[:, pl.ds(0, count * MINI_BATCH)]
        remote(some, some, tok_send.at[slot], pass_recv.at[0], heads=other_row).wait_send()

    tokens_sent(0, own_steps)
    for slot, more, cond in ((1, 4, me == 0), (2, -2, me >= 2)):
        @pl.when(cond)
        def _():
            tokens_sent(slot, own_steps + more)

        @pl.when(jnp.logical_not(cond))
        def _():
            tokens_sent(slot, own_steps)

    send_row(jnp.int32(steps - 1), 1)
    send_across(jnp.int32(steps - 1), 1)

    first_put.start()
    def early_block(block, carry):
        @pl.when(block + 1 < blocks)
        def _():
            fetch(block + 1).start()

        @pl.when(block >= 2)
        def _():
            put(block - 2).wait()

        fetch(block).wait()
        slot = lax.rem(block, 2)
        val = o_block[slot].reshape(several * part_rows, 2 * width)
        for col in range(0, w_all.shape[1], 256):
            y_block[slot, :, :, col:col + 256] = dot_nn(val, w_all[:, col:col + 256]).astype(bf16).reshape(several, part_rows, 256)
        put(block).start()
        return carry

    lax.fori_loop(0, blocks, early_block, 0)
    first_put.wait()
    put(jnp.int32(blocks - 2)).wait()
    put(jnp.int32(blocks - 1)).wait()
    done(steps - own_steps, out_send.at[0], out_recv.at[0, 0, 0]).wait_send()
    done(steps, out_send.at[1], out_recv.at[0, 0, 0]).wait_send()
    arrive(2)


def late_kernel(y_early, outs, w_full, y_ref, w_all, o_late, y_late, y_kept, in_sem, out_sem, w_sem):
    num_seqs, late = o_late.shape[:2]
    early = y_kept.shape[1]
    parts = in_sem.shape[1]
    group = num_seqs // parts
    early_rows, late_rows = pl.ds(0, early), pl.ds(early, late)
    w_cols = [slice(col, col + 256) for col in range(0, w_all.shape[1], 256)]
    w_loads = [pltpu.make_async_copy(w_full.at[:, cols], w_all.at[:, cols], w_sem.at[i]) for i, cols in enumerate(w_cols)]

    def some(part):
        return pl.ds(group * part, group)

    late_in = [pltpu.make_async_copy(outs.at[some(i), late_rows], o_late.at[some(i)], in_sem.at[0, i]) for i in range(parts)]
    early_in = [pltpu.make_async_copy(y_early.at[some(i)], y_kept.at[some(i)], in_sem.at[1, i]) for i in range(parts)]
    late_out = [pltpu.make_async_copy(y_late.at[some(i)], y_ref.at[some(i), late_rows], out_sem.at[0, i]) for i in range(parts)]
    early_out = [pltpu.make_async_copy(y_kept.at[some(i)], y_ref.at[some(i), early_rows], out_sem.at[1, i]) for i in range(parts)]
    for copy in late_in[:1] + w_loads + late_in[1:] + early_in:
        copy.start()
    for i in range(parts):
        late_in[i].wait()
        val = o_late[some(i)].reshape(group * late, o_late.shape[2])
        for cols, w_load in zip(w_cols, w_loads):
            if i == 0:
                w_load.wait()
            y_late[some(i), :, cols] = dot_nn(val, w_all[:, cols]).astype(bf16).reshape(group, late, 256)
        early_in[i].wait()
        early_out[i].start()
        late_out[i].start()
    for copy in early_out + late_out:
        copy.wait()


def finish(outs, w_full, y_early):
    num_seqs, own_len, width = outs.shape
    early, model_dim = y_early.shape[1:]
    late = own_len - early
    hbm = pl.BlockSpec(memory_space=pl.ANY)
    dma = pltpu.SemaphoreType.DMA
    return pl.pallas_call(
        late_kernel,
        out_shape=jax.ShapeDtypeStruct((num_seqs, own_len, model_dim), bf16),
        in_specs=[hbm] * 3,
        out_specs=hbm,
        scratch_shapes=[pltpu.VMEM((width, model_dim), bf16), pltpu.VMEM((num_seqs, late, width), bf16), pltpu.VMEM((num_seqs, late, model_dim), bf16),
                        pltpu.VMEM((num_seqs, early, model_dim), bf16), dma((2, KP)), dma((2, KP)), dma((model_dim // 256,))],
        compiler_params=pltpu.CompilerParams(vmem_limit_bytes=60 * 2 ** 20),
    )(y_early, outs, w_full)


def run_layer(tokens, theta_k, theta_q, theta_v, w_out, w1, w2t, b1, b2, gain, bias, rate, parts_of_seq):
    num_seqs, own_len, model_dim = tokens.shape
    seqs = num_seqs // parts_of_seq
    steps = own_len * parts_of_seq // MINI_BATCH
    heads = w1.shape[0]
    width = theta_k.shape[1]
    smem = pl.BlockSpec(memory_space=pltpu.SMEM)
    hbm = pl.BlockSpec(memory_space=pl.ANY)
    each = [((128, 256), f32), ((128, 256), f32), ((2, 384, 128), bf16), ((2, 384, 128), bf16), ((16, 256), f32),
            ((2, 192, 128), bf16), ((32, 256), f32), ((2, 96, 128), bf16),
            ((8, 128), f32), ((96, 128), bf16), ((16, 128), f32), ((16, 128), f32), ((32, 128), f32),
            ((16, 128), f32), ((16, 128), f32), ((16, 128), f32), ((48, 128), bf16)]
    scratch = [pltpu.VMEM(val.shape, val.dtype) for val in (theta_k, theta_q, theta_v, w1, w2t)]
    scratch += [pltpu.VMEM((seqs, heads // 2) + shape, dtype) for shape, dtype in each]
    scratch += [pltpu.VMEM((heads // 2, 8, 128), f32)] * 2
    scratch += [pltpu.VMEM((seqs, steps * MINI_BATCH, model_dim), bf16), pltpu.VMEM((seqs, steps * MINI_BATCH, width), bf16)]
    ahead = AHEAD
    several = pltpu.VMEM((ahead, seqs, MINI_BATCH, width), f32)
    scratch += [several] * 3 + [pltpu.VMEM((seqs, MINI_BATCH, width), f32)] + [several] * 3
    own_steps = steps // parts_of_seq
    dma = pltpu.SemaphoreType.DMA
    half_turns = steps // (2 * AHEAD)
    scratch += [dma((9,)), dma((3,)), dma, dma, dma((half_turns,)), dma((half_turns,)), dma((2,)), dma((2,)), dma((2, parts_of_seq, 3)), dma((3,)), dma, dma, dma]
    early = 2 * own_len // 3
    scratch += [pltpu.VMEM((2 * width, model_dim), bf16), pltpu.VMEM((2, 4, early // 2, 2 * width), bf16), pltpu.VMEM((2, 4, early // 2, model_dim), bf16),
                pltpu.VMEM((num_seqs, early // 2, 2 * width), bf16), pltpu.VMEM((num_seqs, early // 2, model_dim), bf16), dma((2,)), dma((3,))]
    scratch += [pltpu.VMEM(val.shape, val.dtype) for val in (b1, b2, gain, bias)]
    return pl.pallas_call(
        functools.partial(layer_kernel, steps, seqs, heads, ahead, parts_of_seq),
        out_shape=(jax.ShapeDtypeStruct((num_seqs, own_len, 2 * width), bf16), jax.ShapeDtypeStruct((2 * width, model_dim), bf16),
                   jax.ShapeDtypeStruct((num_seqs, early, model_dim), bf16)),
        in_specs=[hbm] * 11 + [smem],
        out_specs=(hbm, hbm, hbm),
        scratch_shapes=scratch,
        compiler_params=pltpu.CompilerParams(vmem_limit_bytes=60 * 2 ** 20, collective_id=0, has_side_effects=True),
    )(tokens, w_out, theta_k, theta_q, theta_v, w1, w2t, b1, b2, gain, bias, rate)


def solution(mesh):
    parts_of_seq = mesh.shape['seq']

    def local_fn(tokens, theta_q, theta_k, theta_v, w_out, w_one, b_one, w_two, b_two, ln_gain, ln_bias, inner_lr):
        outs, w_full, y_early = run_layer(tokens, theta_k, theta_q, theta_v, w_out, w_one, jnp.swapaxes(w_two, 1, 2), b_one, b_two, ln_gain, ln_bias, inner_lr, parts_of_seq)
        return finish(outs, w_full, y_early)

    arg_specs = (P('data', 'seq', None), P(None, 'heads'), P(None, 'heads'), P(None, 'heads'), P('heads', None), P('heads', None, None), P('heads', None), P('heads', None, None), P('heads', None), P('heads', None), P('heads', None), P('heads'))
    return jax.shard_map(local_fn, mesh=mesh, in_specs=arg_specs, out_specs=P('data', 'seq', None), check_vma=False)
```
